32 devices in a mesh: lat: 8 (over y, x, core), lev: 4 (over z).
Axes of the slice: x: 2, y: 2, z: 4, core: 2. Of those that a mesh axis runs over, the one named last changes fastest.
Arguments:
- prognostic: float32 [4, 12, 64, 768], P(None, 'lev', 'lat'), may hold values from -6 to 6
- cotangent: bfloat16 [4, 12, 64, 768], P(None, 'lev', 'lat'), may hold values from -6 to 6
- damping: float32 [4, 12], P(None, 'lev'), may hold values from 1 to 30
- in_scale: float32 [4, 12], replicated, may hold values from 0.5 to 4
- w_in: bfloat16 [512, 48], replicated, may hold values from -0.875 to 0.875
- b_in: float32 [512], replicated, may hold values from -3 to 3
- w_mid: bfloat16 [512, 512], replicated, may hold values from -0.25 to 0.25
- b_mid: float32 [512], replicated, may hold values from -3 to 3
- w_out: bfloat16 [48, 512], replicated, may hold values from -0.25 to 0.25
- wave_order: int32 [256], replicated, may hold values from 0 to 255, as said below
- lat_order: int32 [64], replicated, may hold values from 0 to 63, each once
Outputs:
- new_state: float32 [4, 12, 64, 768], P(None, 'lev', 'lat')
- spectral: float32 [256, 2, 4, 12, 256], P('lat', None, None, 'lev')
- grad_w_in: float32 [512, 48], replicated
- grad_b_in: float32 [512], replicated
- grad_w_mid: float32 [512, 512], replicated
- grad_b_mid: float32 [512], replicated
- grad_w_out: float32 [48, 512], replicated
The draws below stay inside these ranges and needn't reach their ends.
Inputs may be any that keep to these rules, and one draw needn't show every extreme that they name: `wave_order`: A permutation of the wavenumbers. Block d, entries d * 32 to (d + 1) * 32 - 1, lists the wavenumbers owned by index d of lat: one from each run of 8 consecutive wavenumbers, taken from alternate ends of the runs so that the triangular work of the blocks is nearly equal. `lat_order`: A permutation of the latitudes.
All inputs are finite; a program needn't handle non-finite values.
Results may differ from the reference program's by a relative error of at most 0.006.
Values may be sent and summed in bfloat16 or wider, within the bound.
No kernel may reach another device: no remote copies, remote signals or barrier semaphores. Data moves between devices by JAX's collectives and lax.ppermute only.
A program may use at most 64 MiB of HBM per device.

```python
import math
import jax
import jax.numpy as jnp
from jax import lax

TRUNC = 256
NLON = 768
FIELDS = 4
HIDDEN_SIZE = 512
WAVE_DEV = 32
NLAT = 64
NLEV = 12
FEAT = 48
N_LAT = 8


def draw_wave_order(key, part):
    owners = jax.random.permutation(jax.random.fold_in(key, 11), N_LAT).astype(jnp.int32)
    groups = jnp.arange(WAVE_DEV, dtype=jnp.int32)
    position = jnp.where(groups[None, :] % 2 == 0, owners[:, None], N_LAT - 1 - owners[:, None])
    return (groups[None, :] * N_LAT + position).reshape(TRUNC).astype(jnp.int32)


def steps_of(own_key, extent, cuts, least, top_value):
    level, own = 1.0, jax.random.fold_in(own_key, 6)
    for dim, shards_of in cuts:
        heights = jnp.exp(jax.random.uniform(jax.random.fold_in(own, dim), (shards_of,), jnp.float32, least / len(cuts), top_value / len(cuts)))
        level = level * jnp.repeat(heights, extent[dim] // shards_of).reshape([-1 if axis == dim else 1 for axis in range(len(extent))])
    return level


def gaussian(key, shape, spread, most, pieces=(), kind=jnp.bfloat16):
    factor_of = steps_of(key, shape, pieces, -0.22, 0.18) if pieces else 1.0
    array = jax.random.normal(key, shape, jnp.float32) * spread * factor_of
    return jnp.minimum(jnp.maximum(array, -most), most).astype(kind)


def setup_inputs(seed: int = 0) -> dict:
    seeds = jax.random.split(jax.random.key(seed), 12)
    return {
        "prognostic": gaussian(seeds[0], (FIELDS, NLEV, NLAT, NLON), 1.0, 6.0, ((1, 4), (2, 8)), jnp.float32),
        "cotangent": gaussian(seeds[1], (FIELDS, NLEV, NLAT, NLON), 1.0, 6.0, ((1, 4), (2, 8))),
        "damping": jnp.clip(jnp.exp(math.log(30.0) - 3.4011974 * jax.random.uniform(seeds[2], (FIELDS, NLEV), jnp.float32) ** steps_of(seeds[2], (FIELDS, NLEV), ((1, 4),), -0.2, 0.2)), 1.0, 30.0),
        "in_scale": jnp.clip(jnp.exp(jax.random.uniform(seeds[3], (FIELDS, NLEV), jnp.float32, math.log(0.5), math.log(4.0))), 0.5, 4.0),
        "w_in": gaussian(seeds[4], (HIDDEN_SIZE, FEAT), FEAT ** -0.5, 0.875),
        "b_in": gaussian(seeds[5], (HIDDEN_SIZE,), 0.5, 3.0, (), jnp.float32),
        "w_mid": gaussian(seeds[6], (HIDDEN_SIZE, HIDDEN_SIZE), HIDDEN_SIZE ** -0.5, 0.25),
        "b_mid": gaussian(seeds[7], (HIDDEN_SIZE,), 0.5, 3.0, (), jnp.float32),
        "w_out": gaussian(seeds[8], (FEAT, HIDDEN_SIZE), HIDDEN_SIZE ** -0.5, 0.25),
        "wave_order": draw_wave_order(jax.random.fold_in(seeds[11], 71), 0),
        "lat_order": jax.random.permutation(seeds[10], NLAT).astype(jnp.int32),
    }


block_rows = 32
rescale_bits = 40.0

def legendre_setup(own_waves, colatitude):
    float_type = colatitude.dtype
    all_orders = jnp.arange(TRUNC, dtype=jnp.int32)
    factor_index = jnp.arange(1, TRUNC, dtype=jnp.int32).astype(float_type)
    ratios = 0.5 * jnp.log((2.0 * factor_index + 1.0) / (2.0 * factor_index))
    totals = jnp.concatenate([jnp.zeros((1,), float_type), jnp.cumsum(ratios)])
    matches = own_waves[:, None] == all_orders[None, :]
    diagonal_log = lax.optimization_barrier(jnp.sum(jnp.where(matches, totals[None, :], 0.0), axis=1)) - 0.5 * math.log(2.0)
    orders = own_waves.astype(float_type)
    log_shift = diagonal_log[:, None] + orders[:, None] * jnp.log(jnp.sin(colatitude))[None, :]
    empty_rows = jnp.zeros_like(log_shift)
    return (empty_rows, empty_rows, log_shift)

def legendre_rows(recurrence, first_degree, orders, cosine):
    latest, before, log_shift = recurrence
    rescale_limit = 2.0 ** rescale_bits
    squared_order = orders * orders
    table_rows = []
    for offset in range(block_rows):
        degree = (first_degree + offset).astype(cosine.dtype)
        upper_coef = jnp.sqrt(jnp.maximum(4.0 * degree * degree - 1.0, 0.0) / jnp.maximum(degree * degree - squared_order, 1.0))
        lower_num = jnp.maximum((degree - 1.0) * (degree - 1.0) - squared_order, 0.0)
        lower_coef = jnp.sqrt(lower_num / jnp.maximum(4.0 * (degree - 1.0) * (degree - 1.0) - 1.0, 1.0))
        recurred = upper_coef[:, None] * (cosine[None, :] * latest - lower_coef[:, None] * before)
        diagonal_start = jnp.where(degree == orders, 1.0, 0.0)[:, None] * jnp.ones_like(latest)
        newest = jnp.where((degree > orders)[:, None], recurred, diagonal_start)
        too_large = jnp.abs(newest) > rescale_limit
        factor = jnp.where(too_large, 1.0 / rescale_limit, 1.0)
        newest = newest * factor
        latest = latest * factor
        log_shift = log_shift + jnp.where(too_large, rescale_bits * math.log(2.0), 0.0)
        table_rows.append(newest * jnp.exp(log_shift))
        before = latest
        latest = newest
    return ((latest, before, log_shift), jnp.stack(table_rows, axis=1))

def spectral_pass(own_waves, colatitude, fourier, damping):
    float_type = fourier.dtype
    lat_total = colatitude.shape[0]
    weight = math.pi / lat_total * jnp.sin(colatitude)
    cosine = jnp.cos(colatitude)
    orders = own_waves.astype(float_type)
    weighted = fourier * weight
    degree_norm = 1.0 / (TRUNC * (TRUNC - 1.0))

    def visit_block(carried, first_degree):
        recurrence, grid_sum = carried
        recurrence, legendre_table = legendre_rows(recurrence, first_degree, orders, cosine)
        coeffs = jnp.einsum('jbn,jkfen->jkfeb', legendre_table, weighted, precision=lax.Precision.HIGHEST)
        degree = (first_degree + jnp.arange(block_rows, dtype=jnp.int32)).astype(float_type)
        degree_ratio = degree * (degree + 1.0) * degree_norm
        coeffs = coeffs / (1.0 + damping[:, :, None] * (degree_ratio * degree_ratio)[None, None, :])
        grid_sum = grid_sum + jnp.einsum('jbn,jkfeb->jkfen', legendre_table, coeffs, precision=lax.Precision.HIGHEST)
        return ((recurrence, grid_sum), coeffs)
    starts = jnp.arange(0, TRUNC, block_rows, dtype=jnp.int32)
    initial = (legendre_setup(own_waves, colatitude), jnp.zeros_like(fourier))
    (recurrence, synthesized), blocks = lax.scan(visit_block, initial, starts)
    waves, two, fields, levels = fourier.shape[:4]
    coeffs = jnp.moveaxis(blocks, 0, 4).reshape(waves, two, fields, levels, TRUNC)
    return (coeffs, synthesized)

def silu_slope(value):
    sigmoid_value = jax.nn.sigmoid(value)
    return sigmoid_value * (1.0 + value * (1.0 - sigmoid_value))

def column_physics(inputs, upstream, w_in, b_in, w_mid, b_mid, w_out):
    pre_in = jnp.dot(w_in, inputs, preferred_element_type=jnp.float32) + b_in[:, None]
    hidden_in = jax.nn.silu(pre_in).astype(jnp.bfloat16)
    pre_mid = jnp.dot(w_mid, hidden_in, preferred_element_type=jnp.float32) + b_mid[:, None]
    hidden_mid = jax.nn.silu(pre_mid).astype(jnp.bfloat16)
    tendency = jnp.dot(w_out, hidden_mid, preferred_element_type=jnp.float32).astype(jnp.bfloat16)
    grad_out = jnp.dot(upstream, hidden_mid.T, preferred_element_type=jnp.float32)
    back_mid = jnp.dot(w_out.T, upstream, preferred_element_type=jnp.float32)
    delta_mid = (back_mid * silu_slope(pre_mid)).astype(jnp.bfloat16)
    grad_mid = jnp.dot(delta_mid, hidden_in.T, preferred_element_type=jnp.float32)
    grad_bmid = lax.optimization_barrier(jnp.sum(delta_mid.astype(jnp.float32), axis=1))
    back_in = jnp.dot(w_mid.T, delta_mid, preferred_element_type=jnp.float32)
    delta_in = (back_in * silu_slope(pre_in)).astype(jnp.bfloat16)
    grad_in = jnp.dot(delta_in, inputs.T, preferred_element_type=jnp.float32)
    grad_bin = lax.optimization_barrier(jnp.sum(delta_in.astype(jnp.float32), axis=1))
    return (tendency, (grad_in, grad_bin, grad_mid, grad_bmid, grad_out))

def physics_rows(inputs, upstream, w_in, b_in, w_mid, b_mid, w_out):
    fields, lev_total, lat_rows, lon_count = inputs.shape
    features = fields * lev_total
    hidden_units = w_in.shape[0]
    rows_in = jnp.moveaxis(inputs.reshape(features, lat_rows, lon_count), 1, 0)
    rows_up = jnp.moveaxis(upstream.reshape(features, lat_rows, lon_count), 1, 0)

    def visit_row(totals, row_pair):
        tendency, gradients = column_physics(row_pair[0], row_pair[1], w_in, b_in, w_mid, b_mid, w_out)
        return (jax.tree.map(jnp.add, totals, gradients), tendency)
    empty_sums = (jnp.zeros((hidden_units, features), jnp.float32), jnp.zeros((hidden_units,), jnp.float32), jnp.zeros((hidden_units, hidden_units), jnp.float32), jnp.zeros((hidden_units,), jnp.float32), jnp.zeros((features, hidden_units), jnp.float32))
    totals, tend_rows = lax.scan(visit_row, empty_sums, (rows_in, rows_up))
    tendency = jnp.moveaxis(tend_rows, 0, 1).reshape(fields, lev_total, lat_rows, lon_count)
    return (tendency, totals)

def reference(prognostic, cotangent, damping, in_scale, w_in, b_in, w_mid, b_mid, w_out, wave_order, lat_order):
    float_type = prognostic.dtype
    fields, lev_total, lat_total, lon_count = prognostic.shape
    colatitude = math.pi * (lat_order.astype(float_type) + 0.5) / lat_total
    spectrum = jnp.fft.rfft(prognostic, axis=3)[:, :, :, :TRUNC] / lon_count
    complex_parts = jnp.stack([jnp.real(spectrum), jnp.imag(spectrum)], axis=0).astype(float_type)
    fourier = jnp.transpose(complex_parts, (4, 0, 1, 2, 3))
    coeffs, synthesized = spectral_pass(jnp.arange(TRUNC, dtype=jnp.int32), colatitude, fourier, damping)
    spectral = jnp.take(coeffs, wave_order, axis=0)
    wave_modes = jnp.transpose(synthesized[:, 0] + 1j * synthesized[:, 1], (1, 2, 3, 0))
    padded = jnp.pad(wave_modes, ((0, 0), (0, 0), (0, 0), (0, lon_count // 2 + 1 - TRUNC)))
    filtered = (jnp.fft.irfft(padded, n=lon_count, axis=3) * lon_count).astype(float_type)
    inputs = (filtered * in_scale[:, :, None, None]).astype(jnp.bfloat16)
    tendency, totals = physics_rows(inputs, cotangent, w_in, b_in, w_mid, b_mid, w_out)
    new_state = filtered + tendency.astype(float_type)
    grad_scale = 1.0 / math.sqrt(lat_total * lon_count)
    gradients = jax.tree.map(lambda value: value * grad_scale, totals)
    return (new_state, spectral, gradients[0], gradients[1], gradients[2], gradients[3], gradients[4])
```

```python
import functools
import math

import jax
import jax.numpy as jnp
import numpy as np
from jax import lax
from jax.experimental import pallas as pl
from jax.experimental.pallas import tpu as pltpu
from jax.sharding import PartitionSpec as P

TRUNC = 256


block_rows = 32
rescale_bits = 40.0


def legendre_setup(own_waves, colatitude):
    float_type = colatitude.dtype
    all_orders = jnp.arange(TRUNC, dtype=jnp.int32)
    factor_index = jnp.arange(1, TRUNC, dtype=jnp.int32).astype(float_type)
    ratios = 0.5 * jnp.log((2.0 * factor_index + 1.0) / (2.0 * factor_index))
    totals = jnp.concatenate([jnp.zeros((1,), float_type), jnp.cumsum(ratios)])
    matches = own_waves[:, None] == all_orders[None, :]
    diagonal_log = jnp.sum(jnp.where(matches, totals[None, :], 0.0), axis=1) - 0.5 * math.log(2.0)
    orders = own_waves.astype(float_type)
    log_shift = diagonal_log[:, None] + orders[:, None] * jnp.log(jnp.sin(colatitude))[None, :]
    empty_rows = jnp.zeros_like(log_shift)
    return (empty_rows, empty_rows, log_shift)


def legendre_rows(recurrence, first_degree, orders, cosine):
    latest, before, log_shift = recurrence
    rescale_limit = 2.0**rescale_bits
    squared_order = orders * orders
    table_rows = []
    for offset in range(block_rows):
        degree = (first_degree + offset).astype(cosine.dtype)
        upper_coef = jnp.sqrt(
            jnp.maximum(4.0 * degree * degree - 1.0, 0.0)
            / jnp.maximum(degree * degree - squared_order, 1.0)
        )
        lower_num = jnp.maximum((degree - 1.0) * (degree - 1.0) - squared_order, 0.0)
        lower_coef = jnp.sqrt(
            lower_num / jnp.maximum(4.0 * (degree - 1.0) * (degree - 1.0) - 1.0, 1.0)
        )
        recurred = upper_coef[:, None] * (cosine[None, :] * latest - lower_coef[:, None] * before)
        diagonal_start = jnp.where(degree == orders, 1.0, 0.0)[:, None] * jnp.ones_like(latest)
        newest = jnp.where((degree > orders)[:, None], recurred, diagonal_start)
        too_large = jnp.abs(newest) > rescale_limit
        factor = jnp.where(too_large, 1.0 / rescale_limit, 1.0)
        newest = newest * factor
        latest = latest * factor
        log_shift = log_shift + jnp.where(too_large, rescale_bits * math.log(2.0), 0.0)
        table_rows.append(newest * jnp.exp(log_shift))
        before = latest
        latest = newest
    return ((latest, before, log_shift), jnp.stack(table_rows, axis=1))


def spectral_pass(own_waves, colatitude, fourier, damping):
    float_type = fourier.dtype
    lat_total = colatitude.shape[0]
    weight = math.pi / lat_total * jnp.sin(colatitude)
    cosine = jnp.cos(colatitude)
    orders = own_waves.astype(float_type)
    weighted = fourier * weight
    degree_norm = 1.0 / (TRUNC * (TRUNC - 1.0))

    def visit_block(carried, first_degree):
        recurrence, grid_sum = carried
        recurrence, legendre_table = legendre_rows(recurrence, first_degree, orders, cosine)
        coeffs = jnp.einsum(
            "jbn,jkfen->jkfeb", legendre_table, weighted, precision=lax.Precision.HIGHEST
        )
        degree = (first_degree + jnp.arange(block_rows, dtype=jnp.int32)).astype(float_type)
        degree_ratio = degree * (degree + 1.0) * degree_norm
        coeffs = coeffs / (1.0 + damping[:, :, None] * (degree_ratio * degree_ratio)[None, None, :])
        grid_sum = grid_sum + jnp.einsum(
            "jbn,jkfeb->jkfen", legendre_table, coeffs, precision=lax.Precision.HIGHEST
        )
        return ((recurrence, grid_sum), coeffs)

    starts = jnp.arange(0, TRUNC, block_rows, dtype=jnp.int32)
    initial = (legendre_setup(own_waves, colatitude), jnp.zeros_like(fourier))
    (recurrence, synthesized), blocks = lax.scan(visit_block, initial, starts)
    waves, two, fields, levels = fourier.shape[:4]
    coeffs = jnp.moveaxis(blocks, 0, 4).reshape(waves, two, fields, levels, TRUNC)
    return (coeffs, synthesized)


def fourier_angles(wave_order, lon_count):
    points = jnp.arange(lon_count, dtype=jnp.int32)
    phase_index = wave_order[:, None] * points[None, :] % lon_count
    return phase_index.astype(jnp.float32) * (2.0 * math.pi / lon_count)


def fourier_forward(wave_order, lon_count):
    angles = fourier_angles(wave_order, lon_count)
    return jnp.stack([jnp.cos(angles), -jnp.sin(angles)], axis=1) / lon_count


def fourier_inverse(wave_order, lon_count):
    angles = fourier_angles(wave_order, lon_count)
    weights = jnp.where(wave_order == 0, 1.0, 2.0)[:, None, None]
    return weights * jnp.stack([jnp.cos(angles), -jnp.sin(angles)], axis=1)


def silu_slope(value):
    sigmoid_value = jax.nn.sigmoid(value)
    return sigmoid_value * (1.0 + value * (1.0 - sigmoid_value))


def column_physics(inputs, upstream, w_in, b_in, w_mid, b_mid, w_out):
    pre_in = jnp.dot(w_in, inputs, preferred_element_type=jnp.float32) + b_in[:, None]
    hidden_in = jax.nn.silu(pre_in).astype(jnp.bfloat16)
    pre_mid = jnp.dot(w_mid, hidden_in, preferred_element_type=jnp.float32) + b_mid[:, None]
    hidden_mid = jax.nn.silu(pre_mid).astype(jnp.bfloat16)
    tendency = jnp.dot(w_out, hidden_mid, preferred_element_type=jnp.float32).astype(jnp.bfloat16)
    grad_out = jnp.dot(upstream, hidden_mid.T, preferred_element_type=jnp.float32)
    back_mid = jnp.dot(w_out.T, upstream, preferred_element_type=jnp.float32)
    delta_mid = (back_mid * silu_slope(pre_mid)).astype(jnp.bfloat16)
    grad_mid = jnp.dot(delta_mid, hidden_in.T, preferred_element_type=jnp.float32)
    grad_bmid = jnp.sum(delta_mid.astype(jnp.float32), axis=1)
    back_in = jnp.dot(w_mid.T, delta_mid, preferred_element_type=jnp.float32)
    delta_in = (back_in * silu_slope(pre_in)).astype(jnp.bfloat16)
    grad_in = jnp.dot(delta_in, inputs.T, preferred_element_type=jnp.float32)
    grad_bin = jnp.sum(delta_in.astype(jnp.float32), axis=1)
    return (tendency, (grad_in, grad_bin, grad_mid, grad_bmid, grad_out))


def physics_rows(inputs, upstream, w_in, b_in, w_mid, b_mid, w_out):
    fields, lev_total, lat_rows, lon_count = inputs.shape
    features = fields * lev_total
    hidden_units = w_in.shape[0]
    rows_in = jnp.moveaxis(inputs.reshape(features, lat_rows, lon_count), 1, 0)
    rows_up = jnp.moveaxis(upstream.reshape(features, lat_rows, lon_count), 1, 0)

    def visit_row(totals, row_pair):
        tendency, gradients = column_physics(
            row_pair[0], row_pair[1], w_in, b_in, w_mid, b_mid, w_out
        )
        return (jax.tree.map(jnp.add, totals, gradients), tendency)

    empty_sums = (
        jnp.zeros((hidden_units, features), jnp.float32),
        jnp.zeros((hidden_units,), jnp.float32),
        jnp.zeros((hidden_units, hidden_units), jnp.float32),
        jnp.zeros((hidden_units,), jnp.float32),
        jnp.zeros((features, hidden_units), jnp.float32),
    )
    totals, tend_rows = lax.scan(visit_row, empty_sums, (rows_in, rows_up))
    tendency = jnp.moveaxis(tend_rows, 0, 1).reshape(fields, lev_total, lat_rows, lon_count)
    return (tendency, totals)


def on_device(
    prognostic, cotangent, damping, in_scale, w_in, b_in, w_mid, b_mid, w_out, wave_order, lat_order
):
    fields, lev_dev, lat_dev, lon_count = prognostic.shape
    lat_width = lax.axis_size("lat")
    wave_dev = wave_order.shape[0] // lat_width
    lat_total = lat_order.shape[0]
    my_index = lax.axis_index("lat")
    own_waves = lax.dynamic_slice_in_dim(wave_order, my_index * wave_dev, wave_dev)
    to_fourier = fourier_forward(wave_order, lon_count)
    fourier = jnp.einsum("jkn,fean->jkfea", to_fourier, prognostic, precision=lax.Precision.HIGHEST)
    fourier = lax.all_to_all(fourier, "lat", split_axis=0, concat_axis=4, tiled=True)
    colatitude = math.pi * (lat_order.astype(jnp.float32) + 0.5) / lat_total
    spectral, synthesized = spectral_pass(own_waves, colatitude, fourier, damping)
    upstream = lax.all_to_all(cotangent, "lev", split_axis=2, concat_axis=1, tiled=True)
    from_fourier = fourier_inverse(wave_order, lon_count)
    row_modes = lax.all_to_all(synthesized, "lat", split_axis=4, concat_axis=0, tiled=True)
    filtered = jnp.einsum(
        "jkfea,jkn->fean", row_modes, from_fourier, precision=lax.Precision.HIGHEST
    )
    lev_index = lax.axis_index("lev")
    local_scale = lax.dynamic_slice_in_dim(in_scale, lev_index * lev_dev, lev_dev, 1)
    local_inputs = (filtered * local_scale[:, :, None, None]).astype(jnp.bfloat16)
    inputs = lax.all_to_all(local_inputs, "lev", split_axis=2, concat_axis=1, tiled=True)
    tend_cols, totals = physics_rows(inputs, upstream, w_in, b_in, w_mid, b_mid, w_out)
    tendency = lax.all_to_all(tend_cols, "lev", split_axis=1, concat_axis=2, tiled=True)
    new_state = filtered + tendency.astype(jnp.float32)
    grad_scale = 1.0 / math.sqrt(lat_total * lon_count)
    summed = lax.psum(
        (
            totals[0] * grad_scale,
            totals[1] * grad_scale,
            totals[2] * grad_scale,
            totals[3] * grad_scale,
            totals[4] * grad_scale,
        ),
        ("lat", "lev"),
    )
    return (new_state, spectral, summed[0], summed[1], summed[2], summed[3], summed[4])


LANES = 128
half_lanes = LANES // 2
feature_rows = 16
bf16 = jnp.bfloat16
f32 = jnp.float32
forward_type = f32
inverse_type = f32
state_type = bf16
grad_type = bf16


def contract_last(left, right):
    return lax.dot_general(left, right, (((1,), (1,)), ((), ())), preferred_element_type=f32)


def matmul(left, right):
    return lax.dot_general(left, right, (((1,), (0,)), ((), ())), preferred_element_type=f32)


def half_turn_sincos(half_angle):
    square = half_angle * half_angle
    sine = 0.0
    cosine = 0.0
    for power in range(6, -1, -1):
        sine = sine * square + (-1.0) ** power / math.factorial(2 * power + 1)
        cosine = cosine * square + (-1.0) ** power / math.factorial(2 * power)
    sine = sine * half_angle
    return 2.0 * sine * cosine, 1.0 - 2.0 * sine * sine


def turn_sincos(product, period):
    reduced = product - period * jnp.floor(product * (1.0 / period) + 0.5)
    return half_turn_sincos(reduced * (math.pi / period))


def lower_lanes(shape):
    return lax.broadcasted_iota(jnp.int32, shape, len(shape) - 1) < half_lanes


def split_pair(value):
    high = value.astype(bf16)
    return high, (value - high.astype(f32)).astype(bf16)


def polar_sine(lat_index, lat_total):
    nearest = jnp.minimum(lat_index, (lat_total - 1.0) - lat_index)
    return half_turn_sincos((nearest + 0.5) * (0.5 * math.pi / lat_total))


def wave_columns(waves_ref):
    return jnp.broadcast_to(waves_ref[...].astype(f32), (LANES, waves_ref.shape[1])).T


def forward_kernel(
    lats_ref, waves_ref, prog_ref, cot_ref, send_ref, high_ref, low_ref, *rest
):
    *cot_refs, cot_scratch = rest
    lat_width, half_rows, _ = send_ref.shape
    wave_total = waves_ref.shape[1]
    wave_dev = wave_total // lat_width
    rows_total, lon_count = prog_ref.shape
    lat_total = lats_ref.shape[0]
    lat_dev = lat_total // lat_width
    waves = wave_columns(waves_ref)
    lane = lax.broadcasted_iota(jnp.int32, waves.shape, 1).astype(f32)
    sine, cosine = turn_sincos(waves * lane, float(lon_count))
    step_sine, step_cosine = turn_sincos(waves * float(LANES), float(lon_count))
    for tile in range(lon_count // LANES):
        lanes = pl.ds(tile * LANES, LANES)
        cosines = split_pair(cosine)
        sines = split_pair(-sine)
        for owner in range(lat_width):
            rows = slice(owner * wave_dev, (owner + 1) * wave_dev)
            for ref, cosine_part, sine_part in zip((high_ref, low_ref), cosines, sines):
                ref[pl.ds(2 * owner * wave_dev, wave_dev), lanes] = cosine_part[rows]
                ref[pl.ds((2 * owner + 1) * wave_dev, wave_dev), lanes] = sine_part[rows]
        cosine, sine = (
            cosine * step_cosine - sine * step_sine,
            sine * step_cosine + cosine * step_sine,
        )
    prog_high, prog_low = split_pair(prog_ref[...])
    modes = contract_last(jnp.concatenate([prog_high, prog_low], axis=0), high_ref[...])
    modes = modes[:rows_total] + modes[rows_total:] + contract_last(prog_high, low_ref[...])
    first_row = lax.axis_index("lat") * lat_dev
    row = lax.broadcasted_iota(jnp.int32, (lat_dev, LANES), 0)
    lat_index = jnp.zeros((lat_dev, LANES), f32)
    for at in range(lat_dev):
        lat_index = jnp.where(row == at, lats_ref[first_row + at].astype(f32), lat_index)
    weight = polar_sine(lat_index, lat_total)[0] * (math.pi / lat_total / lon_count)
    weight = jnp.concatenate([weight] * (half_rows // lat_dev), axis=0)
    lower = lower_lanes((half_rows, LANES))
    for tile in range(lat_width // 2):
        first = modes[:half_rows, tile * LANES : (tile + 1) * LANES] * weight
        second = modes[half_rows:, tile * LANES : (tile + 1) * LANES] * weight
        send_ref[2 * tile] = jnp.where(lower, first, pltpu.roll(second, half_lanes, 1)).astype(send_ref.dtype)
        send_ref[2 * tile + 1] = jnp.where(
            lower, pltpu.roll(first, half_lanes, 1), second
        ).astype(send_ref.dtype)
    lev_width = len(cot_refs)
    row_share = lat_dev // lev_width
    cot_scratch[...] = jnp.zeros_like(cot_scratch)
    cot_all = cot_ref[...].astype(f32)
    tiles = lon_count // LANES
    for tile in range(tiles):
        cot_scratch[tile, pl.ds(0, rows_total), :] = cot_all[:, tile * LANES : (tile + 1) * LANES]
    for shift in range(lev_width):
        dest = (lax.axis_index("lev") + shift) % lev_width
        for share in range(row_share):
            for tile in range(tiles):
                picked = cot_scratch[tile, pl.ds(dest * row_share + share, feature_rows, stride=lat_dev), :]
                cot_refs[shift][share, :, pl.ds(tile * LANES, LANES)] = picked.astype(bf16)


def table_kernel(lats_ref, waves_ref, out_ref, scratch, columns):
    pair_count, degrees, _ = out_ref.shape
    rows = pair_count
    lat_total = lats_ref.shape[1]
    columns[...] = wave_columns(waves_ref)
    first_wave = pl.multiple_of(lax.axis_index("lat") * 2 * rows, 2 * rows)
    orders = jnp.where(
        lower_lanes((rows, LANES)),
        columns[pl.ds(first_wave, rows), :],
        columns[pl.ds(first_wave + rows, rows), :],
    )
    lat_row = lats_ref[...].astype(f32)
    lat_index = jnp.broadcast_to(jnp.concatenate([lat_row, lat_row], axis=1), (rows, LANES))
    sine, cosine = polar_sine(lat_index, lat_total)
    cosine = jnp.where(2.0 * lat_index < lat_total - 1.0, cosine, -cosine)
    index = lax.broadcasted_iota(jnp.int32, (rows, degrees), 1).astype(f32)
    index = jnp.maximum(index, 1.0)
    ratios = 0.5 * jnp.log((2.0 * index + 1.0) / (2.0 * index))
    position = lax.broadcasted_iota(jnp.int32, (rows, degrees), 1)
    counted = position.astype(f32)
    totals = []
    for half in range(2):
        wave = jnp.broadcast_to(orders[:, half * half_lanes : half * half_lanes + 1], (rows, degrees))
        chosen = jnp.where((position > 0) & (counted <= wave), ratios, 0.0)
        totals.append(jnp.broadcast_to(jnp.sum(chosen, axis=1, keepdims=True), (rows, LANES)))
    diagonal_log = jnp.where(lower_lanes((rows, LANES)), totals[0], totals[1])
    log_shift = (
        diagonal_log
        - 0.5 * math.log(2.0)
        - 0.5 * jnp.log(2.0 * orders + 1.0)
        + orders * jnp.log(sine)
    )
    squared = orders * orders
    limit = 2.0**rescale_bits
    zero = jnp.zeros((rows, LANES), f32)

    def visit(block, carried):
        latest, before, previous_root, log_shift = carried
        scale = jnp.exp(log_shift)
        for offset in range(8):
            degree_int = block * 8 + offset
            degree = jnp.full((rows, LANES), degree_int, jnp.int32).astype(f32)
            gap = degree * degree - squared
            inverse_root = lax.rsqrt(jnp.maximum(gap, 1.0))
            root = gap * inverse_root
            recurred = inverse_root * (
                (2.0 * degree - 1.0) * cosine * latest - previous_root * before
            )
            newest = jnp.where(gap > 0.0, recurred, jnp.where(gap == 0.0, 1.0, 0.0))
            scratch[pl.ds(degree_int * rows, rows), :] = newest * scale
            before = latest
            latest = newest
            previous_root = jnp.maximum(root, 0.0)
        too_large = jnp.abs(latest) > limit
        factor = jnp.where(too_large, 1.0 / limit, 1.0)
        log_shift = log_shift + jnp.where(too_large, rescale_bits * math.log(2.0), 0.0)
        return latest * factor, before * factor, previous_root, log_shift

    lax.fori_loop(0, degrees // 8, visit, (zero, zero, zero, log_shift))

    def unpack(pair, carried):
        high, low = split_pair(scratch[pl.ds(pair, degrees, stride=rows), :])
        out_ref[pair, :, pl.ds(0, LANES)] = high
        out_ref[pair, :, pl.ds(LANES, LANES)] = low
        return carried

    lax.fori_loop(0, pair_count, unpack, 0)


def spectral_kernel(
    waves_ref, damping_ref, recv_ref, table_ref, spec_ref, send_ref, modes, sums, picked
):
    pair_count, degrees, _ = table_ref.shape
    wave_dev = 2 * pair_count
    lat_width, half_rows, _ = recv_ref.shape
    lat_total = LANES // 2
    lat_dev = lat_total // lat_width
    fields, lev_dev = damping_ref.shape
    pairs = fields * lev_dev
    half_pairs = pairs // 2
    first_wave = lax.axis_index("lat") * wave_dev
    received = recv_ref[...].astype(f32)
    upper_rows = lax.broadcasted_iota(jnp.int32, (LANES, LANES), 0) % wave_dev >= pair_count
    for index in range(half_pairs):
        stacked = [
            received[source, index * lat_dev : (index + 1) * lat_dev] for source in range(lat_width)
        ]
        stacked.append(jnp.zeros((LANES - lat_total, LANES), f32))
        turned = jnp.concatenate(stacked, axis=0).T
        turned = jnp.where(upper_rows, pltpu.roll(turned, half_lanes, 1), turned)
        for half in range(2):
            for part in range(2):
                start = (half * 2 + part) * wave_dev
                place = (part * pairs + half * half_pairs + index) * wave_dev
                modes[pl.ds(place, wave_dev), :] = turned[start : start + wave_dev]
    degree = lax.broadcasted_iota(jnp.int32, (pairs, degrees), 1).astype(f32)
    degree_ratio = degree * (degree + 1.0) * (1.0 / (degrees * (degrees - 1.0)))
    root = jnp.sqrt(2.0 * degree + 1.0)
    row = lax.broadcasted_iota(jnp.int32, (pairs, degrees), 0)
    strength = jnp.zeros((pairs, degrees), f32)
    for pair in range(pairs):
        strength = jnp.where(row == pair, damping_ref[pair // lev_dev, pair % lev_dev], strength)
    damp = root / (1.0 + strength * (degree_ratio * degree_ratio))
    damp = jnp.concatenate([damp, damp, damp, damp], axis=0)
    root_row = root[:1]
    count = 2 * pairs
    for pair in range(pair_count):
        first = modes[pl.ds(pair, count, stride=wave_dev), :]
        second = modes[pl.ds(pair + pair_count, count, stride=wave_dev), :]
        stacked = jnp.concatenate([first, second], axis=0)
        table = table_ref[pair]
        if recv_ref.dtype == f32:
            stacked = jnp.concatenate(split_pair(stacked), axis=0)
        else:
            stacked = stacked.astype(bf16)
        coeffs = contract_last(jnp.concatenate([stacked, stacked], axis=1), table)
        if recv_ref.dtype == f32:
            coeffs = coeffs[: 2 * count] + coeffs[2 * count :]
        coeffs = coeffs * damp
        spec_ref[pair] = coeffs[:count]
        spec_ref[pair + pair_count] = coeffs[count:]
        first_weight = jnp.where(waves_ref[first_wave + pair] == 0, 1.0, 2.0)
        second_weight = jnp.where(waves_ref[first_wave + pair + pair_count] == 0, 1.0, 2.0)
        rooted = jnp.concatenate(
            [coeffs[:count] * (root_row * first_weight), coeffs[count:] * (root_row * second_weight)],
            axis=0,
        )
        synth = matmul(jnp.concatenate(split_pair(rooted), axis=0), table)
        synth = synth[: 2 * count] + synth[2 * count :]
        synth = synth[:, :LANES] + synth[:, LANES:]
        sums[pl.ds(pair, count, stride=wave_dev), :] = synth[:count]
        sums[pl.ds(pair + pair_count, count, stride=wave_dev), :] = synth[count:]
    owners = send_ref.shape[0] // feature_rows
    lower = lower_lanes((owners, LANES))
    share = lat_total // owners
    blank = jnp.zeros((owners, LANES), f32)
    for row in range(pairs, feature_rows):
        picked[pl.ds(lat_total + row, owners, stride=feature_rows), :] = blank
    for index in range(half_pairs):
        blocks = []
        for half in range(2):
            for part in range(2):
                place = (part * pairs + half * half_pairs + index) * wave_dev
                blocks.append(sums[pl.ds(place, wave_dev), :])
        stacked = jnp.concatenate(blocks, axis=0)
        stacked = jnp.where(upper_rows, pltpu.roll(stacked, half_lanes, 1), stacked)
        picked[pl.ds(0, lat_total), :] = stacked.T[:lat_total]
        even = picked[pl.ds(0, owners, stride=share), :]
        odd = picked[pl.ds(1, owners, stride=share), :]
        picked[pl.ds(lat_total + index, owners, stride=feature_rows), :] = jnp.where(
            lower, even, pltpu.roll(odd, half_lanes, 1)
        )
        picked[pl.ds(lat_total + half_pairs + index, owners, stride=feature_rows), :] = jnp.where(
            lower, pltpu.roll(even, half_lanes, 1), odd
        )
    send_ref[...] = picked[pl.ds(lat_total, owners * feature_rows), :].astype(send_ref.dtype)


def weights_kernel(
    scale_ref, select_ref, w_in_ref, b_in_ref, w_mid_ref, b_mid_ref, w_out_ref,
    in_ref, mid_ref, out_ref, out_turned_ref, bias_ref, scale_out_ref,
):
    hidden = w_mid_ref.shape[0]
    padded = select_ref.shape[0]
    spare = feature_rows * 3 // 4
    select = select_ref[...]
    bias = jnp.broadcast_to(b_in_ref[...], (padded, hidden))
    high = bias.astype(bf16).astype(f32)
    row = lax.broadcasted_iota(jnp.int32, (padded, hidden), 0)
    spread = matmul(select, w_in_ref[...])
    spread = jnp.where(row == spare, high, jnp.where(row == spare + 1, bias - high, spread))
    in_ref[...] = spread.T.astype(bf16)
    mid_ref[...] = w_mid_ref[...].astype(f32).T.astype(bf16)
    spread_out = matmul(select, w_out_ref[...])
    out_ref[...] = spread_out.astype(bf16)
    out_turned_ref[...] = spread_out.T.astype(bf16)
    bias_ref[...] = jnp.broadcast_to(b_mid_ref[...], (LANES, hidden)).T
    fields, lev_total = scale_ref.shape
    lev_dev = spare // fields
    row = lax.broadcasted_iota(jnp.int32, (padded, LANES), 0)
    scales = jnp.zeros((padded, LANES), f32)
    for field in range(fields):
        for level in range(lev_total):
            place = level // lev_dev * feature_rows + field * lev_dev + level % lev_dev
            scales = jnp.where(row == place, scale_ref[field, level], scales)
    scale_out_ref[...] = scales


def columns_kernel(lev_width, recv_ref, high_ref, low_ref, *rest):
    cot_refs, rest = rest[:lev_width], rest[lev_width:]
    w_in_ref, w_mid_ref, w_turned_ref, w_out_ref, w_out_turned_ref, bias_ref, scale_ref, *rest = rest
    state_refs, rest = rest[:lev_width], rest[lev_width:]
    grads_ref, modes, cot_all, state_all, grad_in, grad_mid, grad_out, grad_bias = rest
    row_share, _, lon_count = cot_refs[0].shape
    lat_width = recv_ref.shape[0] // lev_width
    level = lax.axis_index("lev")
    padded = lev_width * feature_rows
    hidden = w_mid_ref.shape[0]
    spare = feature_rows * 3 // 4
    lower = lower_lanes((padded, LANES))
    for tile in range(lat_width // 2):
        pieces = []
        for owner in (2 * tile, 2 * tile + 1):
            piece = recv_ref[pl.ds(owner * lev_width, lev_width)].astype(f32)
            pieces.append(piece.reshape(padded, LANES))
        first, second = pieces
        lanes = pl.ds(tile * LANES, LANES)
        even = jnp.where(lower, first, pltpu.roll(second, half_lanes, 1))
        odd = jnp.where(lower, pltpu.roll(first, half_lanes, 1), second)
        for share, value in enumerate((even, odd)):
            high, low = split_pair(value)
            modes[share, pl.ds(0, padded), lanes] = high
            if recv_ref.dtype == f32:
                modes[share, pl.ds(padded, padded), lanes] = low
    for shift in range(lev_width):
        source = (level + (lev_width - shift)) % lev_width
        start = pl.multiple_of(source * feature_rows, feature_rows)
        cot_all[:, pl.ds(start, feature_rows), :] = cot_refs[shift][...]
    grad_in[...] = jnp.zeros_like(grad_in)
    grad_mid[...] = jnp.zeros_like(grad_mid)
    grad_out[...] = jnp.zeros_like(grad_out)
    grad_bias[...] = jnp.zeros_like(grad_bias)
    width = 2 * LANES
    while lon_count % width:
        width //= 2
    blocks = lon_count // width

    def visit(block, carried):
        share = block // blocks
        lanes = pl.ds(pl.multiple_of(block % blocks * width, width), width)
        filtered = matmul(modes[share], high_ref[:, lanes])
        if recv_ref.dtype == f32:
            filtered = filtered[:padded] + filtered[padded:]
        filtered += matmul(modes[share, :padded], low_ref[:, lanes])
        row = lax.broadcasted_iota(jnp.int32, (padded, width), 0)
        scaled = filtered * jnp.concatenate([scale_ref[...]] * (width // LANES), axis=1)
        inputs = jnp.where((row == spare) | (row == spare + 1), 1.0, scaled).astype(bf16)
        upstream = cot_all[share, :, lanes]
        pre_in = matmul(w_in_ref[...], inputs)
        gate = 0.5 + 0.5 * jnp.tanh(0.5 * pre_in)
        active = pre_in * gate
        slope_in = gate + active * (1.0 - gate)
        hidden_in = active.astype(bf16)
        bias = jnp.concatenate([bias_ref[...]] * (width // LANES), axis=1)
        pre_mid = matmul(w_mid_ref[...], hidden_in) + bias
        gate = 0.5 + 0.5 * jnp.tanh(0.5 * pre_mid)
        active = pre_mid * gate
        slope_mid = gate + active * (1.0 - gate)
        hidden_mid = active.astype(bf16)
        tendency = matmul(w_out_ref[...], hidden_mid).astype(bf16).astype(f32)
        state_all[share, :, lanes] = (filtered + tendency).astype(state_all.dtype)
        delta = matmul(w_out_turned_ref[...], upstream) * slope_mid
        delta_mid = delta.astype(bf16)
        grad_out[...] += contract_last(upstream, hidden_mid)
        grad_mid[...] += contract_last(delta_mid, hidden_in)
        total = delta[:, :LANES]
        for tile in range(1, width // LANES):
            total = total + delta[:, tile * LANES : (tile + 1) * LANES]
        grad_bias[...] += total
        delta_in = (matmul(w_turned_ref[...], delta_mid) * slope_in).astype(bf16)
        grad_in[...] += contract_last(inputs, delta_in)
        return carried

    lax.fori_loop(0, row_share * blocks, visit, 0)
    for shift in range(lev_width):
        dest = (level + shift) % lev_width
        start = pl.multiple_of(dest * feature_rows, feature_rows)
        state_refs[shift][...] = state_all[:, pl.ds(start, feature_rows), :]
    bias_row = lax.dot_general(
        jnp.ones((8, LANES), f32), grad_bias[...], (((1,), (1,)), ((), ())),
        precision=lax.Precision.HIGHEST, preferred_element_type=f32,
    )[:1]
    row = lax.broadcasted_iota(jnp.int32, (padded, hidden), 0)
    first_rows = jnp.where(row == spare + 1, jnp.broadcast_to(bias_row, (padded, hidden)), grad_in[...])
    total_rows = hidden + 2 * padded
    for tile in range(hidden // LANES):
        lanes = slice(tile * LANES, (tile + 1) * LANES)
        start = tile * total_rows
        grads_ref[pl.ds(start, hidden), :] = grad_mid[:, lanes].astype(grads_ref.dtype)
        grads_ref[pl.ds(start + hidden, padded), :] = first_rows[:, lanes].astype(grads_ref.dtype)
        grads_ref[pl.ds(start + hidden + padded, padded), :] = grad_out[:, lanes].astype(grads_ref.dtype)


def reduce_kernel(grad_scale, recv_ref, out_ref):
    total = jnp.sum(recv_ref[...].astype(f32), axis=0) * grad_scale
    out_ref[...] = jnp.broadcast_to(total.astype(bf16)[None], out_ref.shape)


def state_kernel(*refs):
    *recv_refs, out_ref, scratch = refs
    lev_width = len(recv_refs)
    row_share, _, lon_count = recv_refs[0].shape
    lat_dev = lev_width * row_share
    pairs = out_ref.shape[0] // lat_dev
    tiles = lon_count // LANES
    for shift in range(lev_width):
        source = (lax.axis_index("lev") + (lev_width - shift)) % lev_width
        for share in range(row_share):
            rows = recv_refs[shift][share].astype(f32)[:pairs]
            for tile in range(tiles):
                scratch[tile, pl.ds(source * row_share + share, pairs, stride=lat_dev), :] = rows[
                    :, tile * LANES : (tile + 1) * LANES
                ]
    for tile in range(tiles):
        out_ref[:, pl.ds(tile * LANES, LANES)] = scratch[tile]


def unpack_kernel(packed_ref, select_ref, in_ref, bin_ref, mid_ref, bmid_ref, out_ref):
    hidden = mid_ref.shape[0]
    padded = select_ref.shape[1]
    spare = feature_rows * 3 // 4
    total_rows = hidden + 2 * padded
    select = select_ref[...]
    for tile in range(hidden // LANES):
        lanes = pl.ds(tile * LANES, LANES)
        start = tile * total_rows
        mid_ref[:, lanes] = packed_ref[pl.ds(start, hidden), :].astype(f32)
        rows = packed_ref[pl.ds(start + hidden, padded), :]
        wide = rows.astype(f32)
        bin_ref[:, lanes] = wide[spare : spare + 1]
        bmid_ref[:, lanes] = wide[spare + 1 : spare + 2]
        in_ref[:, lanes] = matmul(select, rows)
        out_ref[:, lanes] = matmul(select, packed_ref[pl.ds(start + hidden + padded, padded), :])


def shaped(shape, kind=f32):
    return jax.ShapeDtypeStruct(shape, kind)


def cost(flops, moved):
    return pl.CostEstimate(flops=flops, transcendentals=0, bytes_accessed=moved)


def rotate(pieces, width):
    moved = [pieces[0]]
    for shift in range(1, width):
        route = [(source, (source + shift) % width) for source in range(width)]
        moved.append(lax.ppermute(pieces[shift], "lev", route))
    return moved


def on_device_fast(
    prognostic, cotangent, damping, in_scale, w_in, b_in, w_mid, b_mid, w_out, wave_order, lat_order
):
    fields, lev_dev, lat_dev, lon_count = prognostic.shape
    lat_width = lax.axis_size("lat")
    lev_width = lax.axis_size("lev")
    wave_total = wave_order.shape[0]
    wave_dev = wave_total // lat_width
    lat_total = lat_order.shape[0]
    pairs = fields * lev_dev
    row_share = lat_dev // lev_width
    hidden, features = w_in.shape
    padded = lev_width * feature_rows
    owners = lat_width * lev_width
    pair_count = wave_dev // 2
    lev_total = lev_dev * lev_width

    select = np.zeros((features, padded), np.float32)
    for field in range(fields):
        for level in range(lev_total):
            place = level // lev_dev * feature_rows + field * lev_dev + level % lev_dev
            select[field * lev_total + level, place] = 1.0
    spread_select = jnp.asarray(select.T, bf16)
    select = jnp.asarray(select, bf16)

    smem = pl.BlockSpec(memory_space=pltpu.SMEM)
    vmem = pl.BlockSpec(memory_space=pltpu.VMEM)
    wave_row = wave_order.reshape(1, wave_total)
    piece = shaped((row_share, feature_rows, lon_count), bf16)
    send, trig_high, trig_low, *cot_pieces = pl.pallas_call(
        forward_kernel,
        in_specs=[smem, vmem, vmem, vmem],
        out_shape=(
            shaped((lat_width, pairs * lat_dev // 2, LANES), forward_type),
            shaped((2 * wave_total, lon_count), bf16),
            shaped((2 * wave_total, lon_count), bf16),
            *([piece] * lev_width),
        ),
        scratch_shapes=[pltpu.VMEM((lon_count // LANES, feature_rows * lat_dev, LANES), f32)],
        name="forward",
    )(
        lat_order,
        wave_row,
        prognostic.reshape(pairs * lat_dev, lon_count),
        cotangent.reshape(pairs * lat_dev, lon_count),
    )
    received = lax.all_to_all(send, "lat", split_axis=0, concat_axis=0, tiled=True)
    upstream = rotate(cot_pieces, lev_width)
    table = pl.pallas_call(
        table_kernel,
        out_shape=shaped((pair_count, TRUNC, 2 * LANES), bf16),
        scratch_shapes=[
            pltpu.VMEM((TRUNC * pair_count, LANES), f32),
            pltpu.VMEM((wave_total, LANES), f32),
        ],
        cost_estimate=cost(8000000, 1 << 20),
        name="legendre",
    )(lat_order.reshape(1, lat_total), wave_row)
    spectral, modes_send = pl.pallas_call(
        spectral_kernel,
        in_specs=[smem, smem, vmem, vmem],
        out_shape=(
            shaped((wave_dev, 2 * pairs, TRUNC)),
            shaped((owners * feature_rows, LANES), inverse_type),
        ),
        scratch_shapes=[
            pltpu.VMEM((2 * pairs * wave_dev, LANES), f32),
            pltpu.VMEM((2 * pairs * wave_dev, LANES), f32),
            pltpu.VMEM((lat_total + owners * feature_rows, LANES), f32),
        ],
        name="spectral",
    )(wave_order, damping, received, table)
    both = ("lat", "lev")
    modes = lax.all_to_all(
        modes_send.reshape(owners, feature_rows, LANES), both, split_axis=0, concat_axis=0, tiled=True
    )
    prepared = pl.pallas_call(
        weights_kernel,
        out_shape=(
            shaped((hidden, padded), bf16),
            shaped((hidden, hidden), bf16),
            shaped((padded, hidden), bf16),
            shaped((hidden, padded), bf16),
            shaped((hidden, LANES)),
            shaped((padded, LANES)),
        ),
        in_specs=[smem] + [vmem] * 6,
        cost_estimate=cost(4000000, 1 << 20),
        name="weights",
    )(
        in_scale, spread_select, w_in.T, b_in.reshape(1, hidden), w_mid, b_mid.reshape(1, hidden), w_out
    )
    spread_in, mid_turned, spread_out, out_turned, bias, scales = prepared
    total_rows = hidden + 2 * padded
    packed_rows = total_rows * (hidden // LANES)
    *state_pieces, grads = pl.pallas_call(
        functools.partial(columns_kernel, lev_width),
        out_shape=(
            *([shaped(piece.shape, state_type)] * lev_width),
            shaped((packed_rows, LANES), grad_type),
        ),
        scratch_shapes=[
            pltpu.VMEM((row_share, padded * (2 if inverse_type == f32 else 1), 2 * wave_total), bf16),
            pltpu.VMEM((row_share, padded, lon_count), bf16),
            pltpu.VMEM((row_share, padded, lon_count), state_type),
            pltpu.VMEM((padded, hidden), f32),
            pltpu.VMEM((hidden, hidden), f32),
            pltpu.VMEM((padded, hidden), f32),
            pltpu.VMEM((hidden, LANES), f32),
        ],
        name="columns",
    )(
        modes, trig_high, trig_low, *upstream,
        spread_in, w_mid, mid_turned, spread_out, out_turned, bias, scales,
    )
    chunk = packed_rows // owners
    parts = lax.all_to_all(
        grads.reshape(owners, chunk, LANES), both, split_axis=0, concat_axis=0, tiled=True
    )
    state = rotate(state_pieces, lev_width)
    grad_scale = 1.0 / math.sqrt(lat_total * lon_count)
    summed = pl.pallas_call(
        functools.partial(reduce_kernel, grad_scale),
        out_shape=shaped((owners, chunk, LANES), bf16),
        name="reduce",
    )(parts)
    gathered = lax.all_to_all(summed, both, split_axis=0, concat_axis=0, tiled=True)
    new_state = pl.pallas_call(
        state_kernel,
        out_shape=shaped((pairs * lat_dev, lon_count)),
        scratch_shapes=[pltpu.VMEM((lon_count // LANES, pairs * lat_dev, LANES), f32)],
        cost_estimate=cost(2000000, 1 << 19),
        name="state",
    )(*state)
    grad_in, grad_bin, grad_mid, grad_bmid, grad_out = pl.pallas_call(
        unpack_kernel,
        out_shape=(
            shaped((features, hidden)),
            shaped((1, hidden)),
            shaped((hidden, hidden)),
            shaped((1, hidden)),
            shaped((features, hidden)),
        ),
        name="unpack",
    )(gathered.reshape(packed_rows, LANES), select)
    return (
        new_state.reshape(fields, lev_dev, lat_dev, lon_count),
        spectral.reshape(wave_dev, 2, fields, lev_dev, TRUNC),
        grad_in.T,
        grad_bin.reshape(hidden),
        grad_mid,
        grad_bmid.reshape(hidden),
        grad_out,
    )


def fits_fast(mesh, prognostic, w_in, wave_order, lat_order):
    lat_width, lev_width = mesh.shape["lat"], mesh.shape["lev"]
    fields, lev_total, lat_total, lon_count = prognostic.shape
    hidden = w_in.shape[0]
    pairs = fields * lev_total // lev_width
    lat_dev = lat_total // lat_width
    wave_dev = wave_order.shape[0] // lat_width
    packed_rows = (hidden + 2 * lev_width * feature_rows) * (hidden // LANES)
    return (
        2 * lat_total == LANES
        and 4 * wave_dev == LANES
        and lat_dev == 8
        and lat_dev == 2 * lev_width
        and pairs == feature_rows * 3 // 4
        and lon_count % LANES == 0
        and hidden % LANES == 0
        and packed_rows % (16 * lat_width * lev_width) == 0
    )


def solution(mesh):
    def run(*arguments):
        prognostic, w_in, wave_order, lat_order = (arguments[at] for at in (0, 4, 9, 10))
        fast = fits_fast(mesh, prognostic, w_in, wave_order, lat_order)
        return shard(mesh, on_device_fast if fast else on_device)(*arguments)

    return run


def shard(mesh, body):
    return jax.shard_map(
        body,
        mesh=mesh,
        in_specs=(
            P(None, "lev", "lat", None),
            P(None, "lev", "lat", None),
            P(None, "lev"),
            P(),
            P(),
            P(),
            P(),
            P(),
            P(),
            P(),
            P(),
        ),
        out_specs=(
            P(None, "lev", "lat", None),
            P("lat", None, None, "lev", None),
            P(),
            P(),
            P(),
            P(),
            P(),
        ),
        check_vma=False,
    )
```

```python
import functools
import math

import jax
import jax.numpy as jnp
import numpy as np
from jax import lax
from jax.experimental import pallas as pl
from jax.experimental.pallas import tpu as pltpu
from jax.sharding import PartitionSpec as P

TRUNC = 256


block_rows = 32
rescale_bits = 40.0


def legendre_setup(own_waves, colatitude):
    float_type = colatitude.dtype
    all_orders = jnp.arange(TRUNC, dtype=jnp.int32)
    factor_index = jnp.arange(1, TRUNC, dtype=jnp.int32).astype(float_type)
    ratios = 0.5 * jnp.log((2.0 * factor_index + 1.0) / (2.0 * factor_index))
    totals = jnp.concatenate([jnp.zeros((1,), float_type), jnp.cumsum(ratios)])
    matches = own_waves[:, None] == all_orders[None, :]
    diagonal_log = jnp.sum(jnp.where(matches, totals[None, :], 0.0), axis=1) - 0.5 * math.log(2.0)
    orders = own_waves.astype(float_type)
    log_shift = diagonal_log[:, None] + orders[:, None] * jnp.log(jnp.sin(colatitude))[None, :]
    empty_rows = jnp.zeros_like(log_shift)
    return (empty_rows, empty_rows, log_shift)


def legendre_rows(recurrence, first_degree, orders, cosine):
    latest, before, log_shift = recurrence
    rescale_limit = 2.0**rescale_bits
    squared_order = orders * orders
    table_rows = []
    for offset in range(block_rows):
        degree = (first_degree + offset).astype(cosine.dtype)
        upper_coef = jnp.sqrt(
            jnp.maximum(4.0 * degree * degree - 1.0, 0.0)
            / jnp.maximum(degree * degree - squared_order, 1.0)
        )
        lower_num = jnp.maximum((degree - 1.0) * (degree - 1.0) - squared_order, 0.0)
        lower_coef = jnp.sqrt(
            lower_num / jnp.maximum(4.0 * (degree - 1.0) * (degree - 1.0) - 1.0, 1.0)
        )
        recurred = upper_coef[:, None] * (cosine[None, :] * latest - lower_coef[:, None] * before)
        diagonal_start = jnp.where(degree == orders, 1.0, 0.0)[:, None] * jnp.ones_like(latest)
        newest = jnp.where((degree > orders)[:, None], recurred, diagonal_start)
        too_large = jnp.abs(newest) > rescale_limit
        factor = jnp.where(too_large, 1.0 / rescale_limit, 1.0)
        newest = newest * factor
        latest = latest * factor
        log_shift = log_shift + jnp.where(too_large, rescale_bits * math.log(2.0), 0.0)
        table_rows.append(newest * jnp.exp(log_shift))
        before = latest
        latest = newest
    return ((latest, before, log_shift), jnp.stack(table_rows, axis=1))


def spectral_pass(own_waves, colatitude, fourier, damping):
    float_type = fourier.dtype
    lat_total = colatitude.shape[0]
    weight = math.pi / lat_total * jnp.sin(colatitude)
    cosine = jnp.cos(colatitude)
    orders = own_waves.astype(float_type)
    weighted = fourier * weight
    degree_norm = 1.0 / (TRUNC * (TRUNC - 1.0))

    def visit_block(carried, first_degree):
        recurrence, grid_sum = carried
        recurrence, legendre_table = legendre_rows(recurrence, first_degree, orders, cosine)
        coeffs = jnp.einsum(
            "jbn,jkfen->jkfeb", legendre_table, weighted, precision=lax.Precision.HIGHEST
        )
        degree = (first_degree + jnp.arange(block_rows, dtype=jnp.int32)).astype(float_type)
        degree_ratio = degree * (degree + 1.0) * degree_norm
        coeffs = coeffs / (1.0 + damping[:, :, None] * (degree_ratio * degree_ratio)[None, None, :])
        grid_sum = grid_sum + jnp.einsum(
            "jbn,jkfeb->jkfen", legendre_table, coeffs, precision=lax.Precision.HIGHEST
        )
        return ((recurrence, grid_sum), coeffs)

    starts = jnp.arange(0, TRUNC, block_rows, dtype=jnp.int32)
    initial = (legendre_setup(own_waves, colatitude), jnp.zeros_like(fourier))
    (recurrence, synthesized), blocks = lax.scan(visit_block, initial, starts)
    waves, two, fields, levels = fourier.shape[:4]
    coeffs = jnp.moveaxis(blocks, 0, 4).reshape(waves, two, fields, levels, TRUNC)
    return (coeffs, synthesized)


def fourier_angles(wave_order, lon_count):
    points = jnp.arange(lon_count, dtype=jnp.int32)
    phase_index = wave_order[:, None] * points[None, :] % lon_count
    return phase_index.astype(jnp.float32) * (2.0 * math.pi / lon_count)


def fourier_forward(wave_order, lon_count):
    angles = fourier_angles(wave_order, lon_count)
    return jnp.stack([jnp.cos(angles), -jnp.sin(angles)], axis=1) / lon_count


def fourier_inverse(wave_order, lon_count):
    angles = fourier_angles(wave_order, lon_count)
    weights = jnp.where(wave_order == 0, 1.0, 2.0)[:, None, None]
    return weights * jnp.stack([jnp.cos(angles), -jnp.sin(angles)], axis=1)


def silu_slope(value):
    sigmoid_value = jax.nn.sigmoid(value)
    return sigmoid_value * (1.0 + value * (1.0 - sigmoid_value))


def column_physics(inputs, upstream, w_in, b_in, w_mid, b_mid, w_out):
    pre_in = jnp.dot(w_in, inputs, preferred_element_type=jnp.float32) + b_in[:, None]
    hidden_in = jax.nn.silu(pre_in).astype(jnp.bfloat16)
    pre_mid = jnp.dot(w_mid, hidden_in, preferred_element_type=jnp.float32) + b_mid[:, None]
    hidden_mid = jax.nn.silu(pre_mid).astype(jnp.bfloat16)
    tendency = jnp.dot(w_out, hidden_mid, preferred_element_type=jnp.float32).astype(jnp.bfloat16)
    grad_out = jnp.dot(upstream, hidden_mid.T, preferred_element_type=jnp.float32)
    back_mid = jnp.dot(w_out.T, upstream, preferred_element_type=jnp.float32)
    delta_mid = (back_mid * silu_slope(pre_mid)).astype(jnp.bfloat16)
    grad_mid = jnp.dot(delta_mid, hidden_in.T, preferred_element_type=jnp.float32)
    grad_bmid = jnp.sum(delta_mid.astype(jnp.float32), axis=1)
    back_in = jnp.dot(w_mid.T, delta_mid, preferred_element_type=jnp.float32)
    delta_in = (back_in * silu_slope(pre_in)).astype(jnp.bfloat16)
    grad_in = jnp.dot(delta_in, inputs.T, preferred_element_type=jnp.float32)
    grad_bin = jnp.sum(delta_in.astype(jnp.float32), axis=1)
    return (tendency, (grad_in, grad_bin, grad_mid, grad_bmid, grad_out))


def physics_rows(inputs, upstream, w_in, b_in, w_mid, b_mid, w_out):
    fields, lev_total, lat_rows, lon_count = inputs.shape
    features = fields * lev_total
    hidden_units = w_in.shape[0]
    rows_in = jnp.moveaxis(inputs.reshape(features, lat_rows, lon_count), 1, 0)
    rows_up = jnp.moveaxis(upstream.reshape(features, lat_rows, lon_count), 1, 0)

    def visit_row(totals, row_pair):
        tendency, gradients = column_physics(
            row_pair[0], row_pair[1], w_in, b_in, w_mid, b_mid, w_out
        )
        return (jax.tree.map(jnp.add, totals, gradients), tendency)

    empty_sums = (
        jnp.zeros((hidden_units, features), jnp.float32),
        jnp.zeros((hidden_units,), jnp.float32),
        jnp.zeros((hidden_units, hidden_units), jnp.float32),
        jnp.zeros((hidden_units,), jnp.float32),
        jnp.zeros((features, hidden_units), jnp.float32),
    )
    totals, tend_rows = lax.scan(visit_row, empty_sums, (rows_in, rows_up))
    tendency = jnp.moveaxis(tend_rows, 0, 1).reshape(fields, lev_total, lat_rows, lon_count)
    return (tendency, totals)


def on_device(
    prognostic, cotangent, damping, in_scale, w_in, b_in, w_mid, b_mid, w_out, wave_order, lat_order
):
    fields, lev_dev, lat_dev, lon_count = prognostic.shape
    lat_width = lax.axis_size("lat")
    wave_dev = wave_order.shape[0] // lat_width
    lat_total = lat_order.shape[0]
    my_index = lax.axis_index("lat")
    own_waves = lax.dynamic_slice_in_dim(wave_order, my_index * wave_dev, wave_dev)
    to_fourier = fourier_forward(wave_order, lon_count)
    fourier = jnp.einsum("jkn,fean->jkfea", to_fourier, prognostic, precision=lax.Precision.HIGHEST)
    fourier = lax.all_to_all(fourier, "lat", split_axis=0, concat_axis=4, tiled=True)
    colatitude = math.pi * (lat_order.astype(jnp.float32) + 0.5) / lat_total
    spectral, synthesized = spectral_pass(own_waves, colatitude, fourier, damping)
    upstream = lax.all_to_all(cotangent, "lev", split_axis=2, concat_axis=1, tiled=True)
    from_fourier = fourier_inverse(wave_order, lon_count)
    row_modes = lax.all_to_all(synthesized, "lat", split_axis=4, concat_axis=0, tiled=True)
    filtered = jnp.einsum(
        "jkfea,jkn->fean", row_modes, from_fourier, precision=lax.Precision.HIGHEST
    )
    lev_index = lax.axis_index("lev")
    local_scale = lax.dynamic_slice_in_dim(in_scale, lev_index * lev_dev, lev_dev, 1)
    local_inputs = (filtered * local_scale[:, :, None, None]).astype(jnp.bfloat16)
    inputs = lax.all_to_all(local_inputs, "lev", split_axis=2, concat_axis=1, tiled=True)
    tend_cols, totals = physics_rows(inputs, upstream, w_in, b_in, w_mid, b_mid, w_out)
    tendency = lax.all_to_all(tend_cols, "lev", split_axis=1, concat_axis=2, tiled=True)
    new_state = filtered + tendency.astype(jnp.float32)
    grad_scale = 1.0 / math.sqrt(lat_total * lon_count)
    summed = lax.psum(
        (
            totals[0] * grad_scale,
            totals[1] * grad_scale,
            totals[2] * grad_scale,
            totals[3] * grad_scale,
            totals[4] * grad_scale,
        ),
        ("lat", "lev"),
    )
    return (new_state, spectral, summed[0], summed[1], summed[2], summed[3], summed[4])


LANES = 128
half_lanes = LANES // 2
feature_rows = 16
bf16 = jnp.bfloat16
f32 = jnp.float32
forward_type = f32
inverse_type = f32
state_type = bf16
grad_type = bf16
row_gap = 8


def contract_last(left, right):
    return lax.dot_general(left, right, (((1,), (1,)), ((), ())), preferred_element_type=f32)


def matmul(left, right):
    return lax.dot_general(left, right, (((1,), (0,)), ((), ())), preferred_element_type=f32)


def half_turn_sincos(half_angle):
    square = half_angle * half_angle
    sine = 0.0
    cosine = 0.0
    for power in range(6, -1, -1):
        sine = sine * square + (-1.0) ** power / math.factorial(2 * power + 1)
        cosine = cosine * square + (-1.0) ** power / math.factorial(2 * power)
    sine = sine * half_angle
    return 2.0 * sine * cosine, 1.0 - 2.0 * sine * sine


def turn_sincos(product, period):
    reduced = product - period * jnp.floor(product * (1.0 / period) + 0.5)
    return half_turn_sincos(reduced * (math.pi / period))


def lower_lanes(shape):
    return lax.broadcasted_iota(jnp.int32, shape, len(shape) - 1) < half_lanes


def split_pair(value):
    high = value.astype(bf16)
    return high, (value - high.astype(f32)).astype(bf16)


def polar_sine(lat_index, lat_total):
    nearest = jnp.minimum(lat_index, (lat_total - 1.0) - lat_index)
    return half_turn_sincos((nearest + 0.5) * (0.5 * math.pi / lat_total))


def wave_columns(waves_ref):
    return jnp.broadcast_to(waves_ref[...].astype(f32), (LANES, waves_ref.shape[1])).T


def forward_kernel(
    lats_ref, waves_ref, prog_ref, cot_ref, send_ref, high_ref, low_ref, *rest
):
    *cot_refs, cot_scratch = rest
    lat_width, half_rows, _ = send_ref.shape
    wave_total = waves_ref.shape[1]
    wave_dev = wave_total // lat_width
    rows_total, lon_count = prog_ref.shape
    lat_total = lats_ref.shape[0]
    lat_dev = lat_total // lat_width
    waves = wave_columns(waves_ref)
    lane = lax.broadcasted_iota(jnp.int32, waves.shape, 1).astype(f32)
    sine, cosine = turn_sincos(waves * lane, float(lon_count))
    step_sine, step_cosine = turn_sincos(waves * float(LANES), float(lon_count))
    for tile in range(lon_count // LANES):
        lanes = pl.ds(tile * LANES, LANES)
        cosines = split_pair(cosine)
        sines = split_pair(-sine)
        for owner in range(lat_width):
            rows = slice(owner * wave_dev, (owner + 1) * wave_dev)
            for ref, cosine_part, sine_part in zip((high_ref, low_ref), cosines, sines):
                ref[pl.ds(2 * owner * wave_dev, wave_dev), lanes] = cosine_part[rows]
                ref[pl.ds((2 * owner + 1) * wave_dev, wave_dev), lanes] = sine_part[rows]
        cosine, sine = (
            cosine * step_cosine - sine * step_sine,
            sine * step_cosine + cosine * step_sine,
        )
    prog_high, prog_low = split_pair(prog_ref[...])
    modes = contract_last(jnp.concatenate([prog_high, prog_low], axis=0), high_ref[...])
    modes = modes[:rows_total] + modes[rows_total:] + contract_last(prog_high, low_ref[...])
    first_row = lax.axis_index("lat") * lat_dev
    row = lax.broadcasted_iota(jnp.int32, (lat_dev, LANES), 0)
    lat_index = jnp.zeros((lat_dev, LANES), f32)
    for at in range(lat_dev):
        lat_index = jnp.where(row == at, lats_ref[first_row + at].astype(f32), lat_index)
    weight = polar_sine(lat_index, lat_total)[0] * (math.pi / lat_total / lon_count)
    weight = jnp.concatenate([weight] * (half_rows // lat_dev), axis=0)
    lower = lower_lanes((half_rows, LANES))
    for tile in range(lat_width // 2):
        first = modes[:half_rows, tile * LANES : (tile + 1) * LANES] * weight
        second = modes[half_rows:, tile * LANES : (tile + 1) * LANES] * weight
        send_ref[2 * tile] = jnp.where(lower, first, pltpu.roll(second, half_lanes, 1)).astype(send_ref.dtype)
        send_ref[2 * tile + 1] = jnp.where(
            lower, pltpu.roll(first, half_lanes, 1), second
        ).astype(send_ref.dtype)
    lev_width = len(cot_refs)
    row_share = lat_dev // lev_width
    cot_scratch[...] = jnp.zeros_like(cot_scratch)
    cot_all = cot_ref[...].astype(f32)
    tiles = lon_count // LANES
    for tile in range(tiles):
        cot_scratch[tile, pl.ds(0, rows_total), :] = cot_all[:, tile * LANES : (tile + 1) * LANES]
    for shift in range(lev_width):
        dest = (lax.axis_index("lev") + shift) % lev_width
        for share in range(row_share):
            for tile in range(tiles):
                picked = cot_scratch[tile, pl.ds(dest * row_share + share, feature_rows, stride=lat_dev), :]
                cot_refs[shift][share, :, pl.ds(tile * LANES, LANES)] = picked.astype(bf16)


def table_kernel(lats_ref, waves_ref, out_ref, scratch, columns):
    pair_count, degrees, _ = out_ref.shape
    rows = pair_count
    lat_total = lats_ref.shape[1]
    columns[...] = wave_columns(waves_ref)
    first_wave = pl.multiple_of(lax.axis_index("lat") * 2 * rows, 2 * rows)
    orders = jnp.where(
        lower_lanes((rows, LANES)),
        columns[pl.ds(first_wave, rows), :],
        columns[pl.ds(first_wave + rows, rows), :],
    )
    lat_row = lats_ref[...].astype(f32)
    lat_index = jnp.broadcast_to(jnp.concatenate([lat_row, lat_row], axis=1), (rows, LANES))
    sine, cosine = polar_sine(lat_index, lat_total)
    cosine = jnp.where(2.0 * lat_index < lat_total - 1.0, cosine, -cosine)
    index = lax.broadcasted_iota(jnp.int32, (rows, degrees), 1).astype(f32)
    index = jnp.maximum(index, 1.0)
    ratios = 0.5 * jnp.log((2.0 * index + 1.0) / (2.0 * index))
    position = lax.broadcasted_iota(jnp.int32, (rows, degrees), 1)
    counted = position.astype(f32)
    totals = []
    for half in range(2):
        wave = jnp.broadcast_to(orders[:, half * half_lanes : half * half_lanes + 1], (rows, degrees))
        chosen = jnp.where((position > 0) & (counted <= wave), ratios, 0.0)
        totals.append(jnp.broadcast_to(jnp.sum(chosen, axis=1, keepdims=True), (rows, LANES)))
    diagonal_log = jnp.where(lower_lanes((rows, LANES)), totals[0], totals[1])
    log_shift = (
        diagonal_log
        - 0.5 * math.log(2.0)
        - 0.5 * jnp.log(2.0 * orders + 1.0)
        + orders * jnp.log(sine)
    )
    squared = orders * orders
    limit = 2.0**rescale_bits
    zero = jnp.zeros((rows, LANES), f32)

    def visit(block, carried):
        latest, before, previous_root, log_shift = carried
        scale = jnp.exp(log_shift)
        for offset in range(8):
            degree_int = block * 8 + offset
            degree = jnp.full((rows, LANES), degree_int, jnp.int32).astype(f32)
            gap = degree * degree - squared
            inverse_root = lax.rsqrt(jnp.maximum(gap, 1.0))
            root = gap * inverse_root
            recurred = inverse_root * (
                (2.0 * degree - 1.0) * cosine * latest - previous_root * before
            )
            newest = jnp.where(gap > 0.0, recurred, jnp.where(gap == 0.0, 1.0, 0.0))
            scratch[pl.ds(degree_int * (rows + row_gap), rows), :] = newest * scale
            before = latest
            latest = newest
            previous_root = jnp.maximum(root, 0.0)
        too_large = jnp.abs(latest) > limit
        factor = jnp.where(too_large, 1.0 / limit, 1.0)
        log_shift = log_shift + jnp.where(too_large, rescale_bits * math.log(2.0), 0.0)
        return latest * factor, before * factor, previous_root, log_shift

    lax.fori_loop(0, degrees // 8, visit, (zero, zero, zero, log_shift))

    def unpack(pair, carried):
        high, low = split_pair(scratch[pl.ds(pair, degrees, stride=rows + row_gap), :])
        out_ref[pair, :, pl.ds(0, LANES)] = high
        out_ref[pair, :, pl.ds(LANES, LANES)] = low
        return carried

    lax.fori_loop(0, pair_count, unpack, 0)


def spectral_kernel(
    waves_ref, damping_ref, recv_ref, table_ref, spec_ref, send_ref, modes, sums, picked
):
    pair_count, degrees, _ = table_ref.shape
    wave_dev = 2 * pair_count
    lat_width, half_rows, _ = recv_ref.shape
    lat_total = LANES // 2
    lat_dev = lat_total // lat_width
    fields, lev_dev = damping_ref.shape
    pairs = fields * lev_dev
    half_pairs = pairs // 2
    first_wave = lax.axis_index("lat") * wave_dev
    pitch = wave_dev + row_gap
    received = recv_ref[...].astype(f32)
    upper_rows = lax.broadcasted_iota(jnp.int32, (LANES, LANES), 0) % wave_dev >= pair_count
    for index in range(half_pairs):
        stacked = [
            received[source, index * lat_dev : (index + 1) * lat_dev] for source in range(lat_width)
        ]
        stacked.append(jnp.zeros((LANES - lat_total, LANES), f32))
        turned = jnp.concatenate(stacked, axis=0).T
        turned = jnp.where(upper_rows, pltpu.roll(turned, half_lanes, 1), turned)
        for half in range(2):
            for part in range(2):
                start = (half * 2 + part) * wave_dev
                place = (part * pairs + half * half_pairs + index) * pitch
                modes[pl.ds(place, wave_dev), :] = turned[start : start + wave_dev]
    degree = lax.broadcasted_iota(jnp.int32, (pairs, degrees), 1).astype(f32)
    degree_ratio = degree * (degree + 1.0) * (1.0 / (degrees * (degrees - 1.0)))
    root = jnp.sqrt(2.0 * degree + 1.0)
    row = lax.broadcasted_iota(jnp.int32, (pairs, degrees), 0)
    strength = jnp.zeros((pairs, degrees), f32)
    for pair in range(pairs):
        strength = jnp.where(row == pair, damping_ref[pair // lev_dev, pair % lev_dev], strength)
    damp = root / (1.0 + strength * (degree_ratio * degree_ratio))
    damp = jnp.concatenate([damp, damp, damp, damp], axis=0)
    root_row = root[:1]
    count = 2 * pairs
    for pair in range(pair_count):
        first = modes[pl.ds(pair, count, stride=pitch), :]
        second = modes[pl.ds(pair + pair_count, count, stride=pitch), :]
        stacked = jnp.concatenate([first, second], axis=0)
        table = table_ref[pair]
        if recv_ref.dtype == f32:
            stacked = jnp.concatenate(split_pair(stacked), axis=0)
        else:
            stacked = stacked.astype(bf16)
        coeffs = contract_last(jnp.concatenate([stacked, stacked], axis=1), table)
        if recv_ref.dtype == f32:
            coeffs = coeffs[: 2 * count] + coeffs[2 * count :]
        coeffs = coeffs * damp
        spec_ref[pair] = coeffs[:count]
        spec_ref[pair + pair_count] = coeffs[count:]
        first_weight = jnp.where(waves_ref[first_wave + pair] == 0, 1.0, 2.0)
        second_weight = jnp.where(waves_ref[first_wave + pair + pair_count] == 0, 1.0, 2.0)
        rooted = jnp.concatenate(
            [coeffs[:count] * (root_row * first_weight), coeffs[count:] * (root_row * second_weight)],
            axis=0,
        )
        synth = matmul(jnp.concatenate(split_pair(rooted), axis=0), table)
        synth = synth[: 2 * count] + synth[2 * count :]
        synth = synth[:, :LANES] + synth[:, LANES:]
        sums[pl.ds(pair, count, stride=pitch), :] = synth[:count]
        sums[pl.ds(pair + pair_count, count, stride=pitch), :] = synth[count:]
    owners = send_ref.shape[0] // feature_rows
    lower = lower_lanes((owners, LANES))
    share = lat_total // owners
    blank = jnp.zeros((owners, LANES), f32)
    for row in range(pairs, feature_rows):
        picked[pl.ds(lat_total + row, owners, stride=feature_rows), :] = blank
    for index in range(half_pairs):
        blocks = []
        for half in range(2):
            for part in range(2):
                place = (part * pairs + half * half_pairs + index) * pitch
                blocks.append(sums[pl.ds(place, wave_dev), :])
        stacked = jnp.concatenate(blocks, axis=0)
        stacked = jnp.where(upper_rows, pltpu.roll(stacked, half_lanes, 1), stacked)
        picked[pl.ds(0, lat_total), :] = stacked.T[:lat_total]
        even = picked[pl.ds(0, owners, stride=share), :]
        odd = picked[pl.ds(1, owners, stride=share), :]
        picked[pl.ds(lat_total + index, owners, stride=feature_rows), :] = jnp.where(
            lower, even, pltpu.roll(odd, half_lanes, 1)
        )
        picked[pl.ds(lat_total + half_pairs + index, owners, stride=feature_rows), :] = jnp.where(
            lower, pltpu.roll(even, half_lanes, 1), odd
        )
    send_ref[...] = picked[pl.ds(lat_total, owners * feature_rows), :].astype(send_ref.dtype)


def weights_kernel(
    scale_ref, select_ref, w_in_ref, b_in_ref, w_mid_ref, b_mid_ref, w_out_ref,
    in_ref, mid_ref, out_ref, out_turned_ref, bias_ref, scale_out_ref,
):
    hidden = w_mid_ref.shape[0]
    padded = select_ref.shape[0]
    spare = feature_rows * 3 // 4
    select = select_ref[...]
    bias = jnp.broadcast_to(b_in_ref[...], (padded, hidden))
    high = bias.astype(bf16).astype(f32)
    row = lax.broadcasted_iota(jnp.int32, (padded, hidden), 0)
    spread = matmul(select, w_in_ref[...])
    spread = jnp.where(row == spare, high, jnp.where(row == spare + 1, bias - high, spread))
    in_ref[...] = spread.T.astype(bf16)
    mid_ref[...] = w_mid_ref[...].astype(f32).T.astype(bf16)
    spread_out = matmul(select, w_out_ref[...])
    out_ref[...] = spread_out.astype(bf16)
    out_turned_ref[...] = spread_out.T.astype(bf16)
    bias_ref[...] = jnp.broadcast_to(b_mid_ref[...], (LANES, hidden)).T
    fields, lev_total = scale_ref.shape
    lev_dev = spare // fields
    row = lax.broadcasted_iota(jnp.int32, (padded, LANES), 0)
    scales = jnp.zeros((padded, LANES), f32)
    for field in range(fields):
        for level in range(lev_total):
            place = level // lev_dev * feature_rows + field * lev_dev + level % lev_dev
            scales = jnp.where(row == place, scale_ref[field, level], scales)
    scale_out_ref[...] = scales


def columns_kernel(lev_width, recv_ref, high_ref, low_ref, *rest):
    cot_refs, rest = rest[:lev_width], rest[lev_width:]
    w_in_ref, w_mid_ref, w_turned_ref, w_out_ref, w_out_turned_ref, bias_ref, scale_ref, *rest = rest
    state_refs, rest = rest[:lev_width], rest[lev_width:]
    keep_ref, give_ref, packed, modes, cot_all, state_all, grad_in, grad_mid, grad_out, grad_bias = rest
    row_share, _, lon_count = cot_refs[0].shape
    lat_width = recv_ref.shape[0] // lev_width
    level = lax.axis_index("lev")
    padded = lev_width * feature_rows
    hidden = w_mid_ref.shape[0]
    spare = feature_rows * 3 // 4
    lower = lower_lanes((padded, LANES))
    for tile in range(lat_width // 2):
        pieces = []
        for owner in (2 * tile, 2 * tile + 1):
            piece = recv_ref[pl.ds(owner * lev_width, lev_width)].astype(f32)
            pieces.append(piece.reshape(padded, LANES))
        first, second = pieces
        lanes = pl.ds(tile * LANES, LANES)
        even = jnp.where(lower, first, pltpu.roll(second, half_lanes, 1))
        odd = jnp.where(lower, pltpu.roll(first, half_lanes, 1), second)
        for share, value in enumerate((even, odd)):
            high, low = split_pair(value)
            modes[share, pl.ds(0, padded), lanes] = high
            if recv_ref.dtype == f32:
                modes[share, pl.ds(padded, padded), lanes] = low
    for shift in range(lev_width):
        source = (level + (lev_width - shift)) % lev_width
        start = pl.multiple_of(source * feature_rows, feature_rows)
        cot_all[:, pl.ds(start, feature_rows), :] = cot_refs[shift][...]
    grad_in[...] = jnp.zeros_like(grad_in)
    grad_mid[...] = jnp.zeros_like(grad_mid)
    grad_out[...] = jnp.zeros_like(grad_out)
    grad_bias[...] = jnp.zeros_like(grad_bias)
    width = 6 * LANES
    while lon_count % width:
        width //= 2
    blocks = lon_count // width

    def visit(block, carried):
        share = block // blocks
        lanes = pl.ds(pl.multiple_of(block % blocks * width, width), width)
        filtered = matmul(modes[share], high_ref[:, lanes])
        if recv_ref.dtype == f32:
            filtered = filtered[:padded] + filtered[padded:]
        filtered += matmul(modes[share, :padded], low_ref[:, lanes])
        row = lax.broadcasted_iota(jnp.int32, (padded, width), 0)
        scaled = filtered * jnp.concatenate([scale_ref[...]] * (width // LANES), axis=1)
        inputs = jnp.where((row == spare) | (row == spare + 1), 1.0, scaled).astype(bf16)
        upstream = cot_all[share, :, lanes]
        pre_in = matmul(w_in_ref[...], inputs)
        gate = 0.5 + 0.5 * jnp.tanh(0.5 * pre_in)
        active = pre_in * gate
        slope_in = gate + active * (1.0 - gate)
        hidden_in = active.astype(bf16)
        bias = jnp.concatenate([bias_ref[...]] * (width // LANES), axis=1)
        pre_mid = matmul(w_mid_ref[...], hidden_in) + bias
        gate = 0.5 + 0.5 * jnp.tanh(0.5 * pre_mid)
        active = pre_mid * gate
        slope_mid = gate + active * (1.0 - gate)
        hidden_mid = active.astype(bf16)
        tendency = matmul(w_out_ref[...], hidden_mid).astype(bf16).astype(f32)
        state_all[share, :, lanes] = (filtered + tendency).astype(state_all.dtype)
        delta = matmul(w_out_turned_ref[...], upstream) * slope_mid
        delta_mid = delta.astype(bf16)
        grad_out[...] += contract_last(upstream, hidden_mid)
        grad_mid[...] += contract_last(delta_mid, hidden_in)
        total = delta[:, :LANES]
        for tile in range(1, width // LANES):
            total = total + delta[:, tile * LANES : (tile + 1) * LANES]
        grad_bias[...] += total
        delta_in = (matmul(w_turned_ref[...], delta_mid) * slope_in).astype(bf16)
        grad_in[...] += contract_last(inputs, delta_in)
        return carried

    lax.fori_loop(0, row_share * blocks, visit, 0)
    for shift in range(lev_width):
        dest = (level + shift) % lev_width
        start = pl.multiple_of(dest * feature_rows, feature_rows)
        for share in range(row_share):
            for tile in range(lon_count // LANES):
                place = (share * (lon_count // LANES) + tile) * feature_rows
                state_refs[shift][pl.ds(place, feature_rows), :] = state_all[
                    share, pl.ds(start, feature_rows), pl.ds(tile * LANES, LANES)
                ]
    bias_row = lax.dot_general(
        jnp.ones((8, LANES), f32), grad_bias[...], (((1,), (1,)), ((), ())),
        precision=lax.Precision.HIGHEST, preferred_element_type=f32,
    )[:1]
    row = lax.broadcasted_iota(jnp.int32, (padded, hidden), 0)
    first_rows = jnp.where(row == spare + 1, jnp.broadcast_to(bias_row, (padded, hidden)), grad_in[...])
    total_rows = hidden + 2 * padded
    for tile in range(hidden // LANES):
        lanes = slice(tile * LANES, (tile + 1) * LANES)
        start = tile * total_rows
        packed[pl.ds(start, hidden), :] = grad_mid[:, lanes]
        packed[pl.ds(start + hidden, padded), :] = first_rows[:, lanes]
        packed[pl.ds(start + hidden + padded, padded), :] = grad_out[:, lanes]
    half_rows = packed.shape[0] // 2
    side = lax.axis_index("lat") % 2
    keep_ref[...] = packed[pl.ds(pl.multiple_of(side * half_rows, 16), half_rows), :]
    give_ref[...] = packed[pl.ds(pl.multiple_of((1 - side) * half_rows, 16), half_rows), :].astype(
        give_ref.dtype
    )


def part_rows(index, ref):
    count = ref.shape[0]
    return pl.ds(pl.multiple_of(index * count, 16), count)


def plane_scatter_kernel(keep_ref, recv_ref, rest_ref, *send_refs):
    chip = lax.axis_index("lat") // 2
    for offset, ref in enumerate((rest_ref, *send_refs)):
        rows = part_rows(chip ^ offset, ref)
        ref[...] = (keep_ref[rows, :] + recv_ref[rows, :].astype(f32)).astype(ref.dtype)


def column_scatter_kernel(width, keep_ref, *rest):
    recv_refs, rest = rest[: len(rest) - 2 * width + 1], rest[len(rest) - 2 * width + 1 :]
    state_refs, rest_ref, send_refs = rest[: width - 1], rest[width - 1], rest[width:]
    chunk = rest_ref.shape[0]
    level = lax.axis_index("lev")
    for shift in range(width):
        rows = part_rows((level + shift) % width, rest_ref)
        total = keep_ref[rows, :]
        for ref in recv_refs:
            total = total + ref[rows, :].astype(f32)
        if shift == 0:
            rest_ref[...] = total
        else:
            send_refs[shift - 1][pl.ds(0, chunk), :] = total.astype(bf16)
            send_refs[shift - 1][pl.ds(chunk, state_refs[0].shape[0]), :] = state_refs[shift - 1][...]


def reduce_kernel(grad_scale, keep_ref, *rest):
    *recv_refs, out_ref = rest
    total = keep_ref[...]
    for ref in recv_refs:
        total = total + ref[pl.ds(0, keep_ref.shape[0]), :].astype(f32)
    out_ref[...] = (total * grad_scale).astype(bf16)


def column_gather_kernel(*refs):
    *part_refs, out_ref = refs
    width = len(part_refs)
    level = lax.axis_index("lev")
    for shift, ref in enumerate(part_refs):
        out_ref[part_rows((level + (width - shift)) % width, ref), :] = ref[...]


def plane_gather_kernel(*refs):
    *part_refs, out_ref = refs
    chip = lax.axis_index("lat") // 2
    for offset, ref in enumerate(part_refs):
        out_ref[part_rows(chip ^ offset, ref), :] = ref[...]


def state_kernel(row_share, *refs):
    *recv_refs, out_ref, scratch = refs
    lev_width = len(recv_refs)
    lat_dev = lev_width * row_share
    pairs = out_ref.shape[0] // lat_dev
    tiles = out_ref.shape[1] // LANES
    for shift, ref in enumerate(recv_refs):
        source = (lax.axis_index("lev") + (lev_width - shift)) % lev_width
        first = ref.shape[0] - row_share * tiles * feature_rows
        for share in range(row_share):
            for tile in range(tiles):
                place = first + (share * tiles + tile) * feature_rows
                rows = ref[pl.ds(place, feature_rows), :].astype(f32)[:pairs]
                scratch[tile, pl.ds(source * row_share + share, pairs, stride=lat_dev), :] = rows
    for tile in range(tiles):
        out_ref[:, pl.ds(tile * LANES, LANES)] = scratch[tile]


def unpack_kernel(own_ref, other_ref, select_ref, in_ref, bin_ref, mid_ref, bmid_ref, out_ref):
    hidden = mid_ref.shape[0]
    padded = select_ref.shape[1]
    spare = feature_rows * 3 // 4
    total_rows = hidden + 2 * padded
    select = select_ref[...]
    side = lax.axis_index("lat") % 2
    half_tiles = own_ref.shape[0] // total_rows
    for ref, half in ((own_ref, side), (other_ref, 1 - side)):
        for tile in range(half_tiles):
            lanes = pl.ds(pl.multiple_of((half * half_tiles + tile) * LANES, LANES), LANES)
            start = tile * total_rows
            mid_ref[:, lanes] = ref[pl.ds(start, hidden), :].astype(f32)
            rows = ref[pl.ds(start + hidden, padded), :]
            wide = rows.astype(f32)
            bin_ref[:, lanes] = wide[spare : spare + 1]
            bmid_ref[:, lanes] = wide[spare + 1 : spare + 2]
            in_ref[:, lanes] = matmul(select, rows)
            out_ref[:, lanes] = matmul(select, ref[pl.ds(start + hidden + padded, padded), :])


def shaped(shape, kind=f32):
    return jax.ShapeDtypeStruct(shape, kind)


def room(mib):
    return pltpu.CompilerParams(vmem_limit_bytes=mib << 20)


def kept(shape, kind=f32):
    return pltpu.VMEM(shape, kind)


def near(array):
    return pltpu.with_memory_space_constraint(array, pltpu.VMEM)


def far(array):
    return pltpu.with_memory_space_constraint(array, pltpu.HBM)


def cost(flops, moved):
    return pl.CostEstimate(flops=flops, transcendentals=0, bytes_accessed=moved)


def rotate(pieces, width):
    moved = [pieces[0]]
    for shift in range(1, width):
        route = [(source, (source + shift) % width) for source in range(width)]
        moved.append(lax.ppermute(pieces[shift], "lev", route))
    return moved


def on_device_fast(
    prognostic, cotangent, damping, in_scale, w_in, b_in, w_mid, b_mid, w_out, wave_order, lat_order
):
    fields, lev_dev, lat_dev, lon_count = prognostic.shape
    lat_width = lax.axis_size("lat")
    lev_width = lax.axis_size("lev")
    wave_total = wave_order.shape[0]
    wave_dev = wave_total // lat_width
    lat_total = lat_order.shape[0]
    pairs = fields * lev_dev
    row_share = lat_dev // lev_width
    hidden, features = w_in.shape
    padded = lev_width * feature_rows
    owners = lat_width * lev_width
    pair_count = wave_dev // 2
    lev_total = lev_dev * lev_width

    select = np.zeros((features, padded), np.float32)
    for field in range(fields):
        for level in range(lev_total):
            place = level // lev_dev * feature_rows + field * lev_dev + level % lev_dev
            select[field * lev_total + level, place] = 1.0
    spread_select = jnp.asarray(select.T, bf16)
    select = jnp.asarray(select, bf16)

    smem = pl.BlockSpec(memory_space=pltpu.SMEM)
    vmem = pl.BlockSpec(memory_space=pltpu.VMEM)
    wave_row = wave_order.reshape(1, wave_total)
    piece = (row_share, feature_rows, lon_count)
    send, trig_high, trig_low, *cot_pieces = pl.pallas_call(
        forward_kernel,
        in_specs=[smem, vmem, vmem, vmem],
        out_shape=(
            kept((lat_width, pairs * lat_dev // 2, LANES), forward_type),
            kept((2 * wave_total, lon_count), bf16),
            kept((2 * wave_total, lon_count), bf16),
            *([kept(piece, bf16)] * lev_width),
        ),
        scratch_shapes=[pltpu.VMEM((lon_count // LANES, feature_rows * lat_dev, LANES), f32)],
        compiler_params=room(16),
        name="forward",
    )(
        lat_order,
        far(wave_row),
        far(prognostic.reshape(pairs * lat_dev, lon_count)),
        far(cotangent.reshape(pairs * lat_dev, lon_count)),
    )
    received = lax.all_to_all(send, "lat", split_axis=0, concat_axis=0, tiled=True)
    upstream = rotate(cot_pieces, lev_width)
    table = pl.pallas_call(
        table_kernel,
        out_shape=kept((pair_count, TRUNC, 2 * LANES), bf16),
        scratch_shapes=[
            pltpu.VMEM((TRUNC * (pair_count + row_gap), LANES), f32),
            pltpu.VMEM((wave_total, LANES), f32),
        ],
        cost_estimate=cost(8000000, 1 << 20),
        compiler_params=room(16),
        name="legendre",
    )(far(lat_order.reshape(1, lat_total)), far(wave_row))
    spectral, modes_send = pl.pallas_call(
        spectral_kernel,
        in_specs=[smem, smem, vmem, vmem],
        out_shape=(
            pltpu.HBM((wave_dev, 2 * pairs, TRUNC), f32),
            kept((owners * feature_rows, LANES), inverse_type),
        ),
        scratch_shapes=[
            pltpu.VMEM((2 * pairs * (wave_dev + row_gap), LANES), f32),
            pltpu.VMEM((2 * pairs * (wave_dev + row_gap), LANES), f32),
            pltpu.VMEM((lat_total + owners * feature_rows, LANES), f32),
        ],
        compiler_params=room(16),
        name="spectral",
    )(wave_order, damping, near(received), near(table))
    both = ("lat", "lev")
    modes = lax.all_to_all(
        modes_send.reshape(owners, feature_rows, LANES), both, split_axis=0, concat_axis=0, tiled=True
    )
    prepared = pl.pallas_call(
        weights_kernel,
        out_shape=(
            kept((hidden, padded), bf16),
            kept((hidden, hidden), bf16),
            kept((padded, hidden), bf16),
            kept((hidden, padded), bf16),
            kept((hidden, LANES)),
            kept((padded, LANES)),
        ),
        in_specs=[smem] + [vmem] * 6,
        cost_estimate=cost(4000000, 1 << 20),
        compiler_params=room(12),
        name="weights",
    )(
        in_scale,
        far(spread_select),
        far(w_in.T),
        far(b_in.reshape(1, hidden)),
        far(w_mid),
        far(b_mid.reshape(1, hidden)),
        far(w_out),
    )
    spread_in, mid_turned, spread_out, out_turned, bias, scales = prepared
    total_rows = hidden + 2 * padded
    packed_rows = total_rows * (hidden // LANES)
    state_rows = row_share * feature_rows * (lon_count // LANES)
    *state_pieces, keep, give = pl.pallas_call(
        functools.partial(columns_kernel, lev_width),
        out_shape=(
            *([kept((state_rows, LANES), state_type)] * lev_width),
            kept((packed_rows // 2, LANES)),
            kept((packed_rows // 2, LANES), grad_type),
        ),
        scratch_shapes=[
            pltpu.VMEM((packed_rows, LANES), f32),
            pltpu.VMEM((row_share, padded * (2 if inverse_type == f32 else 1), 2 * wave_total), bf16),
            pltpu.VMEM((row_share, padded, lon_count), bf16),
            pltpu.VMEM((row_share, padded, lon_count), state_type),
            pltpu.VMEM((padded, hidden), f32),
            pltpu.VMEM((hidden, hidden), f32),
            pltpu.VMEM((padded, hidden), f32),
            pltpu.VMEM((hidden, LANES), f32),
        ],
        compiler_params=room(24),
        name="columns",
    )(
        *map(near, (modes, trig_high, trig_low, *upstream, spread_in)),
        far(w_mid),
        *map(near, (mid_turned, spread_out, out_turned, bias, scales)),
    )
    chips = lat_width // 2
    quarter = packed_rows // lat_width
    chunk = packed_rows // owners
    partner = [(at, at ^ 1) for at in range(lat_width)]
    routes = [[(at, at ^ (2 * offset)) for at in range(lat_width)] for offset in range(1, chips)]
    taken = lax.ppermute(give, "lat", partner)
    rest, *sends = pl.pallas_call(
        plane_scatter_kernel,
        out_shape=(
            kept((quarter, LANES)),
            *([kept((quarter, LANES), grad_type)] * (chips - 1)),
        ),
        compiler_params=room(8),
        name="plane_scatter",
    )(near(keep), near(taken))
    taken = [lax.ppermute(send, "lat", route) for send, route in zip(sends, routes)]
    rest, *sends = pl.pallas_call(
        functools.partial(column_scatter_kernel, lev_width),
        out_shape=(
            kept((chunk, LANES)),
            *([kept((chunk + state_rows, LANES), grad_type)] * (lev_width - 1)),
        ),
        compiler_params=room(8),
        name="column_scatter",
    )(*map(near, (rest, *taken, *state_pieces[1:])))
    _, *taken = rotate([None, *sends], lev_width)
    grad_scale = 1.0 / math.sqrt(lat_total * lon_count)
    own_part = pl.pallas_call(
        functools.partial(reduce_kernel, grad_scale),
        out_shape=kept((chunk, LANES), grad_type),
        compiler_params=room(8),
        name="reduce",
    )(*map(near, (rest, *taken)))
    new_state = pl.pallas_call(
        functools.partial(state_kernel, row_share),
        out_shape=shaped((pairs * lat_dev, lon_count)),
        scratch_shapes=[pltpu.VMEM((lon_count // LANES, pairs * lat_dev, LANES), f32)],
        cost_estimate=cost(2000000, 1 << 19),
        compiler_params=room(8),
        name="state",
    )(*map(near, (state_pieces[0], *taken)))
    parts = rotate([own_part] * lev_width, lev_width)
    joined = pl.pallas_call(
        column_gather_kernel,
        out_shape=kept((quarter, LANES), grad_type),
        compiler_params=room(8),
        name="column_gather",
    )(*map(near, parts))
    parts = [joined] + [lax.ppermute(joined, "lat", route) for route in routes]
    joined = pl.pallas_call(
        plane_gather_kernel,
        out_shape=kept((packed_rows // 2, LANES), grad_type),
        compiler_params=room(8),
        name="plane_gather",
    )(*map(near, parts))
    other = lax.ppermute(joined, "lat", partner)
    grad_in, grad_bin, grad_mid, grad_bmid, grad_out = pl.pallas_call(
        unpack_kernel,
        out_shape=(
            shaped((features, hidden)),
            shaped((1, hidden)),
            shaped((hidden, hidden)),
            shaped((1, hidden)),
            shaped((features, hidden)),
        ),
        compiler_params=room(12),
        name="unpack",
    )(near(joined), near(other), far(select))
    return (
        new_state.reshape(fields, lev_dev, lat_dev, lon_count),
        spectral.reshape(wave_dev, 2, fields, lev_dev, TRUNC),
        grad_in.T,
        grad_bin.reshape(hidden),
        grad_mid,
        grad_bmid.reshape(hidden),
        grad_out,
    )


def fits_fast(mesh, prognostic, w_in, wave_order, lat_order):
    lat_width, lev_width = mesh.shape["lat"], mesh.shape["lev"]
    fields, lev_total, lat_total, lon_count = prognostic.shape
    hidden = w_in.shape[0]
    pairs = fields * lev_total // lev_width
    lat_dev = lat_total // lat_width
    wave_dev = wave_order.shape[0] // lat_width
    packed_rows = (hidden + 2 * lev_width * feature_rows) * (hidden // LANES)
    return (
        2 * lat_total == LANES
        and 4 * wave_dev == LANES
        and lat_dev == 8
        and lat_dev == 2 * lev_width
        and pairs == feature_rows * 3 // 4
        and lon_count % LANES == 0
        and hidden % LANES == 0
        and packed_rows % (16 * lat_width * lev_width) == 0
        and lat_width & (lat_width - 1) == 0
        and lat_width > 2
    )


def solution(mesh):
    def run(*arguments):
        prognostic, w_in, wave_order, lat_order = (arguments[at] for at in (0, 4, 9, 10))
        fast = fits_fast(mesh, prognostic, w_in, wave_order, lat_order)
        return shard(mesh, on_device_fast if fast else on_device)(*arguments)

    return run


def shard(mesh, body):
    return jax.shard_map(
        body,
        mesh=mesh,
        in_specs=(
            P(None, "lev", "lat", None),
            P(None, "lev", "lat", None),
            P(None, "lev"),
            P(),
            P(),
            P(),
            P(),
            P(),
            P(),
            P(),
            P(),
        ),
        out_specs=(
            P(None, "lev", "lat", None),
            P("lat", None, None, "lev", None),
            P(),
            P(),
            P(),
            P(),
            P(),
        ),
        check_vma=False,
    )
```

```python
import functools
import math

import jax
import jax.numpy as jnp
import numpy as np
from jax import lax
from jax.experimental import pallas as pl
from jax.experimental.pallas import tpu as pltpu
from jax.sharding import PartitionSpec as P

TRUNC = 256


block_rows = 32
rescale_bits = 40.0


def legendre_setup(own_waves, colatitude):
    float_type = colatitude.dtype
    all_orders = jnp.arange(TRUNC, dtype=jnp.int32)
    factor_index = jnp.arange(1, TRUNC, dtype=jnp.int32).astype(float_type)
    ratios = 0.5 * jnp.log((2.0 * factor_index + 1.0) / (2.0 * factor_index))
    totals = jnp.concatenate([jnp.zeros((1,), float_type), jnp.cumsum(ratios)])
    matches = own_waves[:, None] == all_orders[None, :]
    diagonal_log = jnp.sum(jnp.where(matches, totals[None, :], 0.0), axis=1) - 0.5 * math.log(2.0)
    orders = own_waves.astype(float_type)
    log_shift = diagonal_log[:, None] + orders[:, None] * jnp.log(jnp.sin(colatitude))[None, :]
    empty_rows = jnp.zeros_like(log_shift)
    return (empty_rows, empty_rows, log_shift)


def legendre_rows(recurrence, first_degree, orders, cosine):
    latest, before, log_shift = recurrence
    rescale_limit = 2.0**rescale_bits
    squared_order = orders * orders
    table_rows = []
    for offset in range(block_rows):
        degree = (first_degree + offset).astype(cosine.dtype)
        upper_coef = jnp.sqrt(
            jnp.maximum(4.0 * degree * degree - 1.0, 0.0)
            / jnp.maximum(degree * degree - squared_order, 1.0)
        )
        lower_num = jnp.maximum((degree - 1.0) * (degree - 1.0) - squared_order, 0.0)
        lower_coef = jnp.sqrt(
            lower_num / jnp.maximum(4.0 * (degree - 1.0) * (degree - 1.0) - 1.0, 1.0)
        )
        recurred = upper_coef[:, None] * (cosine[None, :] * latest - lower_coef[:, None] * before)
        diagonal_start = jnp.where(degree == orders, 1.0, 0.0)[:, None] * jnp.ones_like(latest)
        newest = jnp.where((degree > orders)[:, None], recurred, diagonal_start)
        too_large = jnp.abs(newest) > rescale_limit
        factor = jnp.where(too_large, 1.0 / rescale_limit, 1.0)
        newest = newest * factor
        latest = latest * factor
        log_shift = log_shift + jnp.where(too_large, rescale_bits * math.log(2.0), 0.0)
        table_rows.append(newest * jnp.exp(log_shift))
        before = latest
        latest = newest
    return ((latest, before, log_shift), jnp.stack(table_rows, axis=1))


def spectral_pass(own_waves, colatitude, fourier, damping):
    float_type = fourier.dtype
    lat_total = colatitude.shape[0]
    weight = math.pi / lat_total * jnp.sin(colatitude)
    cosine = jnp.cos(colatitude)
    orders = own_waves.astype(float_type)
    weighted = fourier * weight
    degree_norm = 1.0 / (TRUNC * (TRUNC - 1.0))

    def visit_block(carried, first_degree):
        recurrence, grid_sum = carried
        recurrence, legendre_table = legendre_rows(recurrence, first_degree, orders, cosine)
        coeffs = jnp.einsum(
            "jbn,jkfen->jkfeb", legendre_table, weighted, precision=lax.Precision.HIGHEST
        )
        degree = (first_degree + jnp.arange(block_rows, dtype=jnp.int32)).astype(float_type)
        degree_ratio = degree * (degree + 1.0) * degree_norm
        coeffs = coeffs / (1.0 + damping[:, :, None] * (degree_ratio * degree_ratio)[None, None, :])
        grid_sum = grid_sum + jnp.einsum(
            "jbn,jkfeb->jkfen", legendre_table, coeffs, precision=lax.Precision.HIGHEST
        )
        return ((recurrence, grid_sum), coeffs)

    starts = jnp.arange(0, TRUNC, block_rows, dtype=jnp.int32)
    initial = (legendre_setup(own_waves, colatitude), jnp.zeros_like(fourier))
    (recurrence, synthesized), blocks = lax.scan(visit_block, initial, starts)
    waves, two, fields, levels = fourier.shape[:4]
    coeffs = jnp.moveaxis(blocks, 0, 4).reshape(waves, two, fields, levels, TRUNC)
    return (coeffs, synthesized)


def fourier_angles(wave_order, lon_count):
    points = jnp.arange(lon_count, dtype=jnp.int32)
    phase_index = wave_order[:, None] * points[None, :] % lon_count
    return phase_index.astype(jnp.float32) * (2.0 * math.pi / lon_count)


def fourier_forward(wave_order, lon_count):
    angles = fourier_angles(wave_order, lon_count)
    return jnp.stack([jnp.cos(angles), -jnp.sin(angles)], axis=1) / lon_count


def fourier_inverse(wave_order, lon_count):
    angles = fourier_angles(wave_order, lon_count)
    weights = jnp.where(wave_order == 0, 1.0, 2.0)[:, None, None]
    return weights * jnp.stack([jnp.cos(angles), -jnp.sin(angles)], axis=1)


def silu_slope(value):
    sigmoid_value = jax.nn.sigmoid(value)
    return sigmoid_value * (1.0 + value * (1.0 - sigmoid_value))


def column_physics(inputs, upstream, w_in, b_in, w_mid, b_mid, w_out):
    pre_in = jnp.dot(w_in, inputs, preferred_element_type=jnp.float32) + b_in[:, None]
    hidden_in = jax.nn.silu(pre_in).astype(jnp.bfloat16)
    pre_mid = jnp.dot(w_mid, hidden_in, preferred_element_type=jnp.float32) + b_mid[:, None]
    hidden_mid = jax.nn.silu(pre_mid).astype(jnp.bfloat16)
    tendency = jnp.dot(w_out, hidden_mid, preferred_element_type=jnp.float32).astype(jnp.bfloat16)
    grad_out = jnp.dot(upstream, hidden_mid.T, preferred_element_type=jnp.float32)
    back_mid = jnp.dot(w_out.T, upstream, preferred_element_type=jnp.float32)
    delta_mid = (back_mid * silu_slope(pre_mid)).astype(jnp.bfloat16)
    grad_mid = jnp.dot(delta_mid, hidden_in.T, preferred_element_type=jnp.float32)
    grad_bmid = jnp.sum(delta_mid.astype(jnp.float32), axis=1)
    back_in = jnp.dot(w_mid.T, delta_mid, preferred_element_type=jnp.float32)
    delta_in = (back_in * silu_slope(pre_in)).astype(jnp.bfloat16)
    grad_in = jnp.dot(delta_in, inputs.T, preferred_element_type=jnp.float32)
    grad_bin = jnp.sum(delta_in.astype(jnp.float32), axis=1)
    return (tendency, (grad_in, grad_bin, grad_mid, grad_bmid, grad_out))


def physics_rows(inputs, upstream, w_in, b_in, w_mid, b_mid, w_out):
    fields, lev_total, lat_rows, lon_count = inputs.shape
    features = fields * lev_total
    hidden_units = w_in.shape[0]
    rows_in = jnp.moveaxis(inputs.reshape(features, lat_rows, lon_count), 1, 0)
    rows_up = jnp.moveaxis(upstream.reshape(features, lat_rows, lon_count), 1, 0)

    def visit_row(totals, row_pair):
        tendency, gradients = column_physics(
            row_pair[0], row_pair[1], w_in, b_in, w_mid, b_mid, w_out
        )
        return (jax.tree.map(jnp.add, totals, gradients), tendency)

    empty_sums = (
        jnp.zeros((hidden_units, features), jnp.float32),
        jnp.zeros((hidden_units,), jnp.float32),
        jnp.zeros((hidden_units, hidden_units), jnp.float32),
        jnp.zeros((hidden_units,), jnp.float32),
        jnp.zeros((features, hidden_units), jnp.float32),
    )
    totals, tend_rows = lax.scan(visit_row, empty_sums, (rows_in, rows_up))
    tendency = jnp.moveaxis(tend_rows, 0, 1).reshape(fields, lev_total, lat_rows, lon_count)
    return (tendency, totals)


def on_device(
    prognostic, cotangent, damping, in_scale, w_in, b_in, w_mid, b_mid, w_out, wave_order, lat_order
):
    fields, lev_dev, lat_dev, lon_count = prognostic.shape
    lat_width = lax.axis_size("lat")
    wave_dev = wave_order.shape[0] // lat_width
    lat_total = lat_order.shape[0]
    my_index = lax.axis_index("lat")
    own_waves = lax.dynamic_slice_in_dim(wave_order, my_index * wave_dev, wave_dev)
    to_fourier = fourier_forward(wave_order, lon_count)
    fourier = jnp.einsum("jkn,fean->jkfea", to_fourier, prognostic, precision=lax.Precision.HIGHEST)
    fourier = lax.all_to_all(fourier, "lat", split_axis=0, concat_axis=4, tiled=True)
    colatitude = math.pi * (lat_order.astype(jnp.float32) + 0.5) / lat_total
    spectral, synthesized = spectral_pass(own_waves, colatitude, fourier, damping)
    upstream = lax.all_to_all(cotangent, "lev", split_axis=2, concat_axis=1, tiled=True)
    from_fourier = fourier_inverse(wave_order, lon_count)
    row_modes = lax.all_to_all(synthesized, "lat", split_axis=4, concat_axis=0, tiled=True)
    filtered = jnp.einsum(
        "jkfea,jkn->fean", row_modes, from_fourier, precision=lax.Precision.HIGHEST
    )
    lev_index = lax.axis_index("lev")
    local_scale = lax.dynamic_slice_in_dim(in_scale, lev_index * lev_dev, lev_dev, 1)
    local_inputs = (filtered * local_scale[:, :, None, None]).astype(jnp.bfloat16)
    inputs = lax.all_to_all(local_inputs, "lev", split_axis=2, concat_axis=1, tiled=True)
    tend_cols, totals = physics_rows(inputs, upstream, w_in, b_in, w_mid, b_mid, w_out)
    tendency = lax.all_to_all(tend_cols, "lev", split_axis=1, concat_axis=2, tiled=True)
    new_state = filtered + tendency.astype(jnp.float32)
    grad_scale = 1.0 / math.sqrt(lat_total * lon_count)
    summed = lax.psum(
        (
            totals[0] * grad_scale,
            totals[1] * grad_scale,
            totals[2] * grad_scale,
            totals[3] * grad_scale,
            totals[4] * grad_scale,
        ),
        ("lat", "lev"),
    )
    return (new_state, spectral, summed[0], summed[1], summed[2], summed[3], summed[4])


LANES = 128
half_lanes = LANES // 2
feature_rows = 16
bf16 = jnp.bfloat16
f32 = jnp.float32
forward_type = f32
inverse_type = bf16
state_type = bf16
grad_type = bf16
row_gap = 8


def contract_last(left, right):
    return lax.dot_general(left, right, (((1,), (1,)), ((), ())), preferred_element_type=f32)


def matmul(left, right):
    return lax.dot_general(left, right, (((1,), (0,)), ((), ())), preferred_element_type=f32)


def half_turn_sincos(half_angle):
    square = half_angle * half_angle
    sine = 0.0
    cosine = 0.0
    for power in range(6, -1, -1):
        sine = sine * square + (-1.0) ** power / math.factorial(2 * power + 1)
        cosine = cosine * square + (-1.0) ** power / math.factorial(2 * power)
    sine = sine * half_angle
    return 2.0 * sine * cosine, 1.0 - 2.0 * sine * sine


def turn_sincos(product, period):
    reduced = product - period * jnp.floor(product * (1.0 / period) + 0.5)
    return half_turn_sincos(reduced * (math.pi / period))


def lower_lanes(shape):
    return lax.broadcasted_iota(jnp.int32, shape, len(shape) - 1) < half_lanes


def split_pair(value):
    high = value.astype(bf16)
    return high, (value - high.astype(f32)).astype(bf16)


def polar_sine(lat_index, lat_total):
    nearest = jnp.minimum(lat_index, (lat_total - 1.0) - lat_index)
    return half_turn_sincos((nearest + 0.5) * (0.5 * math.pi / lat_total))


def wave_columns(waves_ref):
    return jnp.broadcast_to(waves_ref[...].astype(f32), (LANES, waves_ref.shape[1])).T


def fill_trig(waves_ref, trig_ref, wave_dev):
    wave_total = waves_ref.shape[1]
    lon_count = trig_ref.shape[1]
    waves = wave_columns(waves_ref)
    lane = lax.broadcasted_iota(jnp.int32, waves.shape, 1).astype(f32)
    sine, cosine = turn_sincos(waves * lane, float(lon_count))
    step_sine, step_cosine = turn_sincos(waves * float(LANES), float(lon_count))
    for tile in range(lon_count // LANES):
        lanes = pl.ds(tile * LANES, LANES)
        cosines = split_pair(cosine)
        sines = split_pair(-sine)
        for owner in range(wave_total // wave_dev):
            rows = slice(owner * wave_dev, (owner + 1) * wave_dev)
            for part in range(2):
                place = 2 * part * wave_total + 2 * owner * wave_dev
                trig_ref[pl.ds(place, wave_dev), lanes] = cosines[part][rows]
                trig_ref[pl.ds(place + wave_dev, wave_dev), lanes] = sines[part][rows]
        cosine, sine = (
            cosine * step_cosine - sine * step_sine,
            sine * step_cosine + cosine * step_sine,
        )


def forward_kernel(lats_ref, waves_ref, prog_hbm, cot_hbm, send_ref, *rest):
    *cot_refs, trig_ref, cot_scratch, prog_ref, cot_ref, prog_sem, cot_sem = rest
    prog_copy = pltpu.make_async_copy(prog_hbm, prog_ref, prog_sem)
    cot_copy = pltpu.make_async_copy(cot_hbm, cot_ref, cot_sem)
    prog_copy.start()
    cot_copy.start()
    lat_width, half_rows, _ = send_ref.shape
    wave_total = waves_ref.shape[1]
    rows_total, lon_count = prog_ref.shape
    lat_total = lats_ref.shape[0]
    lat_dev = lat_total // lat_width
    fill_trig(waves_ref, trig_ref, wave_total // lat_width)
    prog_copy.wait()
    prog_high, prog_low = split_pair(prog_ref[...])
    modes = contract_last(
        jnp.concatenate([prog_high, prog_low], axis=0), trig_ref[pl.ds(0, 2 * wave_total), :]
    )
    modes = modes[:rows_total] + modes[rows_total:] + contract_last(
        prog_high, trig_ref[pl.ds(2 * wave_total, 2 * wave_total), :]
    )
    first_row = lax.axis_index("lat") * lat_dev
    row = lax.broadcasted_iota(jnp.int32, (lat_dev, LANES), 0)
    lat_index = jnp.zeros((lat_dev, LANES), f32)
    for at in range(lat_dev):
        lat_index = jnp.where(row == at, lats_ref[first_row + at].astype(f32), lat_index)
    weight = polar_sine(lat_index, lat_total)[0] * (math.pi / lat_total / lon_count)
    weight = jnp.concatenate([weight] * (half_rows // lat_dev), axis=0)
    lower = lower_lanes((half_rows, LANES))
    for tile in range(lat_width // 2):
        first = modes[:half_rows, tile * LANES : (tile + 1) * LANES] * weight
        second = modes[half_rows:, tile * LANES : (tile + 1) * LANES] * weight
        send_ref[2 * tile] = jnp.where(lower, first, pltpu.roll(second, half_lanes, 1)).astype(
            send_ref.dtype
        )
        send_ref[2 * tile + 1] = jnp.where(
            lower, pltpu.roll(first, half_lanes, 1), second
        ).astype(send_ref.dtype)
    lev_width = len(cot_refs)
    row_share = lat_dev // lev_width
    cot_copy.wait()
    cot_scratch[...] = jnp.zeros_like(cot_scratch)
    cot_all = cot_ref[...].astype(f32)
    tiles = lon_count // LANES
    for tile in range(tiles):
        cot_scratch[tile, pl.ds(0, rows_total), :] = cot_all[:, tile * LANES : (tile + 1) * LANES]
    for shift in range(lev_width):
        dest = (lax.axis_index("lev") + shift) % lev_width
        for share in range(row_share):
            for tile in range(tiles):
                picked = cot_scratch[tile, pl.ds(dest * row_share + share, feature_rows, stride=lat_dev), :]
                cot_refs[shift][share, :, pl.ds(tile * LANES, LANES)] = picked.astype(bf16)


def table_kernel(lats_ref, waves_ref, out_ref, scratch, columns):
    pair_count, degrees, _ = out_ref.shape
    rows = pair_count
    lat_total = lats_ref.shape[1]
    columns[...] = wave_columns(waves_ref)
    first_wave = pl.multiple_of(lax.axis_index("lat") * 2 * rows, 2 * rows)
    orders = jnp.where(
        lower_lanes((rows, LANES)),
        columns[pl.ds(first_wave, rows), :],
        columns[pl.ds(first_wave + rows, rows), :],
    )
    lat_row = lats_ref[...].astype(f32)
    lat_index = jnp.broadcast_to(jnp.concatenate([lat_row, lat_row], axis=1), (rows, LANES))
    sine, cosine = polar_sine(lat_index, lat_total)
    cosine = jnp.where(2.0 * lat_index < lat_total - 1.0, cosine, -cosine)
    index = lax.broadcasted_iota(jnp.int32, (rows, degrees), 1).astype(f32)
    index = jnp.maximum(index, 1.0)
    ratios = 0.5 * jnp.log((2.0 * index + 1.0) / (2.0 * index))
    position = lax.broadcasted_iota(jnp.int32, (rows, degrees), 1)
    counted = position.astype(f32)
    totals = []
    for half in range(2):
        wave = jnp.broadcast_to(orders[:, half * half_lanes : half * half_lanes + 1], (rows, degrees))
        chosen = jnp.where((position > 0) & (counted <= wave), ratios, 0.0)
        totals.append(jnp.broadcast_to(jnp.sum(chosen, axis=1, keepdims=True), (rows, LANES)))
    diagonal_log = jnp.where(lower_lanes((rows, LANES)), totals[0], totals[1])
    log_shift = (
        diagonal_log
        - 0.5 * math.log(2.0)
        - 0.5 * jnp.log(2.0 * orders + 1.0)
        + orders * jnp.log(sine)
    )
    squared = orders * orders
    limit = 2.0**rescale_bits
    zero = jnp.zeros((rows, LANES), f32)

    def visit(block, carried):
        latest, before, previous_root, log_shift = carried
        scale = jnp.exp(log_shift)
        for offset in range(8):
            degree_int = block * 8 + offset
            degree = jnp.full((rows, LANES), degree_int, jnp.int32).astype(f32)
            gap = degree * degree - squared
            inverse_root = lax.rsqrt(jnp.maximum(gap, 1.0))
            root = gap * inverse_root
            recurred = inverse_root * (
                (2.0 * degree - 1.0) * cosine * latest - previous_root * before
            )
            newest = jnp.where(gap > 0.0, recurred, jnp.where(gap == 0.0, 1.0, 0.0))
            scratch[pl.ds(degree_int * (rows + row_gap), rows), :] = newest * scale
            before = latest
            latest = newest
            previous_root = jnp.maximum(root, 0.0)
        too_large = jnp.abs(latest) > limit
        factor = jnp.where(too_large, 1.0 / limit, 1.0)
        log_shift = log_shift + jnp.where(too_large, rescale_bits * math.log(2.0), 0.0)
        return latest * factor, before * factor, previous_root, log_shift

    lax.fori_loop(0, degrees // 8, visit, (zero, zero, zero, log_shift))

    def unpack(pair, carried):
        high, low = split_pair(scratch[pl.ds(pair, degrees, stride=rows + row_gap), :])
        out_ref[pair, :, pl.ds(0, LANES)] = high
        out_ref[pair, :, pl.ds(LANES, LANES)] = low
        return carried

    lax.fori_loop(0, pair_count, unpack, 0)


def level_major(pair, fields, lev_dev):
    return pair % lev_dev * fields + pair // lev_dev


def spectral_kernel(
    waves_ref, damping_ref, recv_ref, table_ref, spec_ref, send_ref, modes, sums, picked
):
    pair_count, degrees, _ = table_ref.shape
    wave_dev = 2 * pair_count
    lat_width, half_rows, _ = recv_ref.shape
    lat_total = LANES // 2
    lat_dev = lat_total // lat_width
    fields, lev_dev = damping_ref.shape
    pairs = fields * lev_dev
    half_pairs = pairs // 2
    first_wave = lax.axis_index("lat") * wave_dev
    pitch = wave_dev + row_gap
    received = recv_ref[...].astype(f32)
    upper_rows = lax.broadcasted_iota(jnp.int32, (LANES, LANES), 0) % wave_dev >= pair_count
    for index in range(half_pairs):
        stacked = [
            received[source, index * lat_dev : (index + 1) * lat_dev] for source in range(lat_width)
        ]
        stacked.append(jnp.zeros((LANES - lat_total, LANES), f32))
        turned = jnp.concatenate(stacked, axis=0).T
        turned = jnp.where(upper_rows, pltpu.roll(turned, half_lanes, 1), turned)
        for half in range(2):
            for part in range(2):
                start = (half * 2 + part) * wave_dev
                place = (part * pairs + level_major(half * half_pairs + index, fields, lev_dev)) * pitch
                modes[pl.ds(place, wave_dev), :] = turned[start : start + wave_dev]
    degree = lax.broadcasted_iota(jnp.int32, (pairs, degrees), 1).astype(f32)
    degree_ratio = degree * (degree + 1.0) * (1.0 / (degrees * (degrees - 1.0)))
    root = jnp.sqrt(2.0 * degree + 1.0)
    row = lax.broadcasted_iota(jnp.int32, (pairs, degrees), 0)
    strength = jnp.zeros((pairs, degrees), f32)
    for pair in range(pairs):
        at = level_major(pair, fields, lev_dev)
        strength = jnp.where(row == at, damping_ref[pair // lev_dev, pair % lev_dev], strength)
    damp = root / (1.0 + strength * (degree_ratio * degree_ratio))
    damp = jnp.concatenate([damp, damp, damp, damp], axis=0)
    root_row = root[:1]
    count = 2 * pairs
    for pair in range(pair_count):
        first = modes[pl.ds(pair, count, stride=pitch), :]
        second = modes[pl.ds(pair + pair_count, count, stride=pitch), :]
        stacked = jnp.concatenate([first, second], axis=0)
        table = table_ref[pair]
        if recv_ref.dtype == f32:
            stacked = jnp.concatenate(split_pair(stacked), axis=0)
        else:
            stacked = stacked.astype(bf16)
        coeffs = contract_last(jnp.concatenate([stacked, stacked], axis=1), table)
        if recv_ref.dtype == f32:
            coeffs = coeffs[: 2 * count] + coeffs[2 * count :]
        coeffs = coeffs * damp
        shape = (2, lev_dev, fields, degrees)
        spec_ref[pair] = coeffs[:count].reshape(shape)
        spec_ref[pair + pair_count] = coeffs[count:].reshape(shape)
        first_weight = jnp.where(waves_ref[first_wave + pair] == 0, 1.0, 2.0)
        second_weight = jnp.where(waves_ref[first_wave + pair + pair_count] == 0, 1.0, 2.0)
        rooted = jnp.concatenate(
            [coeffs[:count] * (root_row * first_weight), coeffs[count:] * (root_row * second_weight)],
            axis=0,
        )
        synth = matmul(jnp.concatenate(split_pair(rooted), axis=0), table)
        synth = synth[: 2 * count] + synth[2 * count :]
        synth = synth[:, :LANES] + synth[:, LANES:]
        sums[pl.ds(pair, count, stride=pitch), :] = synth[:count]
        sums[pl.ds(pair + pair_count, count, stride=pitch), :] = synth[count:]
    owners = send_ref.shape[0] // (2 * pairs)
    lower = lower_lanes((owners, LANES))
    share = lat_total // owners
    blank = jnp.zeros((owners, LANES), f32)
    sent_rows = 2 * pairs

    def put(row, value):
        high = value.astype(bf16).astype(f32)
        picked[pl.ds(lat_total + row, owners, stride=sent_rows), :] = high
        picked[pl.ds(lat_total + pairs + row, owners, stride=sent_rows), :] = value - high

    for index in range(half_pairs):
        blocks = []
        for half in range(2):
            for part in range(2):
                place = (part * pairs + level_major(half * half_pairs + index, fields, lev_dev)) * pitch
                blocks.append(sums[pl.ds(place, wave_dev), :])
        stacked = jnp.concatenate(blocks, axis=0)
        stacked = jnp.where(upper_rows, pltpu.roll(stacked, half_lanes, 1), stacked)
        picked[pl.ds(0, lat_total), :] = stacked.T[:lat_total]
        even = picked[pl.ds(0, owners, stride=share), :]
        odd = picked[pl.ds(1, owners, stride=share), :]
        put(index, jnp.where(lower, even, pltpu.roll(odd, half_lanes, 1)))
        put(half_pairs + index, jnp.where(lower, pltpu.roll(even, half_lanes, 1), odd))
    send_ref[...] = picked[pl.ds(lat_total, owners * sent_rows), :].astype(send_ref.dtype)


def weights_kernel(
    wave_dev, scale_ref, waves_ref, select_ref, w_in_ref, b_in_ref, w_mid_ref, w_out_ref,
    trig_ref, in_ref, mid_ref, mid_turned_ref, out_ref, out_turned_ref, scale_out_ref,
):
    fill_trig(waves_ref, trig_ref, wave_dev)
    hidden = w_mid_ref.shape[0]
    padded = select_ref.shape[0]
    spare = feature_rows * 3 // 4
    select = select_ref[...]
    bias = jnp.broadcast_to(b_in_ref[...], (padded, hidden))
    high = bias.astype(bf16).astype(f32)
    row = lax.broadcasted_iota(jnp.int32, (padded, hidden), 0)
    spread = matmul(select, w_in_ref[...])
    spread = jnp.where(row == spare, high, jnp.where(row == spare + 1, bias - high, spread))
    in_ref[...] = spread.T.astype(bf16)
    mid_ref[...] = w_mid_ref[...]
    mid_turned_ref[...] = w_mid_ref[...].astype(f32).T.astype(bf16)
    spread_out = matmul(select, w_out_ref[...])
    out_ref[...] = spread_out.astype(bf16)
    out_turned_ref[...] = spread_out.T.astype(bf16)
    fields, lev_total = scale_ref.shape
    lev_dev = spare // fields
    row = lax.broadcasted_iota(jnp.int32, (padded, LANES), 0)
    scales = jnp.zeros((padded, LANES), f32)
    for field in range(fields):
        for level in range(lev_total):
            place = level // lev_dev * feature_rows + field * lev_dev + level % lev_dev
            scales = jnp.where(row == place, scale_ref[field, level], scales)
    scale_out_ref[...] = scales


def columns_kernel(lev_width, recv_ref, *rest):
    cot_refs, rest = rest[:lev_width], rest[lev_width:]
    trig_ref, w_in_ref, w_mid_ref, w_turned_ref, *rest = rest
    w_out_ref, w_out_turned_ref, scale_ref, bias_row_ref, *rest = rest
    state_refs, rest = rest[:lev_width], rest[lev_width:]
    keep_ref, give_ref, packed, modes, cot_all, state_all, grad_in, grad_mid, grad_out, grad_bias, bias_ref = rest
    row_share, _, lon_count = cot_refs[0].shape
    lat_width = recv_ref.shape[0] // lev_width
    level = lax.axis_index("lev")
    padded = lev_width * feature_rows
    hidden = w_mid_ref.shape[0]
    spare = feature_rows * 3 // 4
    lower = lower_lanes((padded, LANES))
    feature = lax.broadcasted_iota(jnp.int32, (lev_width, feature_rows, LANES), 1)

    def unfold(owner):
        piece = recv_ref[pl.ds(owner * lev_width, lev_width)].astype(f32)
        rest = pltpu.roll(piece, spare, 1)
        return [
            jnp.where(feature < spare, part[:, :feature_rows], 0.0).reshape(padded, LANES)
            for part in (piece, rest)
        ]

    for tile in range(lat_width // 2):
        firsts, seconds = unfold(2 * tile), unfold(2 * tile + 1)
        lanes = pl.ds(tile * LANES, LANES)
        for part, (first, second) in enumerate(zip(firsts, seconds)):
            rows = pl.ds(part * padded, padded)
            modes[0, rows, lanes] = jnp.where(lower, first, pltpu.roll(second, half_lanes, 1)).astype(bf16)
            modes[1, rows, lanes] = jnp.where(lower, pltpu.roll(first, half_lanes, 1), second).astype(bf16)
    for shift in range(lev_width):
        source = (level + (lev_width - shift)) % lev_width
        start = pl.multiple_of(source * feature_rows, feature_rows)
        cot_all[:, pl.ds(start, feature_rows), :] = cot_refs[shift][...]
    grad_in[...] = jnp.zeros_like(grad_in)
    grad_mid[...] = jnp.zeros_like(grad_mid)
    grad_out[...] = jnp.zeros_like(grad_out)
    grad_bias[...] = jnp.zeros_like(grad_bias)
    bias_ref[...] = jnp.broadcast_to(bias_row_ref[...], (LANES, hidden)).T
    width = 6 * LANES
    while lon_count % width:
        width //= 2
    blocks = lon_count // width

    def visit(block, carried):
        share = block // blocks
        lanes = pl.ds(pl.multiple_of(block % blocks * width, width), width)
        half = trig_ref.shape[0] // 2
        filtered = matmul(modes[share], trig_ref[pl.ds(0, half), lanes])
        filtered = filtered[:padded] + filtered[padded:]
        filtered += matmul(modes[share, :padded], trig_ref[pl.ds(half, half), lanes])
        row = lax.broadcasted_iota(jnp.int32, (padded, width), 0)
        scaled = filtered * jnp.concatenate([scale_ref[...]] * (width // LANES), axis=1)
        inputs = jnp.where((row == spare) | (row == spare + 1), 1.0, scaled).astype(bf16)
        upstream = cot_all[share, :, lanes]
        pre_in = matmul(w_in_ref[...], inputs)
        gate = 0.5 + 0.5 * jnp.tanh(0.5 * pre_in)
        active = pre_in * gate
        slope_in = gate + active * (1.0 - gate)
        hidden_in = active.astype(bf16)
        bias = jnp.concatenate([bias_ref[...]] * (width // LANES), axis=1)
        pre_mid = matmul(w_mid_ref[...], hidden_in) + bias
        gate = 0.5 + 0.5 * jnp.tanh(0.5 * pre_mid)
        active = pre_mid * gate
        slope_mid = gate + active * (1.0 - gate)
        hidden_mid = active.astype(bf16)
        tendency = matmul(w_out_ref[...], hidden_mid).astype(bf16).astype(f32)
        state_all[share, :, lanes] = (filtered + tendency).astype(state_all.dtype)
        delta = matmul(w_out_turned_ref[...], upstream) * slope_mid
        delta_mid = delta.astype(bf16)
        grad_out[...] += contract_last(upstream, hidden_mid)
        grad_mid[...] += contract_last(delta_mid, hidden_in)
        total = delta[:, :LANES]
        for tile in range(1, width // LANES):
            total = total + delta[:, tile * LANES : (tile + 1) * LANES]
        grad_bias[...] += total
        delta_in = (matmul(w_turned_ref[...], delta_mid) * slope_in).astype(bf16)
        grad_in[...] += contract_last(inputs, delta_in)
        return carried

    lax.fori_loop(0, row_share * blocks, visit, 0)
    for shift in range(lev_width):
        dest = (level + shift) % lev_width
        start = pl.multiple_of(dest * feature_rows, feature_rows)
        for share in range(row_share):
            for tile in range(lon_count // LANES):
                place = (share * (lon_count // LANES) + tile) * feature_rows
                state_refs[shift][pl.ds(place, feature_rows), :] = state_all[
                    share, pl.ds(start, feature_rows), pl.ds(tile * LANES, LANES)
                ]
    bias_row = lax.dot_general(
        jnp.ones((8, LANES), f32), grad_bias[...], (((1,), (1,)), ((), ())),
        precision=lax.Precision.HIGHEST, preferred_element_type=f32,
    )[:1]
    row = lax.broadcasted_iota(jnp.int32, (padded, hidden), 0)
    first_rows = jnp.where(row == spare + 1, jnp.broadcast_to(bias_row, (padded, hidden)), grad_in[...])
    total_rows = hidden + 2 * padded
    for tile in range(hidden // LANES):
        lanes = slice(tile * LANES, (tile + 1) * LANES)
        start = tile * total_rows
        packed[pl.ds(start, hidden), :] = grad_mid[:, lanes]
        packed[pl.ds(start + hidden, padded), :] = first_rows[:, lanes]
        packed[pl.ds(start + hidden + padded, padded), :] = grad_out[:, lanes]
    half_rows = packed.shape[0] // 2
    side = lax.axis_index("lat") % 2
    keep_ref[...] = packed[pl.ds(pl.multiple_of(side * half_rows, 16), half_rows), :]
    give_ref[...] = packed[pl.ds(pl.multiple_of((1 - side) * half_rows, 16), half_rows), :].astype(
        give_ref.dtype
    )


def part_rows(index, ref):
    count = ref.shape[0]
    return pl.ds(pl.multiple_of(index * count, 16), count)


def plane_scatter_kernel(keep_ref, recv_ref, rest_ref, *send_refs):
    chip = lax.axis_index("lat") // 2
    for offset, ref in enumerate((rest_ref, *send_refs)):
        rows = part_rows(chip ^ offset, ref)
        ref[...] = (keep_ref[rows, :] + recv_ref[rows, :].astype(f32)).astype(ref.dtype)


def plane_sum_kernel(keep_ref, *rest):
    *recv_refs, out_ref = rest
    total = keep_ref[...]
    for ref in recv_refs:
        total = total + ref[...].astype(f32)
    out_ref[...] = total.astype(out_ref.dtype)


def reduce_kernel(grad_scale, *refs):
    *part_refs, out_ref, ordered = refs
    width = len(part_refs)
    level = lax.axis_index("lev")
    for shift, ref in enumerate(part_refs):
        ordered[(level + (width - shift)) % width] = ref[...]
    total = ordered[0].astype(f32)
    for source in range(1, width):
        total = total + ordered[source].astype(f32)
    out_ref[...] = (total * grad_scale).astype(bf16)


def plane_gather_kernel(*refs):
    *part_refs, out_ref = refs
    chip = lax.axis_index("lat") // 2
    for offset, ref in enumerate(part_refs):
        out_ref[part_rows(chip ^ offset, ref), :] = ref[...]


def state_kernel(row_share, *refs):
    *recv_refs, out_ref, scratch = refs
    lev_width = len(recv_refs)
    lat_dev = lev_width * row_share
    pairs = out_ref.shape[0] // lat_dev
    tiles = out_ref.shape[1] // LANES
    for shift, ref in enumerate(recv_refs):
        source = (lax.axis_index("lev") + (lev_width - shift)) % lev_width
        first = ref.shape[0] - row_share * tiles * feature_rows
        for share in range(row_share):
            for tile in range(tiles):
                place = first + (share * tiles + tile) * feature_rows
                rows = ref[pl.ds(place, feature_rows), :].astype(f32)[:pairs]
                scratch[tile, pl.ds(source * row_share + share, pairs, stride=lat_dev), :] = rows
    for tile in range(tiles):
        out_ref[:, pl.ds(tile * LANES, LANES)] = scratch[tile]


def unpack_kernel(own_ref, other_ref, select_ref, in_ref, bin_ref, mid_ref, bmid_ref, out_ref):
    hidden = mid_ref.shape[0]
    padded = select_ref.shape[1]
    spare = feature_rows * 3 // 4
    total_rows = hidden + 2 * padded
    select = select_ref[...]
    side = lax.axis_index("lat") % 2
    half_tiles = own_ref.shape[0] // total_rows
    for ref, half in ((own_ref, side), (other_ref, 1 - side)):
        for tile in range(half_tiles):
            lanes = pl.ds(pl.multiple_of((half * half_tiles + tile) * LANES, LANES), LANES)
            start = tile * total_rows
            mid_ref[:, lanes] = ref[pl.ds(start, hidden), :].astype(f32)
            rows = ref[pl.ds(start + hidden, padded), :]
            wide = rows.astype(f32)
            bin_ref[:, lanes] = wide[spare : spare + 1]
            bmid_ref[:, lanes] = wide[spare + 1 : spare + 2]
            in_ref[:, lanes] = matmul(select, rows)
            out_ref[:, lanes] = matmul(select, ref[pl.ds(start + hidden + padded, padded), :])


def shaped(shape, kind=f32):
    return jax.ShapeDtypeStruct(shape, kind)


def room(mib):
    return pltpu.CompilerParams(vmem_limit_bytes=mib << 20)


def kept(shape, kind=f32):
    return pltpu.VMEM(shape, kind)


def near(array):
    return pltpu.with_memory_space_constraint(array, pltpu.VMEM)


def far(array):
    return pltpu.with_memory_space_constraint(array, pltpu.HBM)


def cost(flops, moved):
    return pl.CostEstimate(flops=flops, transcendentals=0, bytes_accessed=moved)


def rotate(pieces, width):
    moved = [pieces[0]]
    for shift in range(1, width):
        route = [(source, (source + shift) % width) for source in range(width)]
        moved.append(lax.ppermute(pieces[shift], "lev", route))
    return moved


def on_device_fast(
    prognostic, cotangent, damping, in_scale, w_in, b_in, w_mid, b_mid, w_out, wave_order, lat_order
):
    fields, lev_dev, lat_dev, lon_count = prognostic.shape
    lat_width = lax.axis_size("lat")
    lev_width = lax.axis_size("lev")
    wave_total = wave_order.shape[0]
    wave_dev = wave_total // lat_width
    lat_total = lat_order.shape[0]
    pairs = fields * lev_dev
    row_share = lat_dev // lev_width
    hidden, features = w_in.shape
    padded = lev_width * feature_rows
    owners = lat_width * lev_width
    pair_count = wave_dev // 2
    lev_total = lev_dev * lev_width

    select = np.zeros((features, padded), np.float32)
    for field in range(fields):
        for level in range(lev_total):
            place = level // lev_dev * feature_rows + field * lev_dev + level % lev_dev
            select[field * lev_total + level, place] = 1.0
    spread_select = jnp.asarray(select.T, bf16)
    select = jnp.asarray(select, bf16)

    smem = pl.BlockSpec(memory_space=pltpu.SMEM)
    hbm = pl.BlockSpec(memory_space=pltpu.HBM)
    vmem = pl.BlockSpec(memory_space=pltpu.VMEM)
    wave_row = wave_order.reshape(1, wave_total)
    piece = (row_share, feature_rows, lon_count)
    send, *cot_pieces = pl.pallas_call(
        forward_kernel,
        in_specs=[smem, vmem, hbm, hbm],
        out_shape=(
            kept((lat_width, pairs * lat_dev // 2, LANES), forward_type),
            *([kept(piece, bf16)] * lev_width),
        ),
        scratch_shapes=[
            pltpu.VMEM((4 * wave_total, lon_count), bf16),
            pltpu.VMEM((lon_count // LANES, feature_rows * lat_dev, LANES), f32),
            pltpu.VMEM((pairs * lat_dev, lon_count), f32),
            pltpu.VMEM((pairs * lat_dev, lon_count), bf16),
            pltpu.SemaphoreType.DMA(()),
            pltpu.SemaphoreType.DMA(()),
        ],
        compiler_params=room(16),
        name="forward",
    )(
        far(lat_order),
        far(wave_row),
        far(prognostic.reshape(pairs * lat_dev, lon_count)),
        far(cotangent.reshape(pairs * lat_dev, lon_count)),
    )
    received = lax.all_to_all(send, "lat", split_axis=0, concat_axis=0, tiled=True)
    upstream = rotate(cot_pieces, lev_width)
    table = pl.pallas_call(
        table_kernel,
        out_shape=kept((pair_count, TRUNC, 2 * LANES), bf16),
        scratch_shapes=[
            pltpu.VMEM((TRUNC * (pair_count + row_gap), LANES), f32),
            pltpu.VMEM((wave_total, LANES), f32),
        ],
        cost_estimate=cost(8000000, 1 << 20),
        compiler_params=room(16),
        name="legendre",
    )(far(lat_order.reshape(1, lat_total)), far(wave_row))
    spectral, modes_send = pl.pallas_call(
        spectral_kernel,
        in_specs=[smem, smem, vmem, vmem],
        out_shape=(
            pltpu.HBM((wave_dev, 2, lev_dev, fields, TRUNC), f32),
            kept((owners * 2 * pairs, LANES), bf16),
        ),
        scratch_shapes=[
            pltpu.VMEM((2 * pairs * (wave_dev + row_gap), LANES), f32),
            pltpu.VMEM((2 * pairs * (wave_dev + row_gap), LANES), f32),
            pltpu.VMEM((lat_total + owners * 2 * pairs, LANES), f32),
        ],
        compiler_params=room(16),
        name="spectral",
    )(far(wave_order), far(damping), near(received), near(table))
    both = ("lat", "lev")
    modes = lax.all_to_all(
        modes_send.reshape(owners, 2 * pairs, LANES), both, split_axis=0, concat_axis=0, tiled=True
    )
    prepared = pl.pallas_call(
        functools.partial(weights_kernel, wave_dev),
        out_shape=(
            kept((4 * wave_total, lon_count), bf16),
            kept((hidden, padded), bf16),
            kept((hidden, hidden), bf16),
            kept((hidden, hidden), bf16),
            kept((padded, hidden), bf16),
            kept((hidden, padded), bf16),
            kept((padded, LANES)),
        ),
        in_specs=[smem] + [vmem] * 6,
        cost_estimate=cost(4000000, 1 << 20),
        compiler_params=room(12),
        name="weights",
    )(
        far(in_scale),
        far(wave_row),
        far(spread_select),
        far(w_in.T),
        far(b_in.reshape(1, hidden)),
        far(w_mid),
        far(w_out),
    )
    total_rows = hidden + 2 * padded
    packed_rows = total_rows * (hidden // LANES)
    state_rows = row_share * feature_rows * (lon_count // LANES)
    *state_pieces, keep, give = pl.pallas_call(
        functools.partial(columns_kernel, lev_width),
        out_shape=(
            *([kept((state_rows, LANES), state_type)] * lev_width),
            kept((packed_rows // 2, LANES)),
            kept((packed_rows // 2, LANES), grad_type),
        ),
        scratch_shapes=[
            pltpu.VMEM((packed_rows, LANES), f32),
            pltpu.VMEM((row_share, 2 * padded, 2 * wave_total), bf16),
            pltpu.VMEM((row_share, padded, lon_count), bf16),
            pltpu.VMEM((row_share, padded, lon_count), state_type),
            pltpu.VMEM((padded, hidden), f32),
            pltpu.VMEM((hidden, hidden), f32),
            pltpu.VMEM((padded, hidden), f32),
            pltpu.VMEM((hidden, LANES), f32),
            pltpu.VMEM((hidden, LANES), f32),
        ],
        compiler_params=room(24),
        name="columns",
    )(
        *map(near, (modes, *upstream, *prepared)), far(b_mid.reshape(1, hidden))
    )
    chips = lat_width // 2
    quarter = packed_rows // lat_width
    partner = [(at, at ^ 1) for at in range(lat_width)]
    routes = [[(at, at ^ (2 * offset)) for at in range(lat_width)] for offset in range(1, chips)]
    taken = lax.ppermute(give, "lat", partner)
    rest, *sends = pl.pallas_call(
        plane_scatter_kernel,
        out_shape=(
            kept((quarter, LANES)),
            *([kept((quarter, LANES), grad_type)] * (chips - 1)),
        ),
        compiler_params=room(8),
        name="plane_scatter",
    )(near(keep), near(taken))
    taken = [lax.ppermute(send, "lat", route) for send, route in zip(sends, routes)]
    taken, state = lax.optimization_barrier((taken, rotate(state_pieces, lev_width)))
    mine = pl.pallas_call(
        plane_sum_kernel,
        out_shape=kept((quarter, LANES), grad_type),
        compiler_params=room(8),
        name="plane_sum",
    )(*map(near, (rest, *taken)))
    grad_scale = 1.0 / math.sqrt(lat_total * lon_count)
    joined = pl.pallas_call(
        functools.partial(reduce_kernel, grad_scale),
        out_shape=kept((quarter, LANES), grad_type),
        scratch_shapes=[pltpu.VMEM((lev_width, quarter, LANES), grad_type)],
        compiler_params=room(8),
        name="reduce",
    )(*map(near, rotate([mine] * lev_width, lev_width)))
    new_state = pl.pallas_call(
        functools.partial(state_kernel, row_share),
        out_shape=pltpu.HBM((pairs * lat_dev, lon_count), f32),
        scratch_shapes=[pltpu.VMEM((lon_count // LANES, pairs * lat_dev, LANES), f32)],
        cost_estimate=cost(2000000, 1 << 19),
        compiler_params=room(8),
        name="state",
    )(*map(near, state))
    joined, new_state = lax.optimization_barrier((joined, new_state))
    parts = [joined] + [lax.ppermute(joined, "lat", route) for route in routes]
    joined = pl.pallas_call(
        plane_gather_kernel,
        out_shape=kept((packed_rows // 2, LANES), grad_type),
        compiler_params=room(8),
        name="plane_gather",
    )(*map(near, parts))
    other = lax.ppermute(joined, "lat", partner)
    grad_in, grad_bin, grad_mid, grad_bmid, grad_out = pl.pallas_call(
        unpack_kernel,
        out_shape=(
            shaped((features, hidden)),
            shaped((1, hidden)),
            shaped((hidden, hidden)),
            shaped((1, hidden)),
            shaped((features, hidden)),
        ),
        compiler_params=room(12),
        name="unpack",
    )(near(joined), near(other), far(select))
    return (
        new_state.reshape(fields, lev_dev, lat_dev, lon_count),
        spectral.transpose(0, 1, 3, 2, 4),
        grad_in.T,
        grad_bin.reshape(hidden),
        grad_mid,
        grad_bmid.reshape(hidden),
        grad_out,
    )


def fits_fast(mesh, prognostic, w_in, wave_order, lat_order):
    lat_width, lev_width = mesh.shape["lat"], mesh.shape["lev"]
    fields, lev_total, lat_total, lon_count = prognostic.shape
    hidden = w_in.shape[0]
    pairs = fields * lev_total // lev_width
    lat_dev = lat_total // lat_width
    wave_dev = wave_order.shape[0] // lat_width
    packed_rows = (hidden + 2 * lev_width * feature_rows) * (hidden // LANES)
    return (
        2 * lat_total == LANES
        and 4 * wave_dev == LANES
        and lat_dev == 8
        and lat_dev == 2 * lev_width
        and pairs == feature_rows * 3 // 4
        and lon_count % LANES == 0
        and hidden % LANES == 0
        and packed_rows % (16 * lat_width * lev_width) == 0
        and lat_width & (lat_width - 1) == 0
        and lat_width > 2
        and lev_width & (lev_width - 1) == 0
    )


def solution(mesh):
    def run(*arguments):
        prognostic, w_in, wave_order, lat_order = (arguments[at] for at in (0, 4, 9, 10))
        fast = fits_fast(mesh, prognostic, w_in, wave_order, lat_order)
        return shard(mesh, on_device_fast if fast else on_device)(*arguments)

    return run


def shard(mesh, body):
    return jax.shard_map(
        body,
        mesh=mesh,
        in_specs=(
            P(None, "lev", "lat", None),
            P(None, "lev", "lat", None),
            P(None, "lev"),
            P(),
            P(),
            P(),
            P(),
            P(),
            P(),
            P(),
            P(),
        ),
        out_specs=(
            P(None, "lev", "lat", None),
            P("lat", None, None, "lev", None),
            P(),
            P(),
            P(),
            P(),
            P(),
        ),
        check_vma=False,
    )
```

```python
import functools
import math

import jax
import jax.numpy as jnp
import numpy as np
from jax import lax
from jax.experimental import pallas as pl
from jax.experimental.pallas import tpu as pltpu
from jax.sharding import PartitionSpec as P

TRUNC = 256


block_rows = 32
rescale_bits = 40.0


def legendre_setup(own_waves, colatitude):
    float_type = colatitude.dtype
    all_orders = jnp.arange(TRUNC, dtype=jnp.int32)
    factor_index = jnp.arange(1, TRUNC, dtype=jnp.int32).astype(float_type)
    ratios = 0.5 * jnp.log((2.0 * factor_index + 1.0) / (2.0 * factor_index))
    totals = jnp.concatenate([jnp.zeros((1,), float_type), jnp.cumsum(ratios)])
    matches = own_waves[:, None] == all_orders[None, :]
    diagonal_log = jnp.sum(jnp.where(matches, totals[None, :], 0.0), axis=1) - 0.5 * math.log(2.0)
    orders = own_waves.astype(float_type)
    log_shift = diagonal_log[:, None] + orders[:, None] * jnp.log(jnp.sin(colatitude))[None, :]
    empty_rows = jnp.zeros_like(log_shift)
    return (empty_rows, empty_rows, log_shift)


def legendre_rows(recurrence, first_degree, orders, cosine):
    latest, before, log_shift = recurrence
    rescale_limit = 2.0**rescale_bits
    squared_order = orders * orders
    table_rows = []
    for offset in range(block_rows):
        degree = (first_degree + offset).astype(cosine.dtype)
        upper_coef = jnp.sqrt(
            jnp.maximum(4.0 * degree * degree - 1.0, 0.0)
            / jnp.maximum(degree * degree - squared_order, 1.0)
        )
        lower_num = jnp.maximum((degree - 1.0) * (degree - 1.0) - squared_order, 0.0)
        lower_coef = jnp.sqrt(
            lower_num / jnp.maximum(4.0 * (degree - 1.0) * (degree - 1.0) - 1.0, 1.0)
        )
        recurred = upper_coef[:, None] * (cosine[None, :] * latest - lower_coef[:, None] * before)
        diagonal_start = jnp.where(degree == orders, 1.0, 0.0)[:, None] * jnp.ones_like(latest)
        newest = jnp.where((degree > orders)[:, None], recurred, diagonal_start)
        too_large = jnp.abs(newest) > rescale_limit
        factor = jnp.where(too_large, 1.0 / rescale_limit, 1.0)
        newest = newest * factor
        latest = latest * factor
        log_shift = log_shift + jnp.where(too_large, rescale_bits * math.log(2.0), 0.0)
        table_rows.append(newest * jnp.exp(log_shift))
        before = latest
        latest = newest
    return ((latest, before, log_shift), jnp.stack(table_rows, axis=1))


def spectral_pass(own_waves, colatitude, fourier, damping):
    float_type = fourier.dtype
    lat_total = colatitude.shape[0]
    weight = math.pi / lat_total * jnp.sin(colatitude)
    cosine = jnp.cos(colatitude)
    orders = own_waves.astype(float_type)
    weighted = fourier * weight
    degree_norm = 1.0 / (TRUNC * (TRUNC - 1.0))

    def visit_block(carried, first_degree):
        recurrence, grid_sum = carried
        recurrence, legendre_table = legendre_rows(recurrence, first_degree, orders, cosine)
        coeffs = jnp.einsum(
            "jbn,jkfen->jkfeb", legendre_table, weighted, precision=lax.Precision.HIGHEST
        )
        degree = (first_degree + jnp.arange(block_rows, dtype=jnp.int32)).astype(float_type)
        degree_ratio = degree * (degree + 1.0) * degree_norm
        coeffs = coeffs / (1.0 + damping[:, :, None] * (degree_ratio * degree_ratio)[None, None, :])
        grid_sum = grid_sum + jnp.einsum(
            "jbn,jkfeb->jkfen", legendre_table, coeffs, precision=lax.Precision.HIGHEST
        )
        return ((recurrence, grid_sum), coeffs)

    starts = jnp.arange(0, TRUNC, block_rows, dtype=jnp.int32)
    initial = (legendre_setup(own_waves, colatitude), jnp.zeros_like(fourier))
    (recurrence, synthesized), blocks = lax.scan(visit_block, initial, starts)
    waves, two, fields, levels = fourier.shape[:4]
    coeffs = jnp.moveaxis(blocks, 0, 4).reshape(waves, two, fields, levels, TRUNC)
    return (coeffs, synthesized)


def fourier_angles(wave_order, lon_count):
    points = jnp.arange(lon_count, dtype=jnp.int32)
    phase_index = wave_order[:, None] * points[None, :] % lon_count
    return phase_index.astype(jnp.float32) * (2.0 * math.pi / lon_count)


def fourier_forward(wave_order, lon_count):
    angles = fourier_angles(wave_order, lon_count)
    return jnp.stack([jnp.cos(angles), -jnp.sin(angles)], axis=1) / lon_count


def fourier_inverse(wave_order, lon_count):
    angles = fourier_angles(wave_order, lon_count)
    weights = jnp.where(wave_order == 0, 1.0, 2.0)[:, None, None]
    return weights * jnp.stack([jnp.cos(angles), -jnp.sin(angles)], axis=1)


def silu_slope(value):
    sigmoid_value = jax.nn.sigmoid(value)
    return sigmoid_value * (1.0 + value * (1.0 - sigmoid_value))


def column_physics(inputs, upstream, w_in, b_in, w_mid, b_mid, w_out):
    pre_in = jnp.dot(w_in, inputs, preferred_element_type=jnp.float32) + b_in[:, None]
    hidden_in = jax.nn.silu(pre_in).astype(jnp.bfloat16)
    pre_mid = jnp.dot(w_mid, hidden_in, preferred_element_type=jnp.float32) + b_mid[:, None]
    hidden_mid = jax.nn.silu(pre_mid).astype(jnp.bfloat16)
    tendency = jnp.dot(w_out, hidden_mid, preferred_element_type=jnp.float32).astype(jnp.bfloat16)
    grad_out = jnp.dot(upstream, hidden_mid.T, preferred_element_type=jnp.float32)
    back_mid = jnp.dot(w_out.T, upstream, preferred_element_type=jnp.float32)
    delta_mid = (back_mid * silu_slope(pre_mid)).astype(jnp.bfloat16)
    grad_mid = jnp.dot(delta_mid, hidden_in.T, preferred_element_type=jnp.float32)
    grad_bmid = jnp.sum(delta_mid.astype(jnp.float32), axis=1)
    back_in = jnp.dot(w_mid.T, delta_mid, preferred_element_type=jnp.float32)
    delta_in = (back_in * silu_slope(pre_in)).astype(jnp.bfloat16)
    grad_in = jnp.dot(delta_in, inputs.T, preferred_element_type=jnp.float32)
    grad_bin = jnp.sum(delta_in.astype(jnp.float32), axis=1)
    return (tendency, (grad_in, grad_bin, grad_mid, grad_bmid, grad_out))


def physics_rows(inputs, upstream, w_in, b_in, w_mid, b_mid, w_out):
    fields, lev_total, lat_rows, lon_count = inputs.shape
    features = fields * lev_total
    hidden_units = w_in.shape[0]
    rows_in = jnp.moveaxis(inputs.reshape(features, lat_rows, lon_count), 1, 0)
    rows_up = jnp.moveaxis(upstream.reshape(features, lat_rows, lon_count), 1, 0)

    def visit_row(totals, row_pair):
        tendency, gradients = column_physics(
            row_pair[0], row_pair[1], w_in, b_in, w_mid, b_mid, w_out
        )
        return (jax.tree.map(jnp.add, totals, gradients), tendency)

    empty_sums = (
        jnp.zeros((hidden_units, features), jnp.float32),
        jnp.zeros((hidden_units,), jnp.float32),
        jnp.zeros((hidden_units, hidden_units), jnp.float32),
        jnp.zeros((hidden_units,), jnp.float32),
        jnp.zeros((features, hidden_units), jnp.float32),
    )
    totals, tend_rows = lax.scan(visit_row, empty_sums, (rows_in, rows_up))
    tendency = jnp.moveaxis(tend_rows, 0, 1).reshape(fields, lev_total, lat_rows, lon_count)
    return (tendency, totals)


def on_device(
    prognostic, cotangent, damping, in_scale, w_in, b_in, w_mid, b_mid, w_out, wave_order, lat_order
):
    fields, lev_dev, lat_dev, lon_count = prognostic.shape
    lat_width = lax.axis_size("lat")
    wave_dev = wave_order.shape[0] // lat_width
    lat_total = lat_order.shape[0]
    my_index = lax.axis_index("lat")
    own_waves = lax.dynamic_slice_in_dim(wave_order, my_index * wave_dev, wave_dev)
    to_fourier = fourier_forward(wave_order, lon_count)
    fourier = jnp.einsum("jkn,fean->jkfea", to_fourier, prognostic, precision=lax.Precision.HIGHEST)
    fourier = lax.all_to_all(fourier, "lat", split_axis=0, concat_axis=4, tiled=True)
    colatitude = math.pi * (lat_order.astype(jnp.float32) + 0.5) / lat_total
    spectral, synthesized = spectral_pass(own_waves, colatitude, fourier, damping)
    upstream = lax.all_to_all(cotangent, "lev", split_axis=2, concat_axis=1, tiled=True)
    from_fourier = fourier_inverse(wave_order, lon_count)
    row_modes = lax.all_to_all(synthesized, "lat", split_axis=4, concat_axis=0, tiled=True)
    filtered = jnp.einsum(
        "jkfea,jkn->fean", row_modes, from_fourier, precision=lax.Precision.HIGHEST
    )
    lev_index = lax.axis_index("lev")
    local_scale = lax.dynamic_slice_in_dim(in_scale, lev_index * lev_dev, lev_dev, 1)
    local_inputs = (filtered * local_scale[:, :, None, None]).astype(jnp.bfloat16)
    inputs = lax.all_to_all(local_inputs, "lev", split_axis=2, concat_axis=1, tiled=True)
    tend_cols, totals = physics_rows(inputs, upstream, w_in, b_in, w_mid, b_mid, w_out)
    tendency = lax.all_to_all(tend_cols, "lev", split_axis=1, concat_axis=2, tiled=True)
    new_state = filtered + tendency.astype(jnp.float32)
    grad_scale = 1.0 / math.sqrt(lat_total * lon_count)
    summed = lax.psum(
        (
            totals[0] * grad_scale,
            totals[1] * grad_scale,
            totals[2] * grad_scale,
            totals[3] * grad_scale,
            totals[4] * grad_scale,
        ),
        ("lat", "lev"),
    )
    return (new_state, spectral, summed[0], summed[1], summed[2], summed[3], summed[4])


LANES = 128
half_lanes = LANES // 2
feature_rows = 16
bf16 = jnp.bfloat16
f32 = jnp.float32
forward_type = f32
inverse_type = bf16
state_type = bf16
grad_type = bf16
row_gap = 8


def contract_last(left, right):
    return lax.dot_general(left, right, (((1,), (1,)), ((), ())), preferred_element_type=f32)


def matmul(left, right):
    return lax.dot_general(left, right, (((1,), (0,)), ((), ())), preferred_element_type=f32)


def half_turn_sincos(half_angle):
    square = half_angle * half_angle
    sine = 0.0
    cosine = 0.0
    for power in range(6, -1, -1):
        sine = sine * square + (-1.0) ** power / math.factorial(2 * power + 1)
        cosine = cosine * square + (-1.0) ** power / math.factorial(2 * power)
    sine = sine * half_angle
    return 2.0 * sine * cosine, 1.0 - 2.0 * sine * sine


def turn_sincos(product, period):
    reduced = product - period * jnp.floor(product * (1.0 / period) + 0.5)
    return half_turn_sincos(reduced * (math.pi / period))


def lower_lanes(shape):
    return lax.broadcasted_iota(jnp.int32, shape, len(shape) - 1) < half_lanes


def split_pair(value):
    high = value.astype(bf16)
    return high, (value - high.astype(f32)).astype(bf16)


def polar_sine(lat_index, lat_total):
    nearest = jnp.minimum(lat_index, (lat_total - 1.0) - lat_index)
    return half_turn_sincos((nearest + 0.5) * (0.5 * math.pi / lat_total))


def wave_columns(waves_ref):
    return jnp.broadcast_to(waves_ref[...].astype(f32), (LANES, waves_ref.shape[1])).T


def fill_trig(waves_ref, trig_ref, wave_dev):
    wave_total = waves_ref.shape[1]
    lon_count = trig_ref.shape[1]
    waves = wave_columns(waves_ref)
    lane = lax.broadcasted_iota(jnp.int32, waves.shape, 1).astype(f32)
    sine, cosine = turn_sincos(waves * lane, float(lon_count))
    step_sine, step_cosine = turn_sincos(waves * float(LANES), float(lon_count))
    for tile in range(lon_count // LANES):
        lanes = pl.ds(tile * LANES, LANES)
        cosines = split_pair(cosine)
        sines = split_pair(-sine)
        for owner in range(wave_total // wave_dev):
            rows = slice(owner * wave_dev, (owner + 1) * wave_dev)
            for part in range(2):
                place = 2 * part * wave_total + 2 * owner * wave_dev
                trig_ref[pl.ds(place, wave_dev), lanes] = cosines[part][rows]
                trig_ref[pl.ds(place + wave_dev, wave_dev), lanes] = sines[part][rows]
        cosine, sine = (
            cosine * step_cosine - sine * step_sine,
            sine * step_cosine + cosine * step_sine,
        )


def forward_kernel(lats_ref, waves_ref, prog_hbm, send_ref, trig_ref, prog_ref, prog_sem):
    prog_copy = pltpu.make_async_copy(prog_hbm, prog_ref, prog_sem)
    prog_copy.start()
    lat_width, half_rows, _ = send_ref.shape
    wave_total = waves_ref.shape[1]
    rows_total, lon_count = prog_ref.shape
    lat_total = lats_ref.shape[0]
    lat_dev = lat_total // lat_width
    fill_trig(waves_ref, trig_ref, wave_total // lat_width)
    prog_copy.wait()
    prog_high, prog_low = split_pair(prog_ref[...])
    modes = contract_last(
        jnp.concatenate([prog_high, prog_low], axis=0), trig_ref[pl.ds(0, 2 * wave_total), :]
    )
    modes = modes[:rows_total] + modes[rows_total:] + contract_last(
        prog_high, trig_ref[pl.ds(2 * wave_total, 2 * wave_total), :]
    )
    first_row = lax.axis_index("lat") * lat_dev
    row = lax.broadcasted_iota(jnp.int32, (lat_dev, LANES), 0)
    lat_index = jnp.zeros((lat_dev, LANES), f32)
    for at in range(lat_dev):
        lat_index = jnp.where(row == at, lats_ref[first_row + at].astype(f32), lat_index)
    weight = polar_sine(lat_index, lat_total)[0] * (math.pi / lat_total / lon_count)
    weight = jnp.concatenate([weight] * (half_rows // lat_dev), axis=0)
    lower = lower_lanes((half_rows, LANES))
    for tile in range(lat_width // 2):
        first = modes[:half_rows, tile * LANES : (tile + 1) * LANES] * weight
        second = modes[half_rows:, tile * LANES : (tile + 1) * LANES] * weight
        send_ref[2 * tile] = jnp.where(lower, first, pltpu.roll(second, half_lanes, 1)).astype(
            send_ref.dtype
        )
        send_ref[2 * tile + 1] = jnp.where(
            lower, pltpu.roll(first, half_lanes, 1), second
        ).astype(send_ref.dtype)


def cotangent_kernel(cot_ref, *rest):
    *cot_refs, cot_scratch = rest
    lev_width = len(cot_refs)
    row_share = cot_refs[0].shape[0]
    lat_dev = lev_width * row_share
    rows_total, lon_count = cot_ref.shape
    cot_scratch[...] = jnp.zeros_like(cot_scratch)
    cot_all = cot_ref[...].astype(f32)
    tiles = lon_count // LANES
    for tile in range(tiles):
        cot_scratch[tile, pl.ds(0, rows_total), :] = cot_all[:, tile * LANES : (tile + 1) * LANES]
    for shift in range(lev_width):
        dest = (lax.axis_index("lev") + shift) % lev_width
        for share in range(row_share):
            for tile in range(tiles):
                picked = cot_scratch[tile, pl.ds(dest * row_share + share, feature_rows, stride=lat_dev), :]
                cot_refs[shift][share, :, pl.ds(tile * LANES, LANES)] = picked.astype(bf16)


def level_major(pair, fields, lev_dev):
    return pair % lev_dev * fields + pair // lev_dev


def table_kernel(damping_ref, lats_ref, waves_ref, out_ref, damp_ref, root_ref, scratch, columns):
    pair_count, degrees, _ = out_ref.shape
    rows = pair_count
    lat_total = lats_ref.shape[1]
    columns[...] = wave_columns(waves_ref)
    first_wave = pl.multiple_of(lax.axis_index("lat") * 2 * rows, 2 * rows)
    orders = jnp.where(
        lower_lanes((rows, LANES)),
        columns[pl.ds(first_wave, rows), :],
        columns[pl.ds(first_wave + rows, rows), :],
    )
    fields, lev_dev = damping_ref.shape
    pairs = fields * lev_dev
    degree = lax.broadcasted_iota(jnp.int32, (pairs, degrees), 1).astype(f32)
    degree_ratio = degree * (degree + 1.0) * (1.0 / (degrees * (degrees - 1.0)))
    root = jnp.sqrt(2.0 * degree + 1.0)
    row = lax.broadcasted_iota(jnp.int32, (pairs, degrees), 0)
    strength = jnp.zeros((pairs, degrees), f32)
    for pair in range(pairs):
        at = level_major(pair, fields, lev_dev)
        strength = jnp.where(row == at, damping_ref[pair // lev_dev, pair % lev_dev], strength)
    damp = root / (1.0 + strength * (degree_ratio * degree_ratio))
    damp_ref[...] = jnp.concatenate([damp, damp, damp, damp], axis=0)
    waves = columns[pl.ds(first_wave, 2 * rows), :]
    waves = jnp.concatenate([waves] * (degrees // LANES), axis=1)
    root_ref[...] = jnp.where(waves == 0.0, 1.0, 2.0) * root[:1]
    lat_row = lats_ref[...].astype(f32)
    lat_index = jnp.broadcast_to(jnp.concatenate([lat_row, lat_row], axis=1), (rows, LANES))
    sine, cosine = polar_sine(lat_index, lat_total)
    cosine = jnp.where(2.0 * lat_index < lat_total - 1.0, cosine, -cosine)
    index = lax.broadcasted_iota(jnp.int32, (rows, degrees), 1).astype(f32)
    index = jnp.maximum(index, 1.0)
    ratios = 0.5 * jnp.log((2.0 * index + 1.0) / (2.0 * index))
    position = lax.broadcasted_iota(jnp.int32, (rows, degrees), 1)
    counted = position.astype(f32)
    totals = []
    for half in range(2):
        wave = jnp.broadcast_to(orders[:, half * half_lanes : half * half_lanes + 1], (rows, degrees))
        chosen = jnp.where((position > 0) & (counted <= wave), ratios, 0.0)
        totals.append(jnp.broadcast_to(jnp.sum(chosen, axis=1, keepdims=True), (rows, LANES)))
    diagonal_log = jnp.where(lower_lanes((rows, LANES)), totals[0], totals[1])
    log_shift = (
        diagonal_log
        - 0.5 * math.log(2.0)
        - 0.5 * jnp.log(2.0 * orders + 1.0)
        + orders * jnp.log(sine)
    )
    squared = orders * orders
    limit = 2.0**rescale_bits
    zero = jnp.zeros((rows, LANES), f32)

    def visit(block, carried):
        latest, before, previous_root, log_shift = carried
        scale = jnp.exp(log_shift)
        for offset in range(8):
            degree_int = block * 8 + offset
            degree = jnp.full((rows, LANES), degree_int, jnp.int32).astype(f32)
            gap = degree * degree - squared
            inverse_root = lax.rsqrt(jnp.maximum(gap, 1.0))
            root = gap * inverse_root
            recurred = inverse_root * (
                (2.0 * degree - 1.0) * cosine * latest - previous_root * before
            )
            newest = jnp.where(gap > 0.0, recurred, jnp.where(gap == 0.0, 1.0, 0.0))
            scratch[pl.ds(degree_int * (rows + row_gap), rows), :] = newest * scale
            before = latest
            latest = newest
            previous_root = jnp.maximum(root, 0.0)
        too_large = jnp.abs(latest) > limit
        factor = jnp.where(too_large, 1.0 / limit, 1.0)
        log_shift = log_shift + jnp.where(too_large, rescale_bits * math.log(2.0), 0.0)
        return latest * factor, before * factor, previous_root, log_shift

    lax.fori_loop(0, degrees // 8, visit, (zero, zero, zero, log_shift))

    def unpack(pair, carried):
        high, low = split_pair(scratch[pl.ds(pair, degrees, stride=rows + row_gap), :])
        out_ref[pair, :, pl.ds(0, LANES)] = high
        out_ref[pair, :, pl.ds(LANES, LANES)] = low
        return carried

    lax.fori_loop(0, pair_count, unpack, 0)


def spectral_kernel(
    recv_ref, table_ref, damp_ref, root_ref, spec_ref, send_ref, modes, sums, picked
):
    pair_count, degrees, _ = table_ref.shape
    wave_dev = 2 * pair_count
    lat_width, half_rows, _ = recv_ref.shape
    lat_total = LANES // 2
    lat_dev = lat_total // lat_width
    _, _, lev_dev, fields, _ = spec_ref.shape
    pairs = fields * lev_dev
    half_pairs = pairs // 2
    pitch = wave_dev + row_gap
    received = recv_ref[...].astype(f32)
    upper_rows = lax.broadcasted_iota(jnp.int32, (LANES, LANES), 0) % wave_dev >= pair_count
    for index in range(half_pairs):
        stacked = [
            received[source, index * lat_dev : (index + 1) * lat_dev] for source in range(lat_width)
        ]
        stacked.append(jnp.zeros((LANES - lat_total, LANES), f32))
        turned = jnp.concatenate(stacked, axis=0).T
        turned = jnp.where(upper_rows, pltpu.roll(turned, half_lanes, 1), turned)
        for half in range(2):
            for part in range(2):
                start = (half * 2 + part) * wave_dev
                place = (part * pairs + level_major(half * half_pairs + index, fields, lev_dev)) * pitch
                modes[pl.ds(place, wave_dev), :] = turned[start : start + wave_dev]
    damp = damp_ref[...]
    count = 2 * pairs
    for pair in range(pair_count):
        first = modes[pl.ds(pair, count, stride=pitch), :]
        second = modes[pl.ds(pair + pair_count, count, stride=pitch), :]
        stacked = jnp.concatenate([first, second], axis=0)
        table = table_ref[pair]
        if recv_ref.dtype == f32:
            stacked = jnp.concatenate(split_pair(stacked), axis=0)
        else:
            stacked = stacked.astype(bf16)
        coeffs = contract_last(jnp.concatenate([stacked, stacked], axis=1), table)
        if recv_ref.dtype == f32:
            coeffs = coeffs[: 2 * count] + coeffs[2 * count :]
        coeffs = coeffs * damp
        shape = (2, lev_dev, fields, degrees)
        spec_ref[pair] = coeffs[:count].reshape(shape)
        spec_ref[pair + pair_count] = coeffs[count:].reshape(shape)
        rooted = jnp.concatenate(
            [
                coeffs[:count] * root_ref[pl.ds(pair, 1), :],
                coeffs[count:] * root_ref[pl.ds(pair + pair_count, 1), :],
            ],
            axis=0,
        )
        synth = matmul(jnp.concatenate(split_pair(rooted), axis=0), table)
        synth = synth[: 2 * count] + synth[2 * count :]
        synth = synth[:, :LANES] + synth[:, LANES:]
        sums[pl.ds(pair, count, stride=pitch), :] = synth[:count]
        sums[pl.ds(pair + pair_count, count, stride=pitch), :] = synth[count:]
    owners = send_ref.shape[0] // (2 * pairs)
    lower = lower_lanes((owners, LANES))
    share = lat_total // owners
    blank = jnp.zeros((owners, LANES), f32)
    sent_rows = 2 * pairs

    def put(row, value):
        high = value.astype(bf16).astype(f32)
        picked[pl.ds(lat_total + row, owners, stride=sent_rows), :] = high
        picked[pl.ds(lat_total + pairs + row, owners, stride=sent_rows), :] = value - high

    for index in range(half_pairs):
        blocks = []
        for half in range(2):
            for part in range(2):
                place = (part * pairs + level_major(half * half_pairs + index, fields, lev_dev)) * pitch
                blocks.append(sums[pl.ds(place, wave_dev), :])
        stacked = jnp.concatenate(blocks, axis=0)
        stacked = jnp.where(upper_rows, pltpu.roll(stacked, half_lanes, 1), stacked)
        picked[pl.ds(0, lat_total), :] = stacked.T[:lat_total]
        even = picked[pl.ds(0, owners, stride=share), :]
        odd = picked[pl.ds(1, owners, stride=share), :]
        put(index, jnp.where(lower, even, pltpu.roll(odd, half_lanes, 1)))
        put(half_pairs + index, jnp.where(lower, pltpu.roll(even, half_lanes, 1), odd))
    send_ref[...] = picked[pl.ds(lat_total, owners * sent_rows), :].astype(send_ref.dtype)


def weights_kernel(
    wave_dev, scale_ref, waves_ref, select_ref, w_in_ref, b_in_ref, w_mid_ref, w_out_ref, b_mid_ref, gather_ref,
    trig_ref, in_ref, mid_ref, mid_turned_ref, out_ref, out_turned_ref, scale_out_ref, bias_row_ref, select_out_ref,
):
    bias_row_ref[...] = b_mid_ref[...]
    select_out_ref[...] = gather_ref[...]
    fill_trig(waves_ref, trig_ref, wave_dev)
    hidden = w_mid_ref.shape[0]
    padded = select_ref.shape[0]
    spare = feature_rows * 3 // 4
    select = select_ref[...]
    bias = jnp.broadcast_to(b_in_ref[...], (padded, hidden))
    high = bias.astype(bf16).astype(f32)
    row = lax.broadcasted_iota(jnp.int32, (padded, hidden), 0)
    spread = matmul(select, w_in_ref[...])
    spread = jnp.where(row == spare, high, jnp.where(row == spare + 1, bias - high, spread))
    in_ref[...] = spread.T.astype(bf16)
    mid_ref[...] = w_mid_ref[...]
    mid_turned_ref[...] = w_mid_ref[...].astype(f32).T.astype(bf16)
    spread_out = matmul(select, w_out_ref[...])
    out_ref[...] = spread_out.astype(bf16)
    out_turned_ref[...] = spread_out.T.astype(bf16)
    fields, lev_total = scale_ref.shape
    lev_dev = spare // fields
    row = lax.broadcasted_iota(jnp.int32, (padded, LANES), 0)
    scales = jnp.zeros((padded, LANES), f32)
    for field in range(fields):
        for level in range(lev_total):
            place = level // lev_dev * feature_rows + field * lev_dev + level % lev_dev
            scales = jnp.where(row == place, scale_ref[field, level], scales)
    scale_out_ref[...] = scales


def columns_kernel(lev_width, recv_ref, *rest):
    cot_refs, rest = rest[:lev_width], rest[lev_width:]
    trig_ref, w_in_ref, w_mid_ref, w_turned_ref, *rest = rest
    w_out_ref, w_out_turned_ref, scale_ref, bias_row_ref, *rest = rest
    state_refs, rest = rest[:lev_width], rest[lev_width:]
    keep_ref, give_ref, packed, modes, cot_all, state_all, grad_in, grad_mid, grad_out, grad_bias, bias_ref = rest
    row_share, _, lon_count = cot_refs[0].shape
    lat_width = recv_ref.shape[0] // lev_width
    level = lax.axis_index("lev")
    padded = lev_width * feature_rows
    hidden = w_mid_ref.shape[0]
    spare = feature_rows * 3 // 4
    lower = lower_lanes((padded, LANES))
    feature = lax.broadcasted_iota(jnp.int32, (lev_width, feature_rows, LANES), 1)

    def unfold(owner):
        piece = recv_ref[pl.ds(owner * lev_width, lev_width)].astype(f32)
        rest = pltpu.roll(piece, spare, 1)
        return [
            jnp.where(feature < spare, part[:, :feature_rows], 0.0).reshape(padded, LANES)
            for part in (piece, rest)
        ]

    for tile in range(lat_width // 2):
        firsts, seconds = unfold(2 * tile), unfold(2 * tile + 1)
        lanes = pl.ds(tile * LANES, LANES)
        for part, (first, second) in enumerate(zip(firsts, seconds)):
            rows = pl.ds(part * padded, padded)
            modes[0, rows, lanes] = jnp.where(lower, first, pltpu.roll(second, half_lanes, 1)).astype(bf16)
            modes[1, rows, lanes] = jnp.where(lower, pltpu.roll(first, half_lanes, 1), second).astype(bf16)
    for shift in range(lev_width):
        source = (level + (lev_width - shift)) % lev_width
        start = pl.multiple_of(source * feature_rows, feature_rows)
        cot_all[:, pl.ds(start, feature_rows), :] = cot_refs[shift][...]
    grad_in[...] = jnp.zeros_like(grad_in)
    grad_mid[...] = jnp.zeros_like(grad_mid)
    grad_out[...] = jnp.zeros_like(grad_out)
    grad_bias[...] = jnp.zeros_like(grad_bias)
    bias_ref[...] = jnp.broadcast_to(bias_row_ref[...], (LANES, hidden)).T
    width = 6 * LANES
    while lon_count % width:
        width //= 2
    blocks = lon_count // width

    def visit(block, carried):
        share = block // blocks
        lanes = pl.ds(pl.multiple_of(block % blocks * width, width), width)
        half = trig_ref.shape[0] // 2
        filtered = matmul(modes[share], trig_ref[pl.ds(0, half), lanes])
        filtered = filtered[:padded] + filtered[padded:]
        filtered += matmul(modes[share, :padded], trig_ref[pl.ds(half, half), lanes])
        row = lax.broadcasted_iota(jnp.int32, (padded, width), 0)
        scaled = filtered * jnp.concatenate([scale_ref[...]] * (width // LANES), axis=1)
        inputs = jnp.where((row == spare) | (row == spare + 1), 1.0, scaled).astype(bf16)
        upstream = cot_all[share, :, lanes]
        pre_in = matmul(w_in_ref[...], inputs)
        gate = 0.5 + 0.5 * jnp.tanh(0.5 * pre_in)
        active = pre_in * gate
        slope_in = gate + active * (1.0 - gate)
        hidden_in = active.astype(bf16)
        bias = jnp.concatenate([bias_ref[...]] * (width // LANES), axis=1)
        pre_mid = matmul(w_mid_ref[...], hidden_in) + bias
        gate = 0.5 + 0.5 * jnp.tanh(0.5 * pre_mid)
        active = pre_mid * gate
        slope_mid = gate + active * (1.0 - gate)
        hidden_mid = active.astype(bf16)
        tendency = matmul(w_out_ref[...], hidden_mid).astype(bf16).astype(f32)
        state_all[share, :, lanes] = (filtered + tendency).astype(state_all.dtype)
        delta = matmul(w_out_turned_ref[...], upstream) * slope_mid
        delta_mid = delta.astype(bf16)
        grad_out[...] += contract_last(upstream, hidden_mid)
        grad_mid[...] += contract_last(delta_mid, hidden_in)
        total = delta[:, :LANES]
        for tile in range(1, width // LANES):
            total = total + delta[:, tile * LANES : (tile + 1) * LANES]
        grad_bias[...] += total
        delta_in = (matmul(w_turned_ref[...], delta_mid) * slope_in).astype(bf16)
        grad_in[...] += contract_last(inputs, delta_in)
        return carried

    lax.fori_loop(0, row_share * blocks, visit, 0)
    for shift in range(lev_width):
        dest = (level + shift) % lev_width
        start = pl.multiple_of(dest * feature_rows, feature_rows)
        for share in range(row_share):
            for tile in range(lon_count // LANES):
                place = (share * (lon_count // LANES) + tile) * feature_rows
                state_refs[shift][pl.ds(place, feature_rows), :] = state_all[
                    share, pl.ds(start, feature_rows), pl.ds(tile * LANES, LANES)
                ]
    bias_row = lax.dot_general(
        jnp.ones((8, LANES), f32), grad_bias[...], (((1,), (1,)), ((), ())),
        precision=lax.Precision.HIGHEST, preferred_element_type=f32,
    )[:1]
    row = lax.broadcasted_iota(jnp.int32, (padded, hidden), 0)
    first_rows = jnp.where(row == spare + 1, jnp.broadcast_to(bias_row, (padded, hidden)), grad_in[...])
    total_rows = hidden + 2 * padded
    for tile in range(hidden // LANES):
        lanes = slice(tile * LANES, (tile + 1) * LANES)
        start = tile * total_rows
        packed[pl.ds(start, hidden), :] = grad_mid[:, lanes]
        packed[pl.ds(start + hidden, padded), :] = first_rows[:, lanes]
        packed[pl.ds(start + hidden + padded, padded), :] = grad_out[:, lanes]
    half_rows = packed.shape[0] // 2
    side = lax.axis_index("lat") % 2
    keep_ref[...] = packed[pl.ds(pl.multiple_of(side * half_rows, 16), half_rows), :]
    give_ref[...] = packed[pl.ds(pl.multiple_of((1 - side) * half_rows, 16), half_rows), :].astype(
        give_ref.dtype
    )


def part_rows(index, ref):
    count = ref.shape[0]
    return pl.ds(pl.multiple_of(index * count, 16), count)


def plane_scatter_kernel(keep_ref, recv_ref, rest_ref, *send_refs):
    chip = lax.axis_index("lat") // 2
    for offset, ref in enumerate((rest_ref, *send_refs)):
        rows = part_rows(chip ^ offset, ref)
        ref[...] = (keep_ref[rows, :] + recv_ref[rows, :].astype(f32)).astype(ref.dtype)


def plane_sum_kernel(keep_ref, *rest):
    *recv_refs, out_ref = rest
    total = keep_ref[...]
    for ref in recv_refs:
        total = total + ref[...].astype(f32)
    out_ref[...] = total.astype(out_ref.dtype)


def reduce_kernel(grad_scale, *refs):
    *part_refs, out_ref, ordered = refs
    width = len(part_refs)
    level = lax.axis_index("lev")
    for shift, ref in enumerate(part_refs):
        ordered[(level + (width - shift)) % width] = ref[...]
    total = ordered[0].astype(f32)
    for source in range(1, width):
        total = total + ordered[source].astype(f32)
    out_ref[...] = (total * grad_scale).astype(bf16)


def plane_gather_kernel(*refs):
    *part_refs, out_ref = refs
    chip = lax.axis_index("lat") // 2
    for offset, ref in enumerate(part_refs):
        out_ref[part_rows(chip ^ offset, ref), :] = ref[...]


def state_kernel(row_share, *refs):
    *recv_refs, out_ref, scratch = refs
    lev_width = len(recv_refs)
    lat_dev = lev_width * row_share
    pairs = out_ref.shape[0] // lat_dev
    tiles = out_ref.shape[1] // LANES
    for shift, ref in enumerate(recv_refs):
        source = (lax.axis_index("lev") + (lev_width - shift)) % lev_width
        first = ref.shape[0] - row_share * tiles * feature_rows
        for share in range(row_share):
            for tile in range(tiles):
                place = first + (share * tiles + tile) * feature_rows
                rows = ref[pl.ds(place, feature_rows), :].astype(f32)[:pairs]
                scratch[tile, pl.ds(source * row_share + share, pairs, stride=lat_dev), :] = rows
    for tile in range(tiles):
        out_ref[:, pl.ds(tile * LANES, LANES)] = scratch[tile]


def unpack_kernel(own, packed_ref, select_ref, *rest):
    *rest, in_rows, bin_row, mid_rows, bmid_row, out_rows, sems = rest
    outputs = rest[-5:]
    hidden, width = mid_rows.shape
    padded = select_ref.shape[1]
    spare = feature_rows * 3 // 4
    total_rows = hidden + 2 * padded
    select = select_ref[...]
    side = lax.axis_index("lat") % 2
    half = side if own else 1 - side
    columns = pl.ds(pl.multiple_of(half * width, width), width)
    for tile in range(width // LANES):
        lanes = pl.ds(tile * LANES, LANES)
        start = tile * total_rows
        mid_rows[:, lanes] = packed_ref[pl.ds(start, hidden), :].astype(f32)
        rows = packed_ref[pl.ds(start + hidden, padded), :]
        wide = rows.astype(f32)
        bin_row[:, lanes] = wide[spare : spare + 1]
        bmid_row[:, lanes] = wide[spare + 1 : spare + 2]
        in_rows[:, lanes] = matmul(select, rows)
        out_rows[:, lanes] = matmul(select, packed_ref[pl.ds(start + hidden + padded, padded), :])
    copies = [
        pltpu.make_async_copy(rows, output.at[:, columns], sems.at[at])
        for at, (rows, output) in enumerate(
            zip((in_rows, bin_row, mid_rows, bmid_row, out_rows), outputs)
        )
    ]
    for copy in copies:
        copy.start()
    for copy in copies:
        copy.wait()


def shaped(shape, kind=f32):
    return jax.ShapeDtypeStruct(shape, kind)


def room(mib):
    return pltpu.CompilerParams(vmem_limit_bytes=mib << 20)


def kept(shape, kind=f32):
    return pltpu.VMEM(shape, kind)


def near(array):
    return pltpu.with_memory_space_constraint(array, pltpu.VMEM)


def far(array):
    return pltpu.with_memory_space_constraint(array, pltpu.HBM)


def cost(flops, moved):
    return pl.CostEstimate(flops=flops, transcendentals=0, bytes_accessed=moved)


def rotate(pieces, width):
    moved = [pieces[0]]
    for shift in range(1, width):
        route = [(source, (source + shift) % width) for source in range(width)]
        moved.append(lax.ppermute(pieces[shift], "lev", route))
    return moved


def on_device_fast(
    prognostic, cotangent, damping, in_scale, w_in, b_in, w_mid, b_mid, w_out, wave_order, lat_order
):
    fields, lev_dev, lat_dev, lon_count = prognostic.shape
    lat_width = lax.axis_size("lat")
    lev_width = lax.axis_size("lev")
    wave_total = wave_order.shape[0]
    wave_dev = wave_total // lat_width
    lat_total = lat_order.shape[0]
    pairs = fields * lev_dev
    row_share = lat_dev // lev_width
    hidden, features = w_in.shape
    padded = lev_width * feature_rows
    owners = lat_width * lev_width
    pair_count = wave_dev // 2
    lev_total = lev_dev * lev_width

    select = np.zeros((features, padded), np.float32)
    for field in range(fields):
        for level in range(lev_total):
            place = level // lev_dev * feature_rows + field * lev_dev + level % lev_dev
            select[field * lev_total + level, place] = 1.0
    spread_select = jnp.asarray(select.T, bf16)
    select = jnp.asarray(select, bf16)

    smem = pl.BlockSpec(memory_space=pltpu.SMEM)
    hbm = pl.BlockSpec(memory_space=pltpu.HBM)
    vmem = pl.BlockSpec(memory_space=pltpu.VMEM)
    wave_row = wave_order.reshape(1, wave_total)
    piece = (row_share, feature_rows, lon_count)
    send = pl.pallas_call(
        forward_kernel,
        in_specs=[smem, vmem, hbm],
        out_shape=kept((lat_width, pairs * lat_dev // 2, LANES), forward_type),
        scratch_shapes=[
            pltpu.VMEM((4 * wave_total, lon_count), bf16),
            pltpu.VMEM((pairs * lat_dev, lon_count), f32),
            pltpu.SemaphoreType.DMA(()),
        ],
        compiler_params=room(16),
        name="forward",
    )(far(lat_order), far(wave_row), far(prognostic.reshape(pairs * lat_dev, lon_count)))
    cot_pieces = pl.pallas_call(
        cotangent_kernel,
        out_shape=[kept(piece, bf16)] * lev_width,
        scratch_shapes=[pltpu.VMEM((lon_count // LANES, feature_rows * lat_dev, LANES), f32)],
        cost_estimate=cost(2000000, 1 << 19),
        compiler_params=room(8),
        name="cotangent",
    )(far(cotangent.reshape(pairs * lat_dev, lon_count)))
    received = lax.all_to_all(send, "lat", split_axis=0, concat_axis=0, tiled=True)
    received, cot_pieces = lax.optimization_barrier((received, cot_pieces))
    upstream = rotate(cot_pieces, lev_width)
    table, damp, roots = pl.pallas_call(
        table_kernel,
        in_specs=[smem, vmem, vmem],
        out_shape=(
            kept((pair_count, TRUNC, 2 * LANES), bf16),
            kept((4 * pairs, TRUNC)),
            kept((wave_dev, TRUNC)),
        ),
        scratch_shapes=[
            pltpu.VMEM((TRUNC * (pair_count + row_gap), LANES), f32),
            pltpu.VMEM((wave_total, LANES), f32),
        ],
        cost_estimate=cost(8000000, 1 << 20),
        compiler_params=room(16),
        name="legendre",
    )(far(damping), far(lat_order.reshape(1, lat_total)), far(wave_row))
    spectral, modes_send = pl.pallas_call(
        spectral_kernel,
        out_shape=(
            pltpu.HBM((wave_dev, 2, lev_dev, fields, TRUNC), f32),
            kept((owners * 2 * pairs, LANES), bf16),
        ),
        scratch_shapes=[
            pltpu.VMEM((2 * pairs * (wave_dev + row_gap), LANES), f32),
            pltpu.VMEM((2 * pairs * (wave_dev + row_gap), LANES), f32),
            pltpu.VMEM((lat_total + owners * 2 * pairs, LANES), f32),
        ],
        compiler_params=room(16),
        name="spectral",
    )(*map(near, (received, table, damp, roots)))
    both = ("lat", "lev")
    modes = lax.all_to_all(
        modes_send.reshape(owners, 2 * pairs, LANES), both, split_axis=0, concat_axis=0, tiled=True
    )
    *prepared, chosen = pl.pallas_call(
        functools.partial(weights_kernel, wave_dev),
        out_shape=(
            kept((4 * wave_total, lon_count), bf16),
            kept((hidden, padded), bf16),
            kept((hidden, hidden), bf16),
            kept((hidden, hidden), bf16),
            kept((padded, hidden), bf16),
            kept((hidden, padded), bf16),
            kept((padded, LANES)),
            kept((1, hidden)),
            kept((features, padded), bf16),
        ),
        in_specs=[smem] + [vmem] * 8,
        cost_estimate=cost(4000000, 1 << 20),
        compiler_params=room(12),
        name="weights",
    )(
        far(in_scale),
        far(wave_row),
        far(spread_select),
        far(w_in.T),
        far(b_in.reshape(1, hidden)),
        far(w_mid),
        far(w_out),
        far(b_mid.reshape(1, hidden)),
        far(select),
    )
    total_rows = hidden + 2 * padded
    packed_rows = total_rows * (hidden // LANES)
    state_rows = row_share * feature_rows * (lon_count // LANES)
    *state_pieces, keep, give = pl.pallas_call(
        functools.partial(columns_kernel, lev_width),
        out_shape=(
            *([kept((state_rows, LANES), state_type)] * lev_width),
            kept((packed_rows // 2, LANES)),
            kept((packed_rows // 2, LANES), grad_type),
        ),
        scratch_shapes=[
            pltpu.VMEM((packed_rows, LANES), f32),
            pltpu.VMEM((row_share, 2 * padded, 2 * wave_total), bf16),
            pltpu.VMEM((row_share, padded, lon_count), bf16),
            pltpu.VMEM((row_share, padded, lon_count), state_type),
            pltpu.VMEM((padded, hidden), f32),
            pltpu.VMEM((hidden, hidden), f32),
            pltpu.VMEM((padded, hidden), f32),
            pltpu.VMEM((hidden, LANES), f32),
            pltpu.VMEM((hidden, LANES), f32),
        ],
        compiler_params=room(24),
        name="columns",
    )(
        *map(near, (modes, *upstream, *prepared))
    )
    chips = lat_width // 2
    quarter = packed_rows // lat_width
    partner = [(at, at ^ 1) for at in range(lat_width)]
    routes = [[(at, at ^ (2 * offset)) for at in range(lat_width)] for offset in range(1, chips)]
    taken = lax.ppermute(give, "lat", partner)
    rest, *sends = pl.pallas_call(
        plane_scatter_kernel,
        out_shape=(
            kept((quarter, LANES)),
            *([kept((quarter, LANES), grad_type)] * (chips - 1)),
        ),
        compiler_params=room(8),
        name="plane_scatter",
    )(near(keep), near(taken))
    taken = [lax.ppermute(send, "lat", route) for send, route in zip(sends, routes)]
    taken, state = lax.optimization_barrier((taken, rotate(state_pieces, lev_width)))
    mine = pl.pallas_call(
        plane_sum_kernel,
        out_shape=kept((quarter, LANES), grad_type),
        compiler_params=room(8),
        name="plane_sum",
    )(*map(near, (rest, *taken)))
    grad_scale = 1.0 / math.sqrt(lat_total * lon_count)
    joined = pl.pallas_call(
        functools.partial(reduce_kernel, grad_scale),
        out_shape=kept((quarter, LANES), grad_type),
        scratch_shapes=[pltpu.VMEM((lev_width, quarter, LANES), grad_type)],
        compiler_params=room(8),
        name="reduce",
    )(*map(near, rotate([mine] * lev_width, lev_width)))
    new_state = pl.pallas_call(
        functools.partial(state_kernel, row_share),
        out_shape=pltpu.HBM((pairs * lat_dev, lon_count), f32),
        scratch_shapes=[pltpu.VMEM((lon_count // LANES, pairs * lat_dev, LANES), f32)],
        cost_estimate=cost(2000000, 1 << 19),
        compiler_params=room(8),
        name="state",
    )(*map(near, state))
    joined, new_state = lax.optimization_barrier((joined, new_state))
    parts = [joined] + [lax.ppermute(joined, "lat", route) for route in routes]
    joined = pl.pallas_call(
        plane_gather_kernel,
        out_shape=kept((packed_rows // 2, LANES), grad_type),
        compiler_params=room(8),
        name="plane_gather",
    )(*map(near, parts))
    other = lax.ppermute(joined, "lat", partner)
    shapes = ((features, hidden), (1, hidden), (hidden, hidden), (1, hidden), (features, hidden))

    def unpack(own, half, *filled):
        return pl.pallas_call(
            functools.partial(unpack_kernel, own),
            in_specs=[vmem, vmem] + [hbm] * len(filled),
            out_shape=[pltpu.HBM(shape, f32) for shape in shapes],
            out_specs=[hbm] * len(shapes),
            scratch_shapes=[pltpu.VMEM((rows, columns // 2), f32) for rows, columns in shapes]
            + [pltpu.SemaphoreType.DMA((len(shapes),))],
            input_output_aliases={2 + at: at for at in range(len(filled))},
            cost_estimate=cost(2000000, 1 << 19),
            compiler_params=room(8),
            name="unpack",
        )(near(half), near(chosen), *filled)

    grad_in, grad_bin, grad_mid, grad_bmid, grad_out = unpack(False, other, *unpack(True, joined))
    return (
        new_state.reshape(fields, lev_dev, lat_dev, lon_count),
        spectral.transpose(0, 1, 3, 2, 4),
        grad_in.T,
        grad_bin.reshape(hidden),
        grad_mid,
        grad_bmid.reshape(hidden),
        grad_out,
    )


def fits_fast(mesh, prognostic, w_in, wave_order, lat_order):
    lat_width, lev_width = mesh.shape["lat"], mesh.shape["lev"]
    fields, lev_total, lat_total, lon_count = prognostic.shape
    hidden = w_in.shape[0]
    pairs = fields * lev_total // lev_width
    lat_dev = lat_total // lat_width
    wave_dev = wave_order.shape[0] // lat_width
    packed_rows = (hidden + 2 * lev_width * feature_rows) * (hidden // LANES)
    return (
        2 * lat_total == LANES
        and 4 * wave_dev == LANES
        and lat_dev == 8
        and lat_dev == 2 * lev_width
        and pairs == feature_rows * 3 // 4
        and lon_count % LANES == 0
        and hidden % LANES == 0
        and packed_rows % (16 * lat_width * lev_width) == 0
        and lat_width & (lat_width - 1) == 0
        and lat_width > 2
        and lev_width & (lev_width - 1) == 0
    )


def solution(mesh):
    def run(*arguments):
        prognostic, w_in, wave_order, lat_order = (arguments[at] for at in (0, 4, 9, 10))
        fast = fits_fast(mesh, prognostic, w_in, wave_order, lat_order)
        return shard(mesh, on_device_fast if fast else on_device)(*arguments)

    return run


def shard(mesh, body):
    return jax.shard_map(
        body,
        mesh=mesh,
        in_specs=(
            P(None, "lev", "lat", None),
            P(None, "lev", "lat", None),
            P(None, "lev"),
            P(),
            P(),
            P(),
            P(),
            P(),
            P(),
            P(),
            P(),
        ),
        out_specs=(
            P(None, "lev", "lat", None),
            P("lat", None, None, "lev", None),
            P(),
            P(),
            P(),
            P(),
            P(),
        ),
        check_vma=False,
    )
```

```python
import functools
import math

import jax
import jax.numpy as jnp
import numpy as np
from jax import lax
from jax.experimental import pallas as pl
from jax.experimental.pallas import tpu as pltpu
from jax.sharding import PartitionSpec as P

TRUNC = 256


block_rows = 32
rescale_bits = 40.0


def legendre_setup(own_waves, colatitude):
    float_type = colatitude.dtype
    all_orders = jnp.arange(TRUNC, dtype=jnp.int32)
    factor_index = jnp.arange(1, TRUNC, dtype=jnp.int32).astype(float_type)
    ratios = 0.5 * jnp.log((2.0 * factor_index + 1.0) / (2.0 * factor_index))
    totals = jnp.concatenate([jnp.zeros((1,), float_type), jnp.cumsum(ratios)])
    matches = own_waves[:, None] == all_orders[None, :]
    diagonal_log = jnp.sum(jnp.where(matches, totals[None, :], 0.0), axis=1) - 0.5 * math.log(2.0)
    orders = own_waves.astype(float_type)
    log_shift = diagonal_log[:, None] + orders[:, None] * jnp.log(jnp.sin(colatitude))[None, :]
    empty_rows = jnp.zeros_like(log_shift)
    return (empty_rows, empty_rows, log_shift)


def legendre_rows(recurrence, first_degree, orders, cosine):
    latest, before, log_shift = recurrence
    rescale_limit = 2.0**rescale_bits
    squared_order = orders * orders
    table_rows = []
    for offset in range(block_rows):
        degree = (first_degree + offset).astype(cosine.dtype)
        upper_coef = jnp.sqrt(
            jnp.maximum(4.0 * degree * degree - 1.0, 0.0)
            / jnp.maximum(degree * degree - squared_order, 1.0)
        )
        lower_num = jnp.maximum((degree - 1.0) * (degree - 1.0) - squared_order, 0.0)
        lower_coef = jnp.sqrt(
            lower_num / jnp.maximum(4.0 * (degree - 1.0) * (degree - 1.0) - 1.0, 1.0)
        )
        recurred = upper_coef[:, None] * (cosine[None, :] * latest - lower_coef[:, None] * before)
        diagonal_start = jnp.where(degree == orders, 1.0, 0.0)[:, None] * jnp.ones_like(latest)
        newest = jnp.where((degree > orders)[:, None], recurred, diagonal_start)
        too_large = jnp.abs(newest) > rescale_limit
        factor = jnp.where(too_large, 1.0 / rescale_limit, 1.0)
        newest = newest * factor
        latest = latest * factor
        log_shift = log_shift + jnp.where(too_large, rescale_bits * math.log(2.0), 0.0)
        table_rows.append(newest * jnp.exp(log_shift))
        before = latest
        latest = newest
    return ((latest, before, log_shift), jnp.stack(table_rows, axis=1))


def spectral_pass(own_waves, colatitude, fourier, damping):
    float_type = fourier.dtype
    lat_total = colatitude.shape[0]
    weight = math.pi / lat_total * jnp.sin(colatitude)
    cosine = jnp.cos(colatitude)
    orders = own_waves.astype(float_type)
    weighted = fourier * weight
    degree_norm = 1.0 / (TRUNC * (TRUNC - 1.0))

    def visit_block(carried, first_degree):
        recurrence, grid_sum = carried
        recurrence, legendre_table = legendre_rows(recurrence, first_degree, orders, cosine)
        coeffs = jnp.einsum(
            "jbn,jkfen->jkfeb", legendre_table, weighted, precision=lax.Precision.HIGHEST
        )
        degree = (first_degree + jnp.arange(block_rows, dtype=jnp.int32)).astype(float_type)
        degree_ratio = degree * (degree + 1.0) * degree_norm
        coeffs = coeffs / (1.0 + damping[:, :, None] * (degree_ratio * degree_ratio)[None, None, :])
        grid_sum = grid_sum + jnp.einsum(
            "jbn,jkfeb->jkfen", legendre_table, coeffs, precision=lax.Precision.HIGHEST
        )
        return ((recurrence, grid_sum), coeffs)

    starts = jnp.arange(0, TRUNC, block_rows, dtype=jnp.int32)
    initial = (legendre_setup(own_waves, colatitude), jnp.zeros_like(fourier))
    (recurrence, synthesized), blocks = lax.scan(visit_block, initial, starts)
    waves, two, fields, levels = fourier.shape[:4]
    coeffs = jnp.moveaxis(blocks, 0, 4).reshape(waves, two, fields, levels, TRUNC)
    return (coeffs, synthesized)


def fourier_angles(wave_order, lon_count):
    points = jnp.arange(lon_count, dtype=jnp.int32)
    phase_index = wave_order[:, None] * points[None, :] % lon_count
    return phase_index.astype(jnp.float32) * (2.0 * math.pi / lon_count)


def fourier_forward(wave_order, lon_count):
    angles = fourier_angles(wave_order, lon_count)
    return jnp.stack([jnp.cos(angles), -jnp.sin(angles)], axis=1) / lon_count


def fourier_inverse(wave_order, lon_count):
    angles = fourier_angles(wave_order, lon_count)
    weights = jnp.where(wave_order == 0, 1.0, 2.0)[:, None, None]
    return weights * jnp.stack([jnp.cos(angles), -jnp.sin(angles)], axis=1)


def silu_slope(value):
    sigmoid_value = jax.nn.sigmoid(value)
    return sigmoid_value * (1.0 + value * (1.0 - sigmoid_value))


def column_physics(inputs, upstream, w_in, b_in, w_mid, b_mid, w_out):
    pre_in = jnp.dot(w_in, inputs, preferred_element_type=jnp.float32) + b_in[:, None]
    hidden_in = jax.nn.silu(pre_in).astype(jnp.bfloat16)
    pre_mid = jnp.dot(w_mid, hidden_in, preferred_element_type=jnp.float32) + b_mid[:, None]
    hidden_mid = jax.nn.silu(pre_mid).astype(jnp.bfloat16)
    tendency = jnp.dot(w_out, hidden_mid, preferred_element_type=jnp.float32).astype(jnp.bfloat16)
    grad_out = jnp.dot(upstream, hidden_mid.T, preferred_element_type=jnp.float32)
    back_mid = jnp.dot(w_out.T, upstream, preferred_element_type=jnp.float32)
    delta_mid = (back_mid * silu_slope(pre_mid)).astype(jnp.bfloat16)
    grad_mid = jnp.dot(delta_mid, hidden_in.T, preferred_element_type=jnp.float32)
    grad_bmid = jnp.sum(delta_mid.astype(jnp.float32), axis=1)
    back_in = jnp.dot(w_mid.T, delta_mid, preferred_element_type=jnp.float32)
    delta_in = (back_in * silu_slope(pre_in)).astype(jnp.bfloat16)
    grad_in = jnp.dot(delta_in, inputs.T, preferred_element_type=jnp.float32)
    grad_bin = jnp.sum(delta_in.astype(jnp.float32), axis=1)
    return (tendency, (grad_in, grad_bin, grad_mid, grad_bmid, grad_out))


def physics_rows(inputs, upstream, w_in, b_in, w_mid, b_mid, w_out):
    fields, lev_total, lat_rows, lon_count = inputs.shape
    features = fields * lev_total
    hidden_units = w_in.shape[0]
    rows_in = jnp.moveaxis(inputs.reshape(features, lat_rows, lon_count), 1, 0)
    rows_up = jnp.moveaxis(upstream.reshape(features, lat_rows, lon_count), 1, 0)

    def visit_row(totals, row_pair):
        tendency, gradients = column_physics(
            row_pair[0], row_pair[1], w_in, b_in, w_mid, b_mid, w_out
        )
        return (jax.tree.map(jnp.add, totals, gradients), tendency)

    empty_sums = (
        jnp.zeros((hidden_units, features), jnp.float32),
        jnp.zeros((hidden_units,), jnp.float32),
        jnp.zeros((hidden_units, hidden_units), jnp.float32),
        jnp.zeros((hidden_units,), jnp.float32),
        jnp.zeros((features, hidden_units), jnp.float32),
    )
    totals, tend_rows = lax.scan(visit_row, empty_sums, (rows_in, rows_up))
    tendency = jnp.moveaxis(tend_rows, 0, 1).reshape(fields, lev_total, lat_rows, lon_count)
    return (tendency, totals)


def on_device(
    prognostic, cotangent, damping, in_scale, w_in, b_in, w_mid, b_mid, w_out, wave_order, lat_order
):
    fields, lev_dev, lat_dev, lon_count = prognostic.shape
    lat_width = lax.axis_size("lat")
    wave_dev = wave_order.shape[0] // lat_width
    lat_total = lat_order.shape[0]
    my_index = lax.axis_index("lat")
    own_waves = lax.dynamic_slice_in_dim(wave_order, my_index * wave_dev, wave_dev)
    to_fourier = fourier_forward(wave_order, lon_count)
    fourier = jnp.einsum("jkn,fean->jkfea", to_fourier, prognostic, precision=lax.Precision.HIGHEST)
    fourier = lax.all_to_all(fourier, "lat", split_axis=0, concat_axis=4, tiled=True)
    colatitude = math.pi * (lat_order.astype(jnp.float32) + 0.5) / lat_total
    spectral, synthesized = spectral_pass(own_waves, colatitude, fourier, damping)
    upstream = lax.all_to_all(cotangent, "lev", split_axis=2, concat_axis=1, tiled=True)
    from_fourier = fourier_inverse(wave_order, lon_count)
    row_modes = lax.all_to_all(synthesized, "lat", split_axis=4, concat_axis=0, tiled=True)
    filtered = jnp.einsum(
        "jkfea,jkn->fean", row_modes, from_fourier, precision=lax.Precision.HIGHEST
    )
    lev_index = lax.axis_index("lev")
    local_scale = lax.dynamic_slice_in_dim(in_scale, lev_index * lev_dev, lev_dev, 1)
    local_inputs = (filtered * local_scale[:, :, None, None]).astype(jnp.bfloat16)
    inputs = lax.all_to_all(local_inputs, "lev", split_axis=2, concat_axis=1, tiled=True)
    tend_cols, totals = physics_rows(inputs, upstream, w_in, b_in, w_mid, b_mid, w_out)
    tendency = lax.all_to_all(tend_cols, "lev", split_axis=1, concat_axis=2, tiled=True)
    new_state = filtered + tendency.astype(jnp.float32)
    grad_scale = 1.0 / math.sqrt(lat_total * lon_count)
    summed = lax.psum(
        (
            totals[0] * grad_scale,
            totals[1] * grad_scale,
            totals[2] * grad_scale,
            totals[3] * grad_scale,
            totals[4] * grad_scale,
        ),
        ("lat", "lev"),
    )
    return (new_state, spectral, summed[0], summed[1], summed[2], summed[3], summed[4])


LANES = 128
half_lanes = LANES // 2
feature_rows = 16
bf16 = jnp.bfloat16
f32 = jnp.float32
forward_type = f32
inverse_type = bf16
state_type = bf16
grad_type = bf16
row_gap = 8


def contract_last(left, right):
    return lax.dot_general(left, right, (((1,), (1,)), ((), ())), preferred_element_type=f32)


def matmul(left, right):
    return lax.dot_general(left, right, (((1,), (0,)), ((), ())), preferred_element_type=f32)


def half_turn_sincos(half_angle):
    square = half_angle * half_angle
    sine = 0.0
    cosine = 0.0
    for power in range(6, -1, -1):
        sine = sine * square + (-1.0) ** power / math.factorial(2 * power + 1)
        cosine = cosine * square + (-1.0) ** power / math.factorial(2 * power)
    sine = sine * half_angle
    return 2.0 * sine * cosine, 1.0 - 2.0 * sine * sine


def turn_sincos(product, period):
    reduced = product - period * jnp.floor(product * (1.0 / period) + 0.5)
    return half_turn_sincos(reduced * (math.pi / period))


def lower_lanes(shape):
    return lax.broadcasted_iota(jnp.int32, shape, len(shape) - 1) < half_lanes


def split_pair(value):
    high = value.astype(bf16)
    return high, (value - high.astype(f32)).astype(bf16)


def polar_sine(lat_index, lat_total):
    nearest = jnp.minimum(lat_index, (lat_total - 1.0) - lat_index)
    return half_turn_sincos((nearest + 0.5) * (0.5 * math.pi / lat_total))


def wave_columns(waves_ref):
    return jnp.broadcast_to(waves_ref[...].astype(f32), (LANES, waves_ref.shape[1])).T


def fill_trig(waves_ref, trig_ref, wave_dev):
    wave_total = waves_ref.shape[1]
    lon_count = trig_ref.shape[1]
    waves = wave_columns(waves_ref)
    lane = lax.broadcasted_iota(jnp.int32, waves.shape, 1).astype(f32)
    sine, cosine = turn_sincos(waves * lane, float(lon_count))
    step_sine, step_cosine = turn_sincos(waves * float(LANES), float(lon_count))
    for tile in range(lon_count // LANES):
        lanes = pl.ds(tile * LANES, LANES)
        cosines = split_pair(cosine)
        sines = split_pair(-sine)
        for owner in range(wave_total // wave_dev):
            rows = slice(owner * wave_dev, (owner + 1) * wave_dev)
            for part in range(2):
                place = 2 * part * wave_total + 2 * owner * wave_dev
                trig_ref[pl.ds(place, wave_dev), lanes] = cosines[part][rows]
                trig_ref[pl.ds(place + wave_dev, wave_dev), lanes] = sines[part][rows]
        cosine, sine = (
            cosine * step_cosine - sine * step_sine,
            sine * step_cosine + cosine * step_sine,
        )


def forward_kernel(lats_ref, waves_ref, prog_hbm, send_ref, trig_ref, prog_ref, prog_sem):
    prog_copy = pltpu.make_async_copy(prog_hbm, prog_ref, prog_sem)
    prog_copy.start()
    lat_width, half_rows, _ = send_ref.shape
    wave_total = waves_ref.shape[1]
    rows_total, lon_count = prog_ref.shape
    lat_total = lats_ref.shape[0]
    lat_dev = lat_total // lat_width
    fill_trig(waves_ref, trig_ref, wave_total // lat_width)
    prog_copy.wait()
    prog_high, prog_low = split_pair(prog_ref[...])
    modes = contract_last(
        jnp.concatenate([prog_high, prog_low], axis=0), trig_ref[pl.ds(0, 2 * wave_total), :]
    )
    modes = modes[:rows_total] + modes[rows_total:] + contract_last(
        prog_high, trig_ref[pl.ds(2 * wave_total, 2 * wave_total), :]
    )
    first_row = lax.axis_index("lat") * lat_dev
    row = lax.broadcasted_iota(jnp.int32, (lat_dev, LANES), 0)
    lat_index = jnp.zeros((lat_dev, LANES), f32)
    for at in range(lat_dev):
        lat_index = jnp.where(row == at, lats_ref[first_row + at].astype(f32), lat_index)
    weight = polar_sine(lat_index, lat_total)[0] * (math.pi / lat_total / lon_count)
    weight = jnp.concatenate([weight] * (half_rows // lat_dev), axis=0)
    lower = lower_lanes((half_rows, LANES))
    for tile in range(lat_width // 2):
        first = modes[:half_rows, tile * LANES : (tile + 1) * LANES] * weight
        second = modes[half_rows:, tile * LANES : (tile + 1) * LANES] * weight
        send_ref[2 * tile] = jnp.where(lower, first, pltpu.roll(second, half_lanes, 1)).astype(
            send_ref.dtype
        )
        send_ref[2 * tile + 1] = jnp.where(
            lower, pltpu.roll(first, half_lanes, 1), second
        ).astype(send_ref.dtype)


def cotangent_kernel(cot_ref, *rest):
    *cot_refs, cot_scratch = rest
    lev_width = len(cot_refs)
    row_share = cot_refs[0].shape[0]
    lat_dev = lev_width * row_share
    rows_total, lon_count = cot_ref.shape
    cot_scratch[...] = jnp.zeros_like(cot_scratch)
    cot_all = cot_ref[...].astype(f32)
    tiles = lon_count // LANES
    for tile in range(tiles):
        cot_scratch[tile, pl.ds(0, rows_total), :] = cot_all[:, tile * LANES : (tile + 1) * LANES]
    for shift in range(lev_width):
        dest = (lax.axis_index("lev") + shift) % lev_width
        for share in range(row_share):
            for tile in range(tiles):
                picked = cot_scratch[tile, pl.ds(dest * row_share + share, feature_rows, stride=lat_dev), :]
                cot_refs[shift][share, :, pl.ds(tile * LANES, LANES)] = picked.astype(bf16)


def level_major(pair, fields, lev_dev):
    return pair % lev_dev * fields + pair // lev_dev


def table_kernel(damping_ref, lats_ref, waves_ref, out_ref, damp_ref, root_ref, scratch, columns):
    pair_count, degrees, _ = out_ref.shape
    rows = pair_count
    lat_total = lats_ref.shape[1]
    columns[...] = wave_columns(waves_ref)
    first_wave = pl.multiple_of(lax.axis_index("lat") * 2 * rows, 2 * rows)
    orders = jnp.where(
        lower_lanes((rows, LANES)),
        columns[pl.ds(first_wave, rows), :],
        columns[pl.ds(first_wave + rows, rows), :],
    )
    fields, lev_dev = damping_ref.shape
    pairs = fields * lev_dev
    degree = lax.broadcasted_iota(jnp.int32, (pairs, degrees), 1).astype(f32)
    degree_ratio = degree * (degree + 1.0) * (1.0 / (degrees * (degrees - 1.0)))
    root = jnp.sqrt(2.0 * degree + 1.0)
    row = lax.broadcasted_iota(jnp.int32, (pairs, degrees), 0)
    strength = jnp.zeros((pairs, degrees), f32)
    for pair in range(pairs):
        at = level_major(pair, fields, lev_dev)
        strength = jnp.where(row == at, damping_ref[pair // lev_dev, pair % lev_dev], strength)
    damp = root / (1.0 + strength * (degree_ratio * degree_ratio))
    damp_ref[...] = jnp.concatenate([damp, damp, damp, damp], axis=0)
    waves = columns[pl.ds(first_wave, 2 * rows), :]
    waves = jnp.concatenate([waves] * (degrees // LANES), axis=1)
    root_ref[...] = jnp.where(waves == 0.0, 1.0, 2.0) * root[:1]
    lat_row = lats_ref[...].astype(f32)
    lat_index = jnp.broadcast_to(jnp.concatenate([lat_row, lat_row], axis=1), (rows, LANES))
    sine, cosine = polar_sine(lat_index, lat_total)
    cosine = jnp.where(2.0 * lat_index < lat_total - 1.0, cosine, -cosine)
    index = lax.broadcasted_iota(jnp.int32, (rows, degrees), 1).astype(f32)
    index = jnp.maximum(index, 1.0)
    ratios = 0.5 * jnp.log((2.0 * index + 1.0) / (2.0 * index))
    position = lax.broadcasted_iota(jnp.int32, (rows, degrees), 1)
    counted = position.astype(f32)
    totals = []
    for half in range(2):
        wave = jnp.broadcast_to(orders[:, half * half_lanes : half * half_lanes + 1], (rows, degrees))
        chosen = jnp.where((position > 0) & (counted <= wave), ratios, 0.0)
        totals.append(jnp.broadcast_to(jnp.sum(chosen, axis=1, keepdims=True), (rows, LANES)))
    diagonal_log = jnp.where(lower_lanes((rows, LANES)), totals[0], totals[1])
    log_shift = (
        diagonal_log
        - 0.5 * math.log(2.0)
        - 0.5 * jnp.log(2.0 * orders + 1.0)
        + orders * jnp.log(sine)
    )
    squared = orders * orders
    limit = 2.0**rescale_bits
    zero = jnp.zeros((rows, LANES), f32)

    def visit(block, carried):
        latest, before, previous_root, log_shift = carried
        scale = jnp.exp(log_shift)
        for offset in range(8):
            degree_int = block * 8 + offset
            degree = jnp.full((rows, LANES), degree_int, jnp.int32).astype(f32)
            gap = degree * degree - squared
            inverse_root = lax.rsqrt(jnp.maximum(gap, 1.0))
            root = gap * inverse_root
            recurred = inverse_root * (
                (2.0 * degree - 1.0) * cosine * latest - previous_root * before
            )
            newest = jnp.where(gap > 0.0, recurred, jnp.where(gap == 0.0, 1.0, 0.0))
            scratch[pl.ds(degree_int * (rows + row_gap), rows), :] = newest * scale
            before = latest
            latest = newest
            previous_root = jnp.maximum(root, 0.0)
        too_large = jnp.abs(latest) > limit
        factor = jnp.where(too_large, 1.0 / limit, 1.0)
        log_shift = log_shift + jnp.where(too_large, rescale_bits * math.log(2.0), 0.0)
        return latest * factor, before * factor, previous_root, log_shift

    lax.fori_loop(0, degrees // 8, visit, (zero, zero, zero, log_shift))

    def unpack(pair, carried):
        high, low = split_pair(scratch[pl.ds(pair, degrees, stride=rows + row_gap), :])
        out_ref[pair, :, pl.ds(0, LANES)] = high
        out_ref[pair, :, pl.ds(LANES, LANES)] = low
        return carried

    lax.fori_loop(0, pair_count, unpack, 0)


def spectral_kernel(
    recv_ref, table_ref, damp_ref, root_ref, spec_ref, send_ref, modes, sums, picked, rooted_ref
):
    pair_count, degrees, _ = table_ref.shape
    wave_dev = 2 * pair_count
    lat_width, half_rows, _ = recv_ref.shape
    lat_total = LANES // 2
    lat_dev = lat_total // lat_width
    _, _, lev_dev, fields, _ = spec_ref.shape
    pairs = fields * lev_dev
    half_pairs = pairs // 2
    pitch = wave_dev + row_gap
    received = recv_ref[...].astype(f32)
    upper_rows = lax.broadcasted_iota(jnp.int32, (LANES, LANES), 0) % wave_dev >= pair_count
    for index in range(half_pairs):
        stacked = [
            received[source, index * lat_dev : (index + 1) * lat_dev] for source in range(lat_width)
        ]
        stacked.append(jnp.zeros((LANES - lat_total, LANES), f32))
        turned = jnp.concatenate(stacked, axis=0).T
        turned = jnp.where(upper_rows, pltpu.roll(turned, half_lanes, 1), turned)
        for half in range(2):
            for part in range(2):
                start = (half * 2 + part) * wave_dev
                place = (part * pairs + level_major(half * half_pairs + index, fields, lev_dev)) * pitch
                modes[pl.ds(place, wave_dev), :] = turned[start : start + wave_dev]
    damp = damp_ref[...]
    count = 2 * pairs
    for pair in range(pair_count):
        first = modes[pl.ds(pair, count, stride=pitch), :]
        second = modes[pl.ds(pair + pair_count, count, stride=pitch), :]
        stacked = jnp.concatenate([first, second], axis=0)
        table = table_ref[pair]
        if recv_ref.dtype == f32:
            stacked = jnp.concatenate(split_pair(stacked), axis=0)
        else:
            stacked = stacked.astype(bf16)
        coeffs = contract_last(jnp.concatenate([stacked, stacked], axis=1), table)
        if recv_ref.dtype == f32:
            coeffs = coeffs[: 2 * count] + coeffs[2 * count :]
        coeffs = coeffs * damp
        shape = (2, lev_dev, fields, degrees)
        spec_ref[pair] = coeffs[:count].reshape(shape)
        spec_ref[pair + pair_count] = coeffs[count:].reshape(shape)
        rooted = jnp.concatenate(
            [
                coeffs[:count] * root_ref[pl.ds(pair, 1), :],
                coeffs[count:] * root_ref[pl.ds(pair + pair_count, 1), :],
            ],
            axis=0,
        )
        rooted_ref[pair] = jnp.concatenate(split_pair(rooted), axis=0)
    for pair in range(pair_count):
        synth = matmul(rooted_ref[pair], table_ref[pair])
        synth = synth[: 2 * count] + synth[2 * count :]
        synth = synth[:, :LANES] + synth[:, LANES:]
        sums[pl.ds(pair, count, stride=pitch), :] = synth[:count]
        sums[pl.ds(pair + pair_count, count, stride=pitch), :] = synth[count:]
    owners = send_ref.shape[0] // (2 * pairs)
    lower = lower_lanes((owners, LANES))
    share = lat_total // owners
    blank = jnp.zeros((owners, LANES), f32)
    sent_rows = 2 * pairs

    def put(row, value):
        high = value.astype(bf16).astype(f32)
        picked[pl.ds(lat_total + row, owners, stride=sent_rows), :] = high
        picked[pl.ds(lat_total + pairs + row, owners, stride=sent_rows), :] = value - high

    for index in range(half_pairs):
        blocks = []
        for half in range(2):
            for part in range(2):
                place = (part * pairs + level_major(half * half_pairs + index, fields, lev_dev)) * pitch
                blocks.append(sums[pl.ds(place, wave_dev), :])
        stacked = jnp.concatenate(blocks, axis=0)
        stacked = jnp.where(upper_rows, pltpu.roll(stacked, half_lanes, 1), stacked)
        picked[pl.ds(0, lat_total), :] = stacked.T[:lat_total]
        even = picked[pl.ds(0, owners, stride=share), :]
        odd = picked[pl.ds(1, owners, stride=share), :]
        put(index, jnp.where(lower, even, pltpu.roll(odd, half_lanes, 1)))
        put(half_pairs + index, jnp.where(lower, pltpu.roll(even, half_lanes, 1), odd))
    send_ref[...] = picked[pl.ds(lat_total, owners * sent_rows), :].astype(send_ref.dtype)


def weights_kernel(
    wave_dev, scale_ref, waves_ref, select_ref, w_in_ref, b_in_ref, w_mid_ref, w_out_ref, b_mid_ref, gather_ref,
    trig_ref, in_ref, mid_ref, mid_turned_ref, out_ref, out_turned_ref, scale_out_ref, bias_row_ref, select_out_ref,
):
    bias_row_ref[...] = b_mid_ref[...]
    select_out_ref[...] = gather_ref[...]
    fill_trig(waves_ref, trig_ref, wave_dev)
    hidden = w_mid_ref.shape[0]
    padded = select_ref.shape[0]
    spare = feature_rows * 3 // 4
    select = select_ref[...]
    bias = jnp.broadcast_to(b_in_ref[...], (padded, hidden))
    high = bias.astype(bf16).astype(f32)
    row = lax.broadcasted_iota(jnp.int32, (padded, hidden), 0)
    spread = matmul(select, w_in_ref[...])
    spread = jnp.where(row == spare, high, jnp.where(row == spare + 1, bias - high, spread))
    in_ref[...] = spread.T.astype(bf16)
    mid_ref[...] = w_mid_ref[...]
    mid_turned_ref[...] = w_mid_ref[...].astype(f32).T.astype(bf16)
    spread_out = matmul(select, w_out_ref[...])
    out_ref[...] = spread_out.astype(bf16)
    out_turned_ref[...] = spread_out.T.astype(bf16)
    fields, lev_total = scale_ref.shape
    lev_dev = spare // fields
    row = lax.broadcasted_iota(jnp.int32, (padded, LANES), 0)
    scales = jnp.zeros((padded, LANES), f32)
    for field in range(fields):
        for level in range(lev_total):
            place = level // lev_dev * feature_rows + field * lev_dev + level % lev_dev
            scales = jnp.where(row == place, scale_ref[field, level], scales)
    scale_out_ref[...] = scales


def columns_kernel(lev_width, recv_ref, *rest):
    cot_refs, rest = rest[:lev_width], rest[lev_width:]
    trig_ref, w_in_ref, w_mid_ref, w_turned_ref, *rest = rest
    w_out_ref, w_out_turned_ref, scale_ref, bias_row_ref, *rest = rest
    state_refs, rest = rest[:lev_width], rest[lev_width:]
    keep_ref, give_ref, packed, modes, cot_all, state_all, grad_in, grad_mid, grad_out, grad_bias, bias_ref = rest
    row_share, _, lon_count = cot_refs[0].shape
    lat_width = recv_ref.shape[0] // lev_width
    level = lax.axis_index("lev")
    padded = lev_width * feature_rows
    hidden = w_mid_ref.shape[0]
    spare = feature_rows * 3 // 4
    lower = lower_lanes((padded, LANES))
    feature = lax.broadcasted_iota(jnp.int32, (lev_width, feature_rows, LANES), 1)

    def unfold(owner):
        piece = recv_ref[pl.ds(owner * lev_width, lev_width)].astype(f32)
        rest = pltpu.roll(piece, spare, 1)
        return [
            jnp.where(feature < spare, part[:, :feature_rows], 0.0).reshape(padded, LANES)
            for part in (piece, rest)
        ]

    for tile in range(lat_width // 2):
        firsts, seconds = unfold(2 * tile), unfold(2 * tile + 1)
        lanes = pl.ds(tile * LANES, LANES)
        for part, (first, second) in enumerate(zip(firsts, seconds)):
            rows = pl.ds(part * padded, padded)
            modes[0, rows, lanes] = jnp.where(lower, first, pltpu.roll(second, half_lanes, 1)).astype(bf16)
            modes[1, rows, lanes] = jnp.where(lower, pltpu.roll(first, half_lanes, 1), second).astype(bf16)
    for shift in range(lev_width):
        source = (level + (lev_width - shift)) % lev_width
        start = pl.multiple_of(source * feature_rows, feature_rows)
        cot_all[:, pl.ds(start, feature_rows), :] = cot_refs[shift][...]
    grad_in[...] = jnp.zeros_like(grad_in)
    grad_mid[...] = jnp.zeros_like(grad_mid)
    grad_out[...] = jnp.zeros_like(grad_out)
    grad_bias[...] = jnp.zeros_like(grad_bias)
    bias_ref[...] = jnp.broadcast_to(bias_row_ref[...], (LANES, hidden)).T
    width = 6 * LANES
    while lon_count % width:
        width //= 2
    blocks = lon_count // width

    def visit(block, carried):
        share = block // blocks
        lanes = pl.ds(pl.multiple_of(block % blocks * width, width), width)
        half = trig_ref.shape[0] // 2
        filtered = matmul(modes[share], trig_ref[pl.ds(0, half), lanes])
        filtered = filtered[:padded] + filtered[padded:]
        filtered += matmul(modes[share, :padded], trig_ref[pl.ds(half, half), lanes])
        row = lax.broadcasted_iota(jnp.int32, (padded, width), 0)
        scaled = filtered * jnp.concatenate([scale_ref[...]] * (width // LANES), axis=1)
        inputs = jnp.where((row == spare) | (row == spare + 1), 1.0, scaled).astype(bf16)
        upstream = cot_all[share, :, lanes]
        pre_in = matmul(w_in_ref[...], inputs)
        gate = 0.5 + 0.5 * jnp.tanh(0.5 * pre_in)
        active = pre_in * gate
        slope_in = gate + active * (1.0 - gate)
        hidden_in = active.astype(bf16)
        bias = jnp.concatenate([bias_ref[...]] * (width // LANES), axis=1)
        pre_mid = matmul(w_mid_ref[...], hidden_in) + bias
        gate = 0.5 + 0.5 * jnp.tanh(0.5 * pre_mid)
        active = pre_mid * gate
        slope_mid = gate + active * (1.0 - gate)
        hidden_mid = active.astype(bf16)
        tendency = matmul(w_out_ref[...], hidden_mid).astype(bf16).astype(f32)
        state_all[share, :, lanes] = (filtered + tendency).astype(state_all.dtype)
        delta = matmul(w_out_turned_ref[...], upstream) * slope_mid
        delta_mid = delta.astype(bf16)
        grad_out[...] += contract_last(upstream, hidden_mid)
        grad_mid[...] += contract_last(delta_mid, hidden_in)
        total = delta[:, :LANES]
        for tile in range(1, width // LANES):
            total = total + delta[:, tile * LANES : (tile + 1) * LANES]
        grad_bias[...] += total
        delta_in = (matmul(w_turned_ref[...], delta_mid) * slope_in).astype(bf16)
        grad_in[...] += contract_last(inputs, delta_in)
        return carried

    lax.fori_loop(0, row_share * blocks, visit, 0)
    for shift in range(lev_width):
        dest = (level + shift) % lev_width
        start = pl.multiple_of(dest * feature_rows, feature_rows)
        for share in range(row_share):
            for tile in range(lon_count // LANES):
                place = (share * (lon_count // LANES) + tile) * feature_rows
                state_refs[shift][pl.ds(place, feature_rows), :] = state_all[
                    share, pl.ds(start, feature_rows), pl.ds(tile * LANES, LANES)
                ]
    bias_row = lax.dot_general(
        jnp.ones((8, LANES), f32), grad_bias[...], (((1,), (1,)), ((), ())),
        precision=lax.Precision.HIGHEST, preferred_element_type=f32,
    )[:1]
    row = lax.broadcasted_iota(jnp.int32, (padded, hidden), 0)
    first_rows = jnp.where(row == spare + 1, jnp.broadcast_to(bias_row, (padded, hidden)), grad_in[...])
    total_rows = hidden + 2 * padded
    for tile in range(hidden // LANES):
        lanes = slice(tile * LANES, (tile + 1) * LANES)
        start = tile * total_rows
        packed[pl.ds(start, hidden), :] = grad_mid[:, lanes]
        packed[pl.ds(start + hidden, padded), :] = first_rows[:, lanes]
        packed[pl.ds(start + hidden + padded, padded), :] = grad_out[:, lanes]
    half_rows = packed.shape[0] // 2
    side = lax.axis_index("lat") % 2
    keep_ref[...] = packed[pl.ds(pl.multiple_of(side * half_rows, 16), half_rows), :]
    give_ref[...] = packed[pl.ds(pl.multiple_of((1 - side) * half_rows, 16), half_rows), :].astype(
        give_ref.dtype
    )


def part_rows(index, ref):
    count = ref.shape[0]
    return pl.ds(pl.multiple_of(index * count, 16), count)


def plane_scatter_kernel(keep_ref, recv_ref, rest_ref, *send_refs):
    chip = lax.axis_index("lat") // 2
    for offset, ref in enumerate((rest_ref, *send_refs)):
        rows = part_rows(chip ^ offset, ref)
        ref[...] = (keep_ref[rows, :] + recv_ref[rows, :].astype(f32)).astype(ref.dtype)


def plane_sum_kernel(keep_ref, *rest):
    *recv_refs, out_ref = rest
    total = keep_ref[...]
    for ref in recv_refs:
        total = total + ref[...].astype(f32)
    out_ref[...] = total.astype(out_ref.dtype)


def reduce_kernel(grad_scale, *refs):
    *part_refs, out_ref, ordered = refs
    width = len(part_refs)
    level = lax.axis_index("lev")
    for shift, ref in enumerate(part_refs):
        ordered[(level + (width - shift)) % width] = ref[...]
    total = ordered[0].astype(f32)
    for source in range(1, width):
        total = total + ordered[source].astype(f32)
    out_ref[...] = (total * grad_scale).astype(bf16)


def plane_gather_kernel(*refs):
    *part_refs, out_ref = refs
    chip = lax.axis_index("lat") // 2
    for offset, ref in enumerate(part_refs):
        out_ref[part_rows(chip ^ offset, ref), :] = ref[...]


def state_kernel(row_share, *refs):
    *recv_refs, out_ref, scratch = refs
    lev_width = len(recv_refs)
    lat_dev = lev_width * row_share
    pairs = out_ref.shape[0] // lat_dev
    tiles = out_ref.shape[1] // LANES
    for shift, ref in enumerate(recv_refs):
        source = (lax.axis_index("lev") + (lev_width - shift)) % lev_width
        first = ref.shape[0] - row_share * tiles * feature_rows
        for share in range(row_share):
            for tile in range(tiles):
                place = first + (share * tiles + tile) * feature_rows
                rows = ref[pl.ds(place, feature_rows), :].astype(f32)[:pairs]
                scratch[tile, pl.ds(source * row_share + share, pairs, stride=lat_dev), :] = rows
    for tile in range(tiles):
        out_ref[:, pl.ds(tile * LANES, LANES)] = scratch[tile]


def unpack_kernel(own, packed_ref, select_ref, *rest):
    *rest, in_rows, bin_row, mid_rows, bmid_row, out_rows, sems = rest
    outputs = rest[-5:]
    hidden, width = mid_rows.shape
    padded = select_ref.shape[1]
    spare = feature_rows * 3 // 4
    total_rows = hidden + 2 * padded
    select = select_ref[...]
    side = lax.axis_index("lat") % 2
    half = side if own else 1 - side
    columns = pl.ds(pl.multiple_of(half * width, width), width)
    for tile in range(width // LANES):
        lanes = pl.ds(tile * LANES, LANES)
        start = tile * total_rows
        mid_rows[:, lanes] = packed_ref[pl.ds(start, hidden), :].astype(f32)
        rows = packed_ref[pl.ds(start + hidden, padded), :]
        wide = rows.astype(f32)
        bin_row[:, lanes] = wide[spare : spare + 1]
        bmid_row[:, lanes] = wide[spare + 1 : spare + 2]
        in_rows[:, lanes] = matmul(select, rows)
        out_rows[:, lanes] = matmul(select, packed_ref[pl.ds(start + hidden + padded, padded), :])
    copies = [
        pltpu.make_async_copy(rows, output.at[:, columns], sems.at[at])
        for at, (rows, output) in enumerate(
            zip((in_rows, bin_row, mid_rows, bmid_row, out_rows), outputs)
        )
    ]
    for copy in copies:
        copy.start()
    for copy in copies:
        copy.wait()


def shaped(shape, kind=f32):
    return jax.ShapeDtypeStruct(shape, kind)


def room(mib):
    return pltpu.CompilerParams(vmem_limit_bytes=mib << 20)


def kept(shape, kind=f32):
    return pltpu.VMEM(shape, kind)


def near(array):
    return pltpu.with_memory_space_constraint(array, pltpu.VMEM)


def far(array):
    return pltpu.with_memory_space_constraint(array, pltpu.HBM)


def cost(flops, moved):
    return pl.CostEstimate(flops=flops, transcendentals=0, bytes_accessed=moved)


def rotate(pieces, width):
    moved = [pieces[0]]
    for shift in range(1, width):
        route = [(source, (source + shift) % width) for source in range(width)]
        moved.append(lax.ppermute(pieces[shift], "lev", route))
    return moved


def on_device_fast(
    prognostic, cotangent, damping, in_scale, w_in, b_in, w_mid, b_mid, w_out, wave_order, lat_order
):
    fields, lev_dev, lat_dev, lon_count = prognostic.shape
    lat_width = lax.axis_size("lat")
    lev_width = lax.axis_size("lev")
    wave_total = wave_order.shape[0]
    wave_dev = wave_total // lat_width
    lat_total = lat_order.shape[0]
    pairs = fields * lev_dev
    row_share = lat_dev // lev_width
    hidden, features = w_in.shape
    padded = lev_width * feature_rows
    owners = lat_width * lev_width
    pair_count = wave_dev // 2
    lev_total = lev_dev * lev_width

    select = np.zeros((features, padded), np.float32)
    for field in range(fields):
        for level in range(lev_total):
            place = level // lev_dev * feature_rows + field * lev_dev + level % lev_dev
            select[field * lev_total + level, place] = 1.0
    spread_select = jnp.asarray(select.T, bf16)
    select = jnp.asarray(select, bf16)

    smem = pl.BlockSpec(memory_space=pltpu.SMEM)
    hbm = pl.BlockSpec(memory_space=pltpu.HBM)
    vmem = pl.BlockSpec(memory_space=pltpu.VMEM)
    wave_row = wave_order.reshape(1, wave_total)
    piece = (row_share, feature_rows, lon_count)
    send = pl.pallas_call(
        forward_kernel,
        in_specs=[smem, vmem, hbm],
        out_shape=kept((lat_width, pairs * lat_dev // 2, LANES), forward_type),
        scratch_shapes=[
            pltpu.VMEM((4 * wave_total, lon_count), bf16),
            pltpu.VMEM((pairs * lat_dev, lon_count), f32),
            pltpu.SemaphoreType.DMA(()),
        ],
        compiler_params=room(16),
        name="forward",
    )(far(lat_order), far(wave_row), far(prognostic.reshape(pairs * lat_dev, lon_count)))
    cot_pieces = pl.pallas_call(
        cotangent_kernel,
        out_shape=[kept(piece, bf16)] * lev_width,
        scratch_shapes=[pltpu.VMEM((lon_count // LANES, feature_rows * lat_dev, LANES), f32)],
        cost_estimate=cost(2000000, 1 << 19),
        compiler_params=room(8),
        name="cotangent",
    )(far(cotangent.reshape(pairs * lat_dev, lon_count)))
    received = lax.all_to_all(send, "lat", split_axis=0, concat_axis=0, tiled=True)
    received, cot_pieces = lax.optimization_barrier((received, cot_pieces))
    upstream = rotate(cot_pieces, lev_width)
    table, damp, roots = pl.pallas_call(
        table_kernel,
        in_specs=[smem, vmem, vmem],
        out_shape=(
            kept((pair_count, TRUNC, 2 * LANES), bf16),
            kept((4 * pairs, TRUNC)),
            kept((wave_dev, TRUNC)),
        ),
        scratch_shapes=[
            pltpu.VMEM((TRUNC * (pair_count + row_gap), LANES), f32),
            pltpu.VMEM((wave_total, LANES), f32),
        ],
        cost_estimate=cost(8000000, 1 << 20),
        compiler_params=room(16),
        name="legendre",
    )(far(damping), far(lat_order.reshape(1, lat_total)), far(wave_row))
    spectral, modes_send = pl.pallas_call(
        spectral_kernel,
        out_shape=(
            pltpu.HBM((wave_dev, 2, lev_dev, fields, TRUNC), f32),
            kept((owners * 2 * pairs, LANES), bf16),
        ),
        scratch_shapes=[
            pltpu.VMEM((2 * pairs * (wave_dev + row_gap), LANES), f32),
            pltpu.VMEM((2 * pairs * (wave_dev + row_gap), LANES), f32),
            pltpu.VMEM((lat_total + owners * 2 * pairs, LANES), f32),
            pltpu.VMEM((pair_count, 8 * pairs, TRUNC), bf16),
        ],
        compiler_params=room(16),
        name="spectral",
    )(*map(near, (received, table, damp, roots)))
    both = ("lat", "lev")
    modes = lax.all_to_all(
        modes_send.reshape(owners, 2 * pairs, LANES), both, split_axis=0, concat_axis=0, tiled=True
    )
    *prepared, chosen = pl.pallas_call(
        functools.partial(weights_kernel, wave_dev),
        out_shape=(
            kept((4 * wave_total, lon_count), bf16),
            kept((hidden, padded), bf16),
            kept((hidden, hidden), bf16),
            kept((hidden, hidden), bf16),
            kept((padded, hidden), bf16),
            kept((hidden, padded), bf16),
            kept((padded, LANES)),
            kept((1, hidden)),
            kept((features, padded), bf16),
        ),
        in_specs=[smem] + [vmem] * 8,
        cost_estimate=cost(4000000, 1 << 20),
        compiler_params=room(12),
        name="weights",
    )(
        far(in_scale),
        far(wave_row),
        far(spread_select),
        far(w_in.T),
        far(b_in.reshape(1, hidden)),
        far(w_mid),
        far(w_out),
        far(b_mid.reshape(1, hidden)),
        far(select),
    )
    total_rows = hidden + 2 * padded
    packed_rows = total_rows * (hidden // LANES)
    state_rows = row_share * feature_rows * (lon_count // LANES)
    *state_pieces, keep, give = pl.pallas_call(
        functools.partial(columns_kernel, lev_width),
        out_shape=(
            *([kept((state_rows, LANES), state_type)] * lev_width),
            kept((packed_rows // 2, LANES)),
            kept((packed_rows // 2, LANES), grad_type),
        ),
        scratch_shapes=[
            pltpu.VMEM((packed_rows, LANES), f32),
            pltpu.VMEM((row_share, 2 * padded, 2 * wave_total), bf16),
            pltpu.VMEM((row_share, padded, lon_count), bf16),
            pltpu.VMEM((row_share, padded, lon_count), state_type),
            pltpu.VMEM((padded, hidden), f32),
            pltpu.VMEM((hidden, hidden), f32),
            pltpu.VMEM((padded, hidden), f32),
            pltpu.VMEM((hidden, LANES), f32),
            pltpu.VMEM((hidden, LANES), f32),
        ],
        compiler_params=room(24),
        name="columns",
    )(
        *map(near, (modes, *upstream, *prepared))
    )
    chips = lat_width // 2
    quarter = packed_rows // lat_width
    partner = [(at, at ^ 1) for at in range(lat_width)]
    routes = [[(at, at ^ (2 * offset)) for at in range(lat_width)] for offset in range(1, chips)]
    taken = lax.ppermute(give, "lat", partner)
    rest, *sends = pl.pallas_call(
        plane_scatter_kernel,
        out_shape=(
            kept((quarter, LANES)),
            *([kept((quarter, LANES), grad_type)] * (chips - 1)),
        ),
        compiler_params=room(8),
        name="plane_scatter",
    )(near(keep), near(taken))
    taken = [lax.ppermute(send, "lat", route) for send, route in zip(sends, routes)]
    taken, state = lax.optimization_barrier((taken, rotate(state_pieces, lev_width)))
    mine = pl.pallas_call(
        plane_sum_kernel,
        out_shape=kept((quarter, LANES), grad_type),
        compiler_params=room(8),
        name="plane_sum",
    )(*map(near, (rest, *taken)))
    grad_scale = 1.0 / math.sqrt(lat_total * lon_count)
    joined = pl.pallas_call(
        functools.partial(reduce_kernel, grad_scale),
        out_shape=kept((quarter, LANES), grad_type),
        scratch_shapes=[pltpu.VMEM((lev_width, quarter, LANES), grad_type)],
        compiler_params=room(8),
        name="reduce",
    )(*map(near, rotate([mine] * lev_width, lev_width)))
    new_state = pl.pallas_call(
        functools.partial(state_kernel, row_share),
        out_shape=pltpu.HBM((pairs * lat_dev, lon_count), f32),
        scratch_shapes=[pltpu.VMEM((lon_count // LANES, pairs * lat_dev, LANES), f32)],
        cost_estimate=cost(2000000, 1 << 19),
        compiler_params=room(8),
        name="state",
    )(*map(near, state))
    joined, new_state = lax.optimization_barrier((joined, new_state))
    parts = [joined] + [lax.ppermute(joined, "lat", route) for route in routes]
    joined = pl.pallas_call(
        plane_gather_kernel,
        out_shape=kept((packed_rows // 2, LANES), grad_type),
        compiler_params=room(8),
        name="plane_gather",
    )(*map(near, parts))
    other = lax.ppermute(joined, "lat", partner)
    shapes = ((features, hidden), (1, hidden), (hidden, hidden), (1, hidden), (features, hidden))

    def unpack(own, half, *filled):
        return pl.pallas_call(
            functools.partial(unpack_kernel, own),
            in_specs=[vmem, vmem] + [hbm] * len(filled),
            out_shape=[pltpu.HBM(shape, f32) for shape in shapes],
            out_specs=[hbm] * len(shapes),
            scratch_shapes=[pltpu.VMEM((rows, columns // 2), f32) for rows, columns in shapes]
            + [pltpu.SemaphoreType.DMA((len(shapes),))],
            input_output_aliases={2 + at: at for at in range(len(filled))},
            cost_estimate=cost(2000000, 1 << 19),
            compiler_params=room(8),
            name="unpack",
        )(near(half), near(chosen), *filled)

    grad_in, grad_bin, grad_mid, grad_bmid, grad_out = unpack(False, other, *unpack(True, joined))
    return (
        new_state.reshape(fields, lev_dev, lat_dev, lon_count),
        spectral.transpose(0, 1, 3, 2, 4),
        grad_in.T,
        grad_bin.reshape(hidden),
        grad_mid,
        grad_bmid.reshape(hidden),
        grad_out,
    )


def fits_fast(mesh, prognostic, w_in, wave_order, lat_order):
    lat_width, lev_width = mesh.shape["lat"], mesh.shape["lev"]
    fields, lev_total, lat_total, lon_count = prognostic.shape
    hidden = w_in.shape[0]
    pairs = fields * lev_total // lev_width
    lat_dev = lat_total // lat_width
    wave_dev = wave_order.shape[0] // lat_width
    packed_rows = (hidden + 2 * lev_width * feature_rows) * (hidden // LANES)
    return (
        2 * lat_total == LANES
        and 4 * wave_dev == LANES
        and lat_dev == 8
        and lat_dev == 2 * lev_width
        and pairs == feature_rows * 3 // 4
        and lon_count % LANES == 0
        and hidden % LANES == 0
        and packed_rows % (16 * lat_width * lev_width) == 0
        and lat_width & (lat_width - 1) == 0
        and lat_width > 2
        and lev_width & (lev_width - 1) == 0
    )


def solution(mesh):
    def run(*arguments):
        prognostic, w_in, wave_order, lat_order = (arguments[at] for at in (0, 4, 9, 10))
        fast = fits_fast(mesh, prognostic, w_in, wave_order, lat_order)
        return shard(mesh, on_device_fast if fast else on_device)(*arguments)

    return run


def shard(mesh, body):
    return jax.shard_map(
        body,
        mesh=mesh,
        in_specs=(
            P(None, "lev", "lat", None),
            P(None, "lev", "lat", None),
            P(None, "lev"),
            P(),
            P(),
            P(),
            P(),
            P(),
            P(),
            P(),
            P(),
        ),
        out_specs=(
            P(None, "lev", "lat", None),
            P("lat", None, None, "lev", None),
            P(),
            P(),
            P(),
            P(),
            P(),
        ),
        check_vma=False,
    )
```

```python
import functools
import math

import jax
import jax.numpy as jnp
import numpy as np
from jax import lax
from jax.experimental import pallas as pl
from jax.experimental.pallas import tpu as pltpu
from jax.sharding import PartitionSpec as P

TRUNC = 256


block_rows = 32
rescale_bits = 40.0


def legendre_setup(own_waves, colatitude):
    float_type = colatitude.dtype
    all_orders = jnp.arange(TRUNC, dtype=jnp.int32)
    factor_index = jnp.arange(1, TRUNC, dtype=jnp.int32).astype(float_type)
    ratios = 0.5 * jnp.log((2.0 * factor_index + 1.0) / (2.0 * factor_index))
    totals = jnp.concatenate([jnp.zeros((1,), float_type), jnp.cumsum(ratios)])
    matches = own_waves[:, None] == all_orders[None, :]
    diagonal_log = jnp.sum(jnp.where(matches, totals[None, :], 0.0), axis=1) - 0.5 * math.log(2.0)
    orders = own_waves.astype(float_type)
    log_shift = diagonal_log[:, None] + orders[:, None] * jnp.log(jnp.sin(colatitude))[None, :]
    empty_rows = jnp.zeros_like(log_shift)
    return (empty_rows, empty_rows, log_shift)


def legendre_rows(recurrence, first_degree, orders, cosine):
    latest, before, log_shift = recurrence
    rescale_limit = 2.0**rescale_bits
    squared_order = orders * orders
    table_rows = []
    for offset in range(block_rows):
        degree = (first_degree + offset).astype(cosine.dtype)
        upper_coef = jnp.sqrt(
            jnp.maximum(4.0 * degree * degree - 1.0, 0.0)
            / jnp.maximum(degree * degree - squared_order, 1.0)
        )
        lower_num = jnp.maximum((degree - 1.0) * (degree - 1.0) - squared_order, 0.0)
        lower_coef = jnp.sqrt(
            lower_num / jnp.maximum(4.0 * (degree - 1.0) * (degree - 1.0) - 1.0, 1.0)
        )
        recurred = upper_coef[:, None] * (cosine[None, :] * latest - lower_coef[:, None] * before)
        diagonal_start = jnp.where(degree == orders, 1.0, 0.0)[:, None] * jnp.ones_like(latest)
        newest = jnp.where((degree > orders)[:, None], recurred, diagonal_start)
        too_large = jnp.abs(newest) > rescale_limit
        factor = jnp.where(too_large, 1.0 / rescale_limit, 1.0)
        newest = newest * factor
        latest = latest * factor
        log_shift = log_shift + jnp.where(too_large, rescale_bits * math.log(2.0), 0.0)
        table_rows.append(newest * jnp.exp(log_shift))
        before = latest
        latest = newest
    return ((latest, before, log_shift), jnp.stack(table_rows, axis=1))


def spectral_pass(own_waves, colatitude, fourier, damping):
    float_type = fourier.dtype
    lat_total = colatitude.shape[0]
    weight = math.pi / lat_total * jnp.sin(colatitude)
    cosine = jnp.cos(colatitude)
    orders = own_waves.astype(float_type)
    weighted = fourier * weight
    degree_norm = 1.0 / (TRUNC * (TRUNC - 1.0))

    def visit_block(carried, first_degree):
        recurrence, grid_sum = carried
        recurrence, legendre_table = legendre_rows(recurrence, first_degree, orders, cosine)
        coeffs = jnp.einsum(
            "jbn,jkfen->jkfeb", legendre_table, weighted, precision=lax.Precision.HIGHEST
        )
        degree = (first_degree + jnp.arange(block_rows, dtype=jnp.int32)).astype(float_type)
        degree_ratio = degree * (degree + 1.0) * degree_norm
        coeffs = coeffs / (1.0 + damping[:, :, None] * (degree_ratio * degree_ratio)[None, None, :])
        grid_sum = grid_sum + jnp.einsum(
            "jbn,jkfeb->jkfen", legendre_table, coeffs, precision=lax.Precision.HIGHEST
        )
        return ((recurrence, grid_sum), coeffs)

    starts = jnp.arange(0, TRUNC, block_rows, dtype=jnp.int32)
    initial = (legendre_setup(own_waves, colatitude), jnp.zeros_like(fourier))
    (recurrence, synthesized), blocks = lax.scan(visit_block, initial, starts)
    waves, two, fields, levels = fourier.shape[:4]
    coeffs = jnp.moveaxis(blocks, 0, 4).reshape(waves, two, fields, levels, TRUNC)
    return (coeffs, synthesized)


def fourier_angles(wave_order, lon_count):
    points = jnp.arange(lon_count, dtype=jnp.int32)
    phase_index = wave_order[:, None] * points[None, :] % lon_count
    return phase_index.astype(jnp.float32) * (2.0 * math.pi / lon_count)


def fourier_forward(wave_order, lon_count):
    angles = fourier_angles(wave_order, lon_count)
    return jnp.stack([jnp.cos(angles), -jnp.sin(angles)], axis=1) / lon_count


def fourier_inverse(wave_order, lon_count):
    angles = fourier_angles(wave_order, lon_count)
    weights = jnp.where(wave_order == 0, 1.0, 2.0)[:, None, None]
    return weights * jnp.stack([jnp.cos(angles), -jnp.sin(angles)], axis=1)


def silu_slope(value):
    sigmoid_value = jax.nn.sigmoid(value)
    return sigmoid_value * (1.0 + value * (1.0 - sigmoid_value))


def column_physics(inputs, upstream, w_in, b_in, w_mid, b_mid, w_out):
    pre_in = jnp.dot(w_in, inputs, preferred_element_type=jnp.float32) + b_in[:, None]
    hidden_in = jax.nn.silu(pre_in).astype(jnp.bfloat16)
    pre_mid = jnp.dot(w_mid, hidden_in, preferred_element_type=jnp.float32) + b_mid[:, None]
    hidden_mid = jax.nn.silu(pre_mid).astype(jnp.bfloat16)
    tendency = jnp.dot(w_out, hidden_mid, preferred_element_type=jnp.float32).astype(jnp.bfloat16)
    grad_out = jnp.dot(upstream, hidden_mid.T, preferred_element_type=jnp.float32)
    back_mid = jnp.dot(w_out.T, upstream, preferred_element_type=jnp.float32)
    delta_mid = (back_mid * silu_slope(pre_mid)).astype(jnp.bfloat16)
    grad_mid = jnp.dot(delta_mid, hidden_in.T, preferred_element_type=jnp.float32)
    grad_bmid = jnp.sum(delta_mid.astype(jnp.float32), axis=1)
    back_in = jnp.dot(w_mid.T, delta_mid, preferred_element_type=jnp.float32)
    delta_in = (back_in * silu_slope(pre_in)).astype(jnp.bfloat16)
    grad_in = jnp.dot(delta_in, inputs.T, preferred_element_type=jnp.float32)
    grad_bin = jnp.sum(delta_in.astype(jnp.float32), axis=1)
    return (tendency, (grad_in, grad_bin, grad_mid, grad_bmid, grad_out))


def physics_rows(inputs, upstream, w_in, b_in, w_mid, b_mid, w_out):
    fields, lev_total, lat_rows, lon_count = inputs.shape
    features = fields * lev_total
    hidden_units = w_in.shape[0]
    rows_in = jnp.moveaxis(inputs.reshape(features, lat_rows, lon_count), 1, 0)
    rows_up = jnp.moveaxis(upstream.reshape(features, lat_rows, lon_count), 1, 0)

    def visit_row(totals, row_pair):
        tendency, gradients = column_physics(
            row_pair[0], row_pair[1], w_in, b_in, w_mid, b_mid, w_out
        )
        return (jax.tree.map(jnp.add, totals, gradients), tendency)

    empty_sums = (
        jnp.zeros((hidden_units, features), jnp.float32),
        jnp.zeros((hidden_units,), jnp.float32),
        jnp.zeros((hidden_units, hidden_units), jnp.float32),
        jnp.zeros((hidden_units,), jnp.float32),
        jnp.zeros((features, hidden_units), jnp.float32),
    )
    totals, tend_rows = lax.scan(visit_row, empty_sums, (rows_in, rows_up))
    tendency = jnp.moveaxis(tend_rows, 0, 1).reshape(fields, lev_total, lat_rows, lon_count)
    return (tendency, totals)


def on_device(
    prognostic, cotangent, damping, in_scale, w_in, b_in, w_mid, b_mid, w_out, wave_order, lat_order
):
    fields, lev_dev, lat_dev, lon_count = prognostic.shape
    lat_width = lax.axis_size("lat")
    wave_dev = wave_order.shape[0] // lat_width
    lat_total = lat_order.shape[0]
    my_index = lax.axis_index("lat")
    own_waves = lax.dynamic_slice_in_dim(wave_order, my_index * wave_dev, wave_dev)
    to_fourier = fourier_forward(wave_order, lon_count)
    fourier = jnp.einsum("jkn,fean->jkfea", to_fourier, prognostic, precision=lax.Precision.HIGHEST)
    fourier = lax.all_to_all(fourier, "lat", split_axis=0, concat_axis=4, tiled=True)
    colatitude = math.pi * (lat_order.astype(jnp.float32) + 0.5) / lat_total
    spectral, synthesized = spectral_pass(own_waves, colatitude, fourier, damping)
    upstream = lax.all_to_all(cotangent, "lev", split_axis=2, concat_axis=1, tiled=True)
    from_fourier = fourier_inverse(wave_order, lon_count)
    row_modes = lax.all_to_all(synthesized, "lat", split_axis=4, concat_axis=0, tiled=True)
    filtered = jnp.einsum(
        "jkfea,jkn->fean", row_modes, from_fourier, precision=lax.Precision.HIGHEST
    )
    lev_index = lax.axis_index("lev")
    local_scale = lax.dynamic_slice_in_dim(in_scale, lev_index * lev_dev, lev_dev, 1)
    local_inputs = (filtered * local_scale[:, :, None, None]).astype(jnp.bfloat16)
    inputs = lax.all_to_all(local_inputs, "lev", split_axis=2, concat_axis=1, tiled=True)
    tend_cols, totals = physics_rows(inputs, upstream, w_in, b_in, w_mid, b_mid, w_out)
    tendency = lax.all_to_all(tend_cols, "lev", split_axis=1, concat_axis=2, tiled=True)
    new_state = filtered + tendency.astype(jnp.float32)
    grad_scale = 1.0 / math.sqrt(lat_total * lon_count)
    summed = lax.psum(
        (
            totals[0] * grad_scale,
            totals[1] * grad_scale,
            totals[2] * grad_scale,
            totals[3] * grad_scale,
            totals[4] * grad_scale,
        ),
        ("lat", "lev"),
    )
    return (new_state, spectral, summed[0], summed[1], summed[2], summed[3], summed[4])


LANES = 128
half_lanes = LANES // 2
feature_rows = 16
bf16 = jnp.bfloat16
f32 = jnp.float32
forward_type = f32
inverse_type = bf16
state_type = bf16
grad_type = bf16
row_gap = 8


def contract_last(left, right):
    return lax.dot_general(left, right, (((1,), (1,)), ((), ())), preferred_element_type=f32)


def matmul(left, right):
    return lax.dot_general(left, right, (((1,), (0,)), ((), ())), preferred_element_type=f32)


def half_turn_sincos(half_angle):
    square = half_angle * half_angle
    sine = 0.0
    cosine = 0.0
    for power in range(6, -1, -1):
        sine = sine * square + (-1.0) ** power / math.factorial(2 * power + 1)
        cosine = cosine * square + (-1.0) ** power / math.factorial(2 * power)
    sine = sine * half_angle
    return 2.0 * sine * cosine, 1.0 - 2.0 * sine * sine


def turn_sincos(product, period):
    reduced = product - period * jnp.floor(product * (1.0 / period) + 0.5)
    return half_turn_sincos(reduced * (math.pi / period))


def lower_lanes(shape):
    return lax.broadcasted_iota(jnp.int32, shape, len(shape) - 1) < half_lanes


def split_pair(value):
    high = value.astype(bf16)
    return high, (value - high.astype(f32)).astype(bf16)


def polar_sine(lat_index, lat_total):
    nearest = jnp.minimum(lat_index, (lat_total - 1.0) - lat_index)
    return half_turn_sincos((nearest + 0.5) * (0.5 * math.pi / lat_total))


def wave_columns(waves_ref):
    return jnp.broadcast_to(waves_ref[...].astype(f32), (LANES, waves_ref.shape[1])).T


def fill_trig(waves_ref, trig_ref, wave_dev):
    wave_total = waves_ref.shape[1]
    lon_count = trig_ref.shape[1]
    waves = wave_columns(waves_ref)
    lane = lax.broadcasted_iota(jnp.int32, waves.shape, 1).astype(f32)
    sine, cosine = turn_sincos(waves * lane, float(lon_count))
    step_sine, step_cosine = turn_sincos(waves * float(LANES), float(lon_count))
    for tile in range(lon_count // LANES):
        lanes = pl.ds(tile * LANES, LANES)
        cosines = split_pair(cosine)
        sines = split_pair(-sine)
        for owner in range(wave_total // wave_dev):
            rows = slice(owner * wave_dev, (owner + 1) * wave_dev)
            for part in range(2):
                place = 2 * part * wave_total + 2 * owner * wave_dev
                trig_ref[pl.ds(place, wave_dev), lanes] = cosines[part][rows]
                trig_ref[pl.ds(place + wave_dev, wave_dev), lanes] = sines[part][rows]
        cosine, sine = (
            cosine * step_cosine - sine * step_sine,
            sine * step_cosine + cosine * step_sine,
        )


def forward_kernel(lats_ref, waves_ref, prog_hbm, send_ref, trig_ref, prog_ref, prog_sem):
    prog_copy = pltpu.make_async_copy(prog_hbm, prog_ref, prog_sem)
    prog_copy.start()
    lat_width, half_rows, _ = send_ref.shape
    wave_total = waves_ref.shape[1]
    rows_total, lon_count = prog_ref.shape
    lat_total = lats_ref.shape[0]
    lat_dev = lat_total // lat_width
    fill_trig(waves_ref, trig_ref, wave_total // lat_width)
    prog_copy.wait()
    prog_high, prog_low = split_pair(prog_ref[...])
    modes = contract_last(
        jnp.concatenate([prog_high, prog_low], axis=0), trig_ref[pl.ds(0, 2 * wave_total), :]
    )
    modes = modes[:rows_total] + modes[rows_total:] + contract_last(
        prog_high, trig_ref[pl.ds(2 * wave_total, 2 * wave_total), :]
    )
    first_row = lax.axis_index("lat") * lat_dev
    row = lax.broadcasted_iota(jnp.int32, (lat_dev, LANES), 0)
    lat_index = jnp.zeros((lat_dev, LANES), f32)
    for at in range(lat_dev):
        lat_index = jnp.where(row == at, lats_ref[first_row + at].astype(f32), lat_index)
    weight = polar_sine(lat_index, lat_total)[0] * (math.pi / lat_total / lon_count)
    weight = jnp.concatenate([weight] * (half_rows // lat_dev), axis=0)
    lower = lower_lanes((half_rows, LANES))
    for tile in range(lat_width // 2):
        first = modes[:half_rows, tile * LANES : (tile + 1) * LANES] * weight
        second = modes[half_rows:, tile * LANES : (tile + 1) * LANES] * weight
        send_ref[2 * tile] = jnp.where(lower, first, pltpu.roll(second, half_lanes, 1)).astype(
            send_ref.dtype
        )
        send_ref[2 * tile + 1] = jnp.where(
            lower, pltpu.roll(first, half_lanes, 1), second
        ).astype(send_ref.dtype)


def cotangent_kernel(cot_ref, *rest):
    *cot_refs, cot_scratch = rest
    lev_width = len(cot_refs)
    rows_total, lon_count = cot_ref.shape
    row_share = cot_refs[0].shape[0] // (feature_rows * 3 // 4)
    lat_dev = lev_width * row_share
    pairs = rows_total // lat_dev
    cot_scratch[...] = jnp.zeros_like(cot_scratch)
    cot_all = cot_ref[...].astype(f32)
    tiles = lon_count // LANES
    for tile in range(tiles):
        cot_scratch[tile, pl.ds(0, rows_total), :] = cot_all[:, tile * LANES : (tile + 1) * LANES]
    for shift in range(lev_width):
        dest = (lax.axis_index("lev") + shift) % lev_width
        for tile in range(tiles):
            picked = [
                cot_scratch[tile, pl.ds(dest * row_share + share, pairs, stride=lat_dev), :]
                for share in range(row_share)
            ]
            cot_refs[shift][:, pl.ds(tile * LANES, LANES)] = jnp.concatenate(picked, axis=0).astype(bf16)


def level_major(pair, fields, lev_dev):
    return pair % lev_dev * fields + pair // lev_dev


def table_kernel(damping_ref, lats_ref, waves_ref, out_ref, damp_ref, root_ref, scratch, columns):
    pair_count, degrees, _ = out_ref.shape
    rows = pair_count
    lat_total = lats_ref.shape[1]
    columns[...] = wave_columns(waves_ref)
    first_wave = pl.multiple_of(lax.axis_index("lat") * 2 * rows, 2 * rows)
    orders = jnp.where(
        lower_lanes((rows, LANES)),
        columns[pl.ds(first_wave, rows), :],
        columns[pl.ds(first_wave + rows, rows), :],
    )
    fields, lev_dev = damping_ref.shape
    pairs = fields * lev_dev
    degree = lax.broadcasted_iota(jnp.int32, (pairs, degrees), 1).astype(f32)
    degree_ratio = degree * (degree + 1.0) * (1.0 / (degrees * (degrees - 1.0)))
    root = jnp.sqrt(2.0 * degree + 1.0)
    row = lax.broadcasted_iota(jnp.int32, (pairs, degrees), 0)
    strength = jnp.zeros((pairs, degrees), f32)
    for pair in range(pairs):
        at = level_major(pair, fields, lev_dev)
        strength = jnp.where(row == at, damping_ref[pair // lev_dev, pair % lev_dev], strength)
    damp = root / (1.0 + strength * (degree_ratio * degree_ratio))
    damp_ref[...] = jnp.concatenate([damp, damp, damp, damp], axis=0)
    waves = columns[pl.ds(first_wave, 2 * rows), :]
    waves = jnp.concatenate([waves] * (degrees // LANES), axis=1)
    root_ref[...] = jnp.where(waves == 0.0, 1.0, 2.0) * root[:1]
    lat_row = lats_ref[...].astype(f32)
    lat_index = jnp.broadcast_to(jnp.concatenate([lat_row, lat_row], axis=1), (rows, LANES))
    sine, cosine = polar_sine(lat_index, lat_total)
    cosine = jnp.where(2.0 * lat_index < lat_total - 1.0, cosine, -cosine)
    index = lax.broadcasted_iota(jnp.int32, (rows, degrees), 1).astype(f32)
    index = jnp.maximum(index, 1.0)
    ratios = 0.5 * jnp.log((2.0 * index + 1.0) / (2.0 * index))
    position = lax.broadcasted_iota(jnp.int32, (rows, degrees), 1)
    counted = position.astype(f32)
    totals = []
    for half in range(2):
        wave = jnp.broadcast_to(orders[:, half * half_lanes : half * half_lanes + 1], (rows, degrees))
        chosen = jnp.where((position > 0) & (counted <= wave), ratios, 0.0)
        totals.append(jnp.broadcast_to(jnp.sum(chosen, axis=1, keepdims=True), (rows, LANES)))
    diagonal_log = jnp.where(lower_lanes((rows, LANES)), totals[0], totals[1])
    log_shift = (
        diagonal_log
        - 0.5 * math.log(2.0)
        - 0.5 * jnp.log(2.0 * orders + 1.0)
        + orders * jnp.log(sine)
    )
    squared = orders * orders
    limit = 2.0**rescale_bits
    zero = jnp.zeros((rows, LANES), f32)

    def visit(block, carried):
        latest, before, previous_root, log_shift = carried
        scale = jnp.exp(log_shift)
        for offset in range(8):
            degree_int = block * 8 + offset
            degree = jnp.full((rows, LANES), degree_int, jnp.int32).astype(f32)
            gap = degree * degree - squared
            inverse_root = lax.rsqrt(jnp.maximum(gap, 1.0))
            root = gap * inverse_root
            recurred = inverse_root * (
                (2.0 * degree - 1.0) * cosine * latest - previous_root * before
            )
            newest = jnp.where(gap > 0.0, recurred, jnp.where(gap == 0.0, 1.0, 0.0))
            scratch[pl.ds(degree_int * (rows + row_gap), rows), :] = newest * scale
            before = latest
            latest = newest
            previous_root = jnp.maximum(root, 0.0)
        too_large = jnp.abs(latest) > limit
        factor = jnp.where(too_large, 1.0 / limit, 1.0)
        log_shift = log_shift + jnp.where(too_large, rescale_bits * math.log(2.0), 0.0)
        return latest * factor, before * factor, previous_root, log_shift

    lax.fori_loop(0, degrees // 8, visit, (zero, zero, zero, log_shift))

    def unpack(pair, carried):
        high, low = split_pair(scratch[pl.ds(pair, degrees, stride=rows + row_gap), :])
        out_ref[pair, :, pl.ds(0, LANES)] = high
        out_ref[pair, :, pl.ds(LANES, LANES)] = low
        return carried

    lax.fori_loop(0, pair_count, unpack, 0)


def spectral_kernel(
    recv_ref, table_ref, damp_ref, root_ref, spec_ref, send_ref, modes, sums, picked, rooted_ref
):
    pair_count, degrees, _ = table_ref.shape
    wave_dev = 2 * pair_count
    lat_width, half_rows, _ = recv_ref.shape
    lat_total = LANES // 2
    lat_dev = lat_total // lat_width
    _, _, lev_dev, fields, _ = spec_ref.shape
    pairs = fields * lev_dev
    half_pairs = pairs // 2
    pitch = wave_dev + row_gap
    received = recv_ref[...].astype(f32)
    upper_rows = lax.broadcasted_iota(jnp.int32, (LANES, LANES), 0) % wave_dev >= pair_count
    for index in range(half_pairs):
        stacked = [
            received[source, index * lat_dev : (index + 1) * lat_dev] for source in range(lat_width)
        ]
        stacked.append(jnp.zeros((LANES - lat_total, LANES), f32))
        turned = jnp.concatenate(stacked, axis=0).T
        turned = jnp.where(upper_rows, pltpu.roll(turned, half_lanes, 1), turned)
        for half in range(2):
            for part in range(2):
                start = (half * 2 + part) * wave_dev
                place = (part * pairs + level_major(half * half_pairs + index, fields, lev_dev)) * pitch
                modes[pl.ds(place, wave_dev), :] = turned[start : start + wave_dev]
    damp = damp_ref[...]
    count = 2 * pairs
    for pair in range(pair_count):
        first = modes[pl.ds(pair, count, stride=pitch), :]
        second = modes[pl.ds(pair + pair_count, count, stride=pitch), :]
        stacked = jnp.concatenate([first, second], axis=0)
        table = table_ref[pair]
        if recv_ref.dtype == f32:
            stacked = jnp.concatenate(split_pair(stacked), axis=0)
        else:
            stacked = stacked.astype(bf16)
        coeffs = contract_last(jnp.concatenate([stacked, stacked], axis=1), table)
        if recv_ref.dtype == f32:
            coeffs = coeffs[: 2 * count] + coeffs[2 * count :]
        coeffs = coeffs * damp
        shape = (2, lev_dev, fields, degrees)
        spec_ref[pair] = coeffs[:count].reshape(shape)
        spec_ref[pair + pair_count] = coeffs[count:].reshape(shape)
        rooted = jnp.concatenate(
            [
                coeffs[:count] * root_ref[pl.ds(pair, 1), :],
                coeffs[count:] * root_ref[pl.ds(pair + pair_count, 1), :],
            ],
            axis=0,
        )
        rooted_ref[pair] = jnp.concatenate(split_pair(rooted), axis=0)
    for pair in range(pair_count):
        synth = matmul(rooted_ref[pair], table_ref[pair])
        synth = synth[: 2 * count] + synth[2 * count :]
        synth = synth[:, :LANES] + synth[:, LANES:]
        sums[pl.ds(pair, count, stride=pitch), :] = synth[:count]
        sums[pl.ds(pair + pair_count, count, stride=pitch), :] = synth[count:]
    owners = send_ref.shape[0] // (2 * pairs)
    lower = lower_lanes((owners, LANES))
    share = lat_total // owners
    blank = jnp.zeros((owners, LANES), f32)
    sent_rows = 2 * pairs

    def put(row, value):
        high = value.astype(bf16).astype(f32)
        picked[pl.ds(lat_total + row, owners, stride=sent_rows), :] = high
        picked[pl.ds(lat_total + pairs + row, owners, stride=sent_rows), :] = value - high

    for index in range(half_pairs):
        blocks = []
        for half in range(2):
            for part in range(2):
                place = (part * pairs + level_major(half * half_pairs + index, fields, lev_dev)) * pitch
                blocks.append(sums[pl.ds(place, wave_dev), :])
        stacked = jnp.concatenate(blocks, axis=0)
        stacked = jnp.where(upper_rows, pltpu.roll(stacked, half_lanes, 1), stacked)
        picked[pl.ds(0, lat_total), :] = stacked.T[:lat_total]
        even = picked[pl.ds(0, owners, stride=share), :]
        odd = picked[pl.ds(1, owners, stride=share), :]
        put(index, jnp.where(lower, even, pltpu.roll(odd, half_lanes, 1)))
        put(half_pairs + index, jnp.where(lower, pltpu.roll(even, half_lanes, 1), odd))
    send_ref[...] = picked[pl.ds(lat_total, owners * sent_rows), :].astype(send_ref.dtype)


def weights_kernel(
    wave_dev, scale_ref, waves_ref, select_ref, w_in_ref, b_in_ref, w_mid_ref, w_out_ref, b_mid_ref, gather_ref,
    trig_ref, in_ref, mid_ref, mid_turned_ref, out_ref, out_turned_ref, scale_out_ref, bias_row_ref, select_out_ref,
):
    bias_row_ref[...] = b_mid_ref[...]
    select_out_ref[...] = gather_ref[...]
    fill_trig(waves_ref, trig_ref, wave_dev)
    hidden = w_mid_ref.shape[0]
    padded = select_ref.shape[0]
    spare = feature_rows * 3 // 4
    select = select_ref[...]
    bias = jnp.broadcast_to(b_in_ref[...], (padded, hidden))
    high = bias.astype(bf16).astype(f32)
    row = lax.broadcasted_iota(jnp.int32, (padded, hidden), 0)
    spread = matmul(select, w_in_ref[...])
    spread = jnp.where(row == spare, high, jnp.where(row == spare + 1, bias - high, spread))
    in_ref[...] = spread.T.astype(bf16)
    mid_ref[...] = w_mid_ref[...]
    mid_turned_ref[...] = w_mid_ref[...].astype(f32).T.astype(bf16)
    spread_out = matmul(select, w_out_ref[...])
    out_ref[...] = spread_out.astype(bf16)
    out_turned_ref[...] = spread_out.T.astype(bf16)
    fields, lev_total = scale_ref.shape
    lev_dev = spare // fields
    row = lax.broadcasted_iota(jnp.int32, (padded, LANES), 0)
    scales = jnp.zeros((padded, LANES), f32)
    for field in range(fields):
        for level in range(lev_total):
            place = level // lev_dev * feature_rows + field * lev_dev + level % lev_dev
            scales = jnp.where(row == place, scale_ref[field, level], scales)
    scale_out_ref[...] = scales


def columns_kernel(lev_width, recv_ref, *rest):
    cot_refs, rest = rest[:lev_width], rest[lev_width:]
    trig_ref, w_in_ref, w_mid_ref, w_turned_ref, *rest = rest
    w_out_ref, w_out_turned_ref, scale_ref, bias_row_ref, *rest = rest
    state_refs, rest = rest[:lev_width], rest[lev_width:]
    keep_ref, give_ref, packed, modes, cot_all, state_all, grad_in, grad_mid, grad_out, grad_bias, bias_ref = rest
    spare = feature_rows * 3 // 4
    row_share, lon_count = cot_refs[0].shape[0] // spare, cot_refs[0].shape[1]
    lat_width = recv_ref.shape[0] // lev_width
    level = lax.axis_index("lev")
    padded = lev_width * feature_rows
    hidden = w_mid_ref.shape[0]
    spare = feature_rows * 3 // 4
    lower = lower_lanes((padded, LANES))
    feature = lax.broadcasted_iota(jnp.int32, (lev_width, feature_rows, LANES), 1)

    def unfold(owner):
        piece = recv_ref[pl.ds(owner * lev_width, lev_width)].astype(f32)
        rest = pltpu.roll(piece, spare, 1)
        return [
            jnp.where(feature < spare, part[:, :feature_rows], 0.0).reshape(padded, LANES)
            for part in (piece, rest)
        ]

    for tile in range(lat_width // 2):
        firsts, seconds = unfold(2 * tile), unfold(2 * tile + 1)
        lanes = pl.ds(tile * LANES, LANES)
        for part, (first, second) in enumerate(zip(firsts, seconds)):
            rows = pl.ds(part * padded, padded)
            modes[0, rows, lanes] = jnp.where(lower, first, pltpu.roll(second, half_lanes, 1)).astype(bf16)
            modes[1, rows, lanes] = jnp.where(lower, pltpu.roll(first, half_lanes, 1), second).astype(bf16)
    for shift in range(lev_width):
        source = (level + (lev_width - shift)) % lev_width
        start = pl.multiple_of(source * feature_rows, feature_rows)
        piece = cot_refs[shift][...].astype(f32)
        row = lax.broadcasted_iota(jnp.int32, (feature_rows, lon_count), 0)
        for share in range(row_share):
            turned = pltpu.roll(piece, piece.shape[0] - share * spare, 0) if share else piece
            turned = jnp.where(row < spare, turned[:feature_rows], 0.0)
            cot_all[share, pl.ds(start, feature_rows), :] = turned.astype(bf16)
    grad_in[...] = jnp.zeros_like(grad_in)
    grad_mid[...] = jnp.zeros_like(grad_mid)
    grad_out[...] = jnp.zeros_like(grad_out)
    grad_bias[...] = jnp.zeros_like(grad_bias)
    bias_ref[...] = jnp.broadcast_to(bias_row_ref[...], (LANES, hidden)).T
    width = 6 * LANES
    while lon_count % width:
        width //= 2
    blocks = lon_count // width

    def visit(block, carried):
        share = block // blocks
        lanes = pl.ds(pl.multiple_of(block % blocks * width, width), width)
        half = trig_ref.shape[0] // 2
        filtered = matmul(modes[share], trig_ref[pl.ds(0, half), lanes])
        filtered = filtered[:padded] + filtered[padded:]
        filtered += matmul(modes[share, :padded], trig_ref[pl.ds(half, half), lanes])
        row = lax.broadcasted_iota(jnp.int32, (padded, width), 0)
        scaled = filtered * jnp.concatenate([scale_ref[...]] * (width // LANES), axis=1)
        inputs = jnp.where((row == spare) | (row == spare + 1), 1.0, scaled).astype(bf16)
        upstream = cot_all[share, :, lanes]
        pre_in = matmul(w_in_ref[...], inputs)
        gate = 0.5 + 0.5 * jnp.tanh(0.5 * pre_in)
        active = pre_in * gate
        slope_in = gate + active * (1.0 - gate)
        hidden_in = active.astype(bf16)
        bias = jnp.concatenate([bias_ref[...]] * (width // LANES), axis=1)
        pre_mid = matmul(w_mid_ref[...], hidden_in) + bias
        gate = 0.5 + 0.5 * jnp.tanh(0.5 * pre_mid)
        active = pre_mid * gate
        slope_mid = gate + active * (1.0 - gate)
        hidden_mid = active.astype(bf16)
        tendency = matmul(w_out_ref[...], hidden_mid).astype(bf16).astype(f32)
        state_all[share, :, lanes] = (filtered + tendency).astype(state_all.dtype)
        delta = matmul(w_out_turned_ref[...], upstream) * slope_mid
        delta_mid = delta.astype(bf16)
        grad_out[...] += contract_last(upstream, hidden_mid)
        grad_mid[...] += contract_last(delta_mid, hidden_in)
        total = delta[:, :LANES]
        for tile in range(1, width // LANES):
            total = total + delta[:, tile * LANES : (tile + 1) * LANES]
        grad_bias[...] += total
        delta_in = (matmul(w_turned_ref[...], delta_mid) * slope_in).astype(bf16)
        grad_in[...] += contract_last(inputs, delta_in)
        return carried

    lax.fori_loop(0, row_share * blocks, visit, 0)
    for shift in range(lev_width):
        dest = (level + shift) % lev_width
        start = pl.multiple_of(dest * feature_rows, feature_rows)
        for tile in range(lon_count // LANES):
            parts = [
                state_all[share, pl.ds(start, feature_rows), pl.ds(tile * LANES, LANES)].astype(f32)[:spare]
                for share in range(row_share)
            ]
            state_refs[shift][pl.ds(tile * row_share * spare, row_share * spare), :] = jnp.concatenate(
                parts, axis=0
            ).astype(bf16)
    bias_row = lax.dot_general(
        jnp.ones((8, LANES), f32), grad_bias[...], (((1,), (1,)), ((), ())),
        precision=lax.Precision.HIGHEST, preferred_element_type=f32,
    )[:1]
    row = lax.broadcasted_iota(jnp.int32, (padded, hidden), 0)
    first_rows = jnp.where(row == spare + 1, jnp.broadcast_to(bias_row, (padded, hidden)), grad_in[...])
    total_rows = hidden + 2 * padded
    for tile in range(hidden // LANES):
        lanes = slice(tile * LANES, (tile + 1) * LANES)
        start = tile * total_rows
        packed[pl.ds(start, hidden), :] = grad_mid[:, lanes]
        packed[pl.ds(start + hidden, padded), :] = first_rows[:, lanes]
        packed[pl.ds(start + hidden + padded, padded), :] = grad_out[:, lanes]
    half_rows = packed.shape[0] // 2
    side = lax.axis_index("lat") % 2
    keep_ref[...] = packed[pl.ds(pl.multiple_of(side * half_rows, 16), half_rows), :]
    give_ref[...] = packed[pl.ds(pl.multiple_of((1 - side) * half_rows, 16), half_rows), :].astype(
        give_ref.dtype
    )


def part_rows(index, ref):
    count = ref.shape[0]
    return pl.ds(pl.multiple_of(index * count, 16), count)


def plane_scatter_kernel(keep_ref, recv_ref, rest_ref, *send_refs):
    chip = lax.axis_index("lat") // 2
    for offset, ref in enumerate((rest_ref, *send_refs)):
        rows = part_rows(chip ^ offset, ref)
        ref[...] = (keep_ref[rows, :] + recv_ref[rows, :].astype(f32)).astype(ref.dtype)


def plane_sum_kernel(keep_ref, *rest):
    *recv_refs, out_ref = rest
    total = keep_ref[...]
    for ref in recv_refs:
        total = total + ref[...].astype(f32)
    out_ref[...] = total.astype(out_ref.dtype)


def reduce_kernel(grad_scale, *refs):
    *part_refs, out_ref, ordered = refs
    width = len(part_refs)
    level = lax.axis_index("lev")
    for shift, ref in enumerate(part_refs):
        ordered[(level + (width - shift)) % width] = ref[...]
    total = ordered[0].astype(f32)
    for source in range(1, width):
        total = total + ordered[source].astype(f32)
    out_ref[...] = (total * grad_scale).astype(bf16)


def plane_gather_kernel(*refs):
    *part_refs, out_ref = refs
    chip = lax.axis_index("lat") // 2
    for offset, ref in enumerate(part_refs):
        out_ref[part_rows(chip ^ offset, ref), :] = ref[...]


def state_kernel(row_share, *refs):
    *recv_refs, out_ref, scratch = refs
    lev_width = len(recv_refs)
    lat_dev = lev_width * row_share
    pairs = out_ref.shape[0] // lat_dev
    tiles = out_ref.shape[1] // LANES
    for shift, ref in enumerate(recv_refs):
        source = (lax.axis_index("lev") + (lev_width - shift)) % lev_width
        for tile in range(tiles):
            rows = ref[pl.ds(tile * row_share * pairs, row_share * pairs), :].astype(f32)
            for share in range(row_share):
                scratch[tile, pl.ds(source * row_share + share, pairs, stride=lat_dev), :] = rows[
                    share * pairs : (share + 1) * pairs
                ]
    for tile in range(tiles):
        out_ref[:, pl.ds(tile * LANES, LANES)] = scratch[tile]


def unpack_kernel(own, packed_ref, select_ref, *rest):
    *rest, in_rows, bin_row, mid_rows, bmid_row, out_rows, sems = rest
    outputs = rest[-5:]
    hidden, width = mid_rows.shape
    padded = select_ref.shape[1]
    spare = feature_rows * 3 // 4
    total_rows = hidden + 2 * padded
    select = select_ref[...]
    side = lax.axis_index("lat") % 2
    half = side if own else 1 - side
    columns = pl.ds(pl.multiple_of(half * width, width), width)
    for tile in range(width // LANES):
        lanes = pl.ds(tile * LANES, LANES)
        start = tile * total_rows
        mid_rows[:, lanes] = packed_ref[pl.ds(start, hidden), :].astype(f32)
        rows = packed_ref[pl.ds(start + hidden, padded), :]
        wide = rows.astype(f32)
        bin_row[:, lanes] = wide[spare : spare + 1]
        bmid_row[:, lanes] = wide[spare + 1 : spare + 2]
        in_rows[:, lanes] = matmul(select, rows)
        out_rows[:, lanes] = matmul(select, packed_ref[pl.ds(start + hidden + padded, padded), :])
    copies = [
        pltpu.make_async_copy(rows, output.at[:, columns], sems.at[at])
        for at, (rows, output) in enumerate(
            zip((in_rows, bin_row, mid_rows, bmid_row, out_rows), outputs)
        )
    ]
    for copy in copies:
        copy.start()
    for copy in copies:
        copy.wait()


def shaped(shape, kind=f32):
    return jax.ShapeDtypeStruct(shape, kind)


def room(mib):
    return pltpu.CompilerParams(vmem_limit_bytes=mib << 20)


def kept(shape, kind=f32):
    return pltpu.VMEM(shape, kind)


def near(array):
    return pltpu.with_memory_space_constraint(array, pltpu.VMEM)


def far(array):
    return pltpu.with_memory_space_constraint(array, pltpu.HBM)


def cost(flops, moved):
    return pl.CostEstimate(flops=flops, transcendentals=0, bytes_accessed=moved)


def rotate(pieces, width):
    moved = [pieces[0]]
    for shift in range(1, width):
        route = [(source, (source + shift) % width) for source in range(width)]
        moved.append(lax.ppermute(pieces[shift], "lev", route))
    return moved


def on_device_fast(
    prognostic, cotangent, damping, in_scale, w_in, b_in, w_mid, b_mid, w_out, wave_order, lat_order
):
    fields, lev_dev, lat_dev, lon_count = prognostic.shape
    lat_width = lax.axis_size("lat")
    lev_width = lax.axis_size("lev")
    wave_total = wave_order.shape[0]
    wave_dev = wave_total // lat_width
    lat_total = lat_order.shape[0]
    pairs = fields * lev_dev
    row_share = lat_dev // lev_width
    hidden, features = w_in.shape
    padded = lev_width * feature_rows
    owners = lat_width * lev_width
    pair_count = wave_dev // 2
    lev_total = lev_dev * lev_width

    select = np.zeros((features, padded), np.float32)
    for field in range(fields):
        for level in range(lev_total):
            place = level // lev_dev * feature_rows + field * lev_dev + level % lev_dev
            select[field * lev_total + level, place] = 1.0
    spread_select = jnp.asarray(select.T, bf16)
    select = jnp.asarray(select, bf16)

    smem = pl.BlockSpec(memory_space=pltpu.SMEM)
    hbm = pl.BlockSpec(memory_space=pltpu.HBM)
    vmem = pl.BlockSpec(memory_space=pltpu.VMEM)
    wave_row = wave_order.reshape(1, wave_total)
    piece = (row_share * pairs, lon_count)
    send = pl.pallas_call(
        forward_kernel,
        in_specs=[smem, vmem, hbm],
        out_shape=kept((lat_width, pairs * lat_dev // 2, LANES), forward_type),
        scratch_shapes=[
            pltpu.VMEM((4 * wave_total, lon_count), bf16),
            pltpu.VMEM((pairs * lat_dev, lon_count), f32),
            pltpu.SemaphoreType.DMA(()),
        ],
        compiler_params=room(16),
        name="forward",
    )(far(lat_order), far(wave_row), far(prognostic.reshape(pairs * lat_dev, lon_count)))
    cot_pieces = pl.pallas_call(
        cotangent_kernel,
        out_shape=[kept(piece, bf16)] * lev_width,
        scratch_shapes=[pltpu.VMEM((lon_count // LANES, feature_rows * lat_dev, LANES), f32)],
        cost_estimate=cost(2000000, 1 << 19),
        compiler_params=room(8),
        name="cotangent",
    )(far(cotangent.reshape(pairs * lat_dev, lon_count)))
    received = lax.all_to_all(send, "lat", split_axis=0, concat_axis=0, tiled=True)
    received, cot_pieces = lax.optimization_barrier((received, cot_pieces))
    upstream = rotate(cot_pieces, lev_width)
    table, damp, roots = pl.pallas_call(
        table_kernel,
        in_specs=[smem, vmem, vmem],
        out_shape=(
            kept((pair_count, TRUNC, 2 * LANES), bf16),
            kept((4 * pairs, TRUNC)),
            kept((wave_dev, TRUNC)),
        ),
        scratch_shapes=[
            pltpu.VMEM((TRUNC * (pair_count + row_gap), LANES), f32),
            pltpu.VMEM((wave_total, LANES), f32),
        ],
        cost_estimate=cost(8000000, 1 << 20),
        compiler_params=room(16),
        name="legendre",
    )(far(damping), far(lat_order.reshape(1, lat_total)), far(wave_row))
    spectral, modes_send = pl.pallas_call(
        spectral_kernel,
        out_shape=(
            pltpu.HBM((wave_dev, 2, lev_dev, fields, TRUNC), f32),
            kept((owners * 2 * pairs, LANES), bf16),
        ),
        scratch_shapes=[
            pltpu.VMEM((2 * pairs * (wave_dev + row_gap), LANES), f32),
            pltpu.VMEM((2 * pairs * (wave_dev + row_gap), LANES), f32),
            pltpu.VMEM((lat_total + owners * 2 * pairs, LANES), f32),
            pltpu.VMEM((pair_count, 8 * pairs, TRUNC), bf16),
        ],
        compiler_params=room(16),
        name="spectral",
    )(*map(near, (received, table, damp, roots)))
    both = ("lat", "lev")
    modes = lax.all_to_all(
        modes_send.reshape(owners, 2 * pairs, LANES), both, split_axis=0, concat_axis=0, tiled=True
    )
    *prepared, chosen = pl.pallas_call(
        functools.partial(weights_kernel, wave_dev),
        out_shape=(
            kept((4 * wave_total, lon_count), bf16),
            kept((hidden, padded), bf16),
            kept((hidden, hidden), bf16),
            kept((hidden, hidden), bf16),
            kept((padded, hidden), bf16),
            kept((hidden, padded), bf16),
            kept((padded, LANES)),
            kept((1, hidden)),
            kept((features, padded), bf16),
        ),
        in_specs=[smem] + [vmem] * 8,
        cost_estimate=cost(4000000, 1 << 20),
        compiler_params=room(12),
        name="weights",
    )(
        far(in_scale),
        far(wave_row),
        far(spread_select),
        far(w_in.T),
        far(b_in.reshape(1, hidden)),
        far(w_mid),
        far(w_out),
        far(b_mid.reshape(1, hidden)),
        far(select),
    )
    total_rows = hidden + 2 * padded
    packed_rows = total_rows * (hidden // LANES)
    state_rows = row_share * pairs * (lon_count // LANES)
    *state_pieces, keep, give = pl.pallas_call(
        functools.partial(columns_kernel, lev_width),
        out_shape=(
            *([kept((state_rows, LANES), state_type)] * lev_width),
            kept((packed_rows // 2, LANES)),
            kept((packed_rows // 2, LANES), grad_type),
        ),
        scratch_shapes=[
            pltpu.VMEM((packed_rows, LANES), f32),
            pltpu.VMEM((row_share, 2 * padded, 2 * wave_total), bf16),
            pltpu.VMEM((row_share, padded, lon_count), bf16),
            pltpu.VMEM((row_share, padded, lon_count), state_type),
            pltpu.VMEM((padded, hidden), f32),
            pltpu.VMEM((hidden, hidden), f32),
            pltpu.VMEM((padded, hidden), f32),
            pltpu.VMEM((hidden, LANES), f32),
            pltpu.VMEM((hidden, LANES), f32),
        ],
        compiler_params=room(24),
        name="columns",
    )(
        *map(near, (modes, *upstream, *prepared))
    )
    chips = lat_width // 2
    quarter = packed_rows // lat_width
    partner = [(at, at ^ 1) for at in range(lat_width)]
    routes = [[(at, at ^ (2 * offset)) for at in range(lat_width)] for offset in range(1, chips)]
    taken = lax.ppermute(give, "lat", partner)
    rest, *sends = pl.pallas_call(
        plane_scatter_kernel,
        out_shape=(
            kept((quarter, LANES)),
            *([kept((quarter, LANES), grad_type)] * (chips - 1)),
        ),
        compiler_params=room(8),
        name="plane_scatter",
    )(near(keep), near(taken))
    taken = [lax.ppermute(send, "lat", route) for send, route in zip(sends, routes)]
    taken, state = lax.optimization_barrier((taken, rotate(state_pieces, lev_width)))
    mine = pl.pallas_call(
        plane_sum_kernel,
        out_shape=kept((quarter, LANES), grad_type),
        compiler_params=room(8),
        name="plane_sum",
    )(*map(near, (rest, *taken)))
    grad_scale = 1.0 / math.sqrt(lat_total * lon_count)
    joined = pl.pallas_call(
        functools.partial(reduce_kernel, grad_scale),
        out_shape=kept((quarter, LANES), grad_type),
        scratch_shapes=[pltpu.VMEM((lev_width, quarter, LANES), grad_type)],
        compiler_params=room(8),
        name="reduce",
    )(*map(near, rotate([mine] * lev_width, lev_width)))
    new_state = pl.pallas_call(
        functools.partial(state_kernel, row_share),
        out_shape=pltpu.HBM((pairs * lat_dev, lon_count), f32),
        scratch_shapes=[pltpu.VMEM((lon_count // LANES, pairs * lat_dev, LANES), f32)],
        cost_estimate=cost(2000000, 1 << 19),
        compiler_params=room(8),
        name="state",
    )(*map(near, state))
    joined, new_state = lax.optimization_barrier((joined, new_state))
    parts = [joined] + [lax.ppermute(joined, "lat", route) for route in routes]
    joined = pl.pallas_call(
        plane_gather_kernel,
        out_shape=kept((packed_rows // 2, LANES), grad_type),
        compiler_params=room(8),
        name="plane_gather",
    )(*map(near, parts))
    other = lax.ppermute(joined, "lat", partner)
    shapes = ((features, hidden), (1, hidden), (hidden, hidden), (1, hidden), (features, hidden))

    def unpack(own, half, *filled):
        return pl.pallas_call(
            functools.partial(unpack_kernel, own),
            in_specs=[vmem, vmem] + [hbm] * len(filled),
            out_shape=[pltpu.HBM(shape, f32) for shape in shapes],
            out_specs=[hbm] * len(shapes),
            scratch_shapes=[pltpu.VMEM((rows, columns // 2), f32) for rows, columns in shapes]
            + [pltpu.SemaphoreType.DMA((len(shapes),))],
            input_output_aliases={2 + at: at for at in range(len(filled))},
            cost_estimate=cost(2000000, 1 << 19),
            compiler_params=room(8),
            name="unpack",
        )(near(half), near(chosen), *filled)

    grad_in, grad_bin, grad_mid, grad_bmid, grad_out = unpack(False, other, *unpack(True, joined))
    return (
        new_state.reshape(fields, lev_dev, lat_dev, lon_count),
        spectral.transpose(0, 1, 3, 2, 4),
        grad_in.T,
        grad_bin.reshape(hidden),
        grad_mid,
        grad_bmid.reshape(hidden),
        grad_out,
    )


def fits_fast(mesh, prognostic, w_in, wave_order, lat_order):
    lat_width, lev_width = mesh.shape["lat"], mesh.shape["lev"]
    fields, lev_total, lat_total, lon_count = prognostic.shape
    hidden = w_in.shape[0]
    pairs = fields * lev_total // lev_width
    lat_dev = lat_total // lat_width
    wave_dev = wave_order.shape[0] // lat_width
    packed_rows = (hidden + 2 * lev_width * feature_rows) * (hidden // LANES)
    return (
        2 * lat_total == LANES
        and 4 * wave_dev == LANES
        and lat_dev == 8
        and lat_dev == 2 * lev_width
        and pairs == feature_rows * 3 // 4
        and lon_count % LANES == 0
        and hidden % LANES == 0
        and packed_rows % (16 * lat_width * lev_width) == 0
        and lat_width & (lat_width - 1) == 0
        and lat_width > 2
        and lev_width & (lev_width - 1) == 0
    )


def solution(mesh):
    def run(*arguments):
        prognostic, w_in, wave_order, lat_order = (arguments[at] for at in (0, 4, 9, 10))
        fast = fits_fast(mesh, prognostic, w_in, wave_order, lat_order)
        return shard(mesh, on_device_fast if fast else on_device)(*arguments)

    return run


def shard(mesh, body):
    return jax.shard_map(
        body,
        mesh=mesh,
        in_specs=(
            P(None, "lev", "lat", None),
            P(None, "lev", "lat", None),
            P(None, "lev"),
            P(),
            P(),
            P(),
            P(),
            P(),
            P(),
            P(),
            P(),
        ),
        out_specs=(
            P(None, "lev", "lat", None),
            P("lat", None, None, "lev", None),
            P(),
            P(),
            P(),
            P(),
            P(),
        ),
        check_vma=False,
    )
```
